256 devices in a mesh: dp: 32 (over z, x), fsdp: 8 (over y, core).
Axes of the slice: x: 4, y: 4, z: 8, core: 2. Of those that a mesh axis runs over, the one named last changes fastest.
Arguments:
- latents: bfloat16 [384, 2, 4096], P('dp'), may hold values from -6 to 6
- noise: bfloat16 [384, 2, 4096], P('dp'), may hold values from -6 to 6
- behavior_velocity: bfloat16 [384, 2, 4096], P('dp'), may hold values from -6 to 6
- timestep: int32 [384, 2], P('dp'), may hold values from 0 to 9
- reward_rank_integer: int32 [384], P('dp'), may hold values from 0 to 1023
- surviving_source_index: int32 [192], replicated, may hold values from 0 to 31, as said below
- surviving_slot_index: int32 [192], replicated, may hold values from 0 to 11, as said below
- group_kept_count: int32 [48], replicated, may hold values from 1 to 24, 192 in all
- patch_input_weight: bfloat16 [64, 1536], replicated, may hold values from -0.75 to 0.75
- modulation_lookup: float32 [10, 3, 1536], replicated, may hold values from -3 to 3
- up_projection_weight: bfloat16 [1536, 8192], P(None, 'fsdp'), may hold values from -0.15625 to 0.15625
- down_projection_weight: bfloat16 [1536, 8192], P(None, 'fsdp'), may hold values from -0.0625 to 0.0625
- velocity_head_weight: bfloat16 [1536, 64], replicated, may hold values from -0.15625 to 0.15625
Outputs:
- up_weight_gradient: float32 [1536, 8192], P('dp', 'fsdp')
- down_weight_gradient: float32 [1536, 8192], P('dp', 'fsdp')
- loss: float32 [], replicated
The draws below stay inside these ranges and needn't reach their ends.
Inputs may be any that keep to these rules, and one draw needn't show every extreme that they name: `surviving_source_index`: survivors are listed by source in ascending order; survivor j is trained on dp index j // 6, and every survivor of source d is trained on dp index d or d + 1. `surviving_slot_index`: the slots of one source's survivors are distinct.
All inputs are finite; a program needn't handle non-finite values.
Results may differ from the reference program's by a relative error of at most 0.013.
Values may be sent and summed in bfloat16 or wider, within the bound.
A program may use at most 128 MiB of HBM per device.

```python
import math
import jax
import jax.numpy as jnp
import numpy as np
from jax import lax

D = 1536
FF = 8192
PATCH = 64
SEQ = 64
TRAINED_STEPS = 2
KSTEPS = 10
GROUP = 24
TRAJ_DEV = 6
SLOT_CAPACITY = 12
SURV = 192
PROMPTS = 48
N_DP = 32


def surviving_arrangement(key):
    base_key = jax.random.fold_in(key, 7)
    drifts = jax.random.randint(jax.random.fold_in(base_key, 1), (N_DP - 1,), 0, TRAJ_DEV + 1).astype(jnp.int32)
    nothing = jnp.zeros((1,), jnp.int32)
    drifts = jnp.concatenate([nothing, drifts, nothing])
    group_starts = jnp.arange(N_DP + 1, dtype=jnp.int32) * TRAJ_DEV + drifts
    positions = jnp.arange(N_DP * TRAJ_DEV, dtype=jnp.int32)
    source = jnp.sum((group_starts[None, 1:N_DP] <= positions[:, None]).astype(jnp.int32), axis=1)
    offset = positions - jnp.take(group_starts, source)
    scores = jax.random.randint(jax.random.fold_in(base_key, 2), (N_DP, SLOT_CAPACITY), 0, 1 << 20).astype(jnp.int32) * SLOT_CAPACITY + jnp.arange(SLOT_CAPACITY, dtype=jnp.int32)[None, :]
    ordering = jnp.argsort(scores, axis=1, stable=True).astype(jnp.int32)
    slot_ids = ordering[source, offset]
    return (source.astype(jnp.int32), slot_ids.astype(jnp.int32))


def draw_surviving_source_index(key, part):
    return surviving_arrangement(key)[0]


def draw_surviving_slot_index(key, part):
    return surviving_arrangement(key)[1]


def set_ends(entries, stream_key, least, top_value):
    longest = entries.shape.index(max(entries.shape))
    spots = []
    for shift in (0, 1):
        where = [jax.random.randint(jax.random.fold_in(stream_key, axis), (), 0, length) for axis, length in enumerate(entries.shape)]
        where[longest] = (where[longest] + shift) % entries.shape[longest]
        spots.append(tuple(where))
    return entries.at[spots[0]].set(least).at[spots[1]].set(top_value)


def block_levels(key, extent, shards, smallest, largest):
    gain, own = 1.0, jax.random.fold_in(key, 6)
    for axis_at, parts in shards:
        steps = jnp.exp(jax.random.uniform(jax.random.fold_in(own, axis_at), (parts,), jnp.float32, smallest / len(shards), largest / len(shards)))
        gain = gain * jnp.repeat(steps, extent[axis_at] // parts).reshape([-1 if axis == axis_at else 1 for axis in range(len(extent))])
    return gain


def split_up(amount, total, reach, skew):
    weights = [(1 << 20) // math.isqrt(rank ** skew) + 1 for rank in range(2, amount + 1)]
    surplus, given = total - reach - (amount - 1), [1] * (amount - 1)
    while surplus > 0:
        movable = [i for i in range(amount - 1) if given[i] < reach]
        pool, remaining = sum([weights[i] for i in movable]), surplus
        for i in movable:
            extra = min(reach - given[i], max(1, remaining * weights[i] // pool), surplus)
            given[i] = given[i] + extra
            surplus = surplus - extra
    return np.array([reach] + given)


def ragged(key, number_of, total, limit, skew):
    if number_of == 2:
        one = jax.random.randint(key, (), max(1, total - limit), min(limit, total - 1) + 1)
        return jnp.stack([one, total - one])
    tallies = jnp.asarray(split_up(number_of, total, limit, skew), jnp.int32)
    couples = (number_of - 1) // 2
    donor, receiver = tallies[1:1 + 2 * couples:2], tallies[2:2 + 2 * couples:2]
    room = jnp.minimum(donor - 1, limit - receiver)
    passed = jax.random.randint(jax.random.fold_in(key, 1), (couples,), 0, 1 << 20) % (room + 1)
    tallies = tallies.at[1:1 + 2 * couples:2].set(donor - passed).at[2:2 + 2 * couples:2].set(receiver + passed)
    return tallies[jax.random.permutation(jax.random.fold_in(key, 2), number_of)]


def centred(rng, extent, scale, most, cuts=(), held_as=jnp.bfloat16):
    array = jax.random.normal(rng, extent, jnp.float32) * scale
    if len(cuts) > 0:
        array = block_levels(rng, extent, cuts, -0.22, 0.18) * array
    return jnp.clip(array, min=-most, max=most).astype(held_as)


def setup_inputs(seed: int = 0) -> dict:
    keys = jax.random.split(jax.random.key(seed), 14)
    return {
        "latents": centred(keys[0], (N_DP * SLOT_CAPACITY, TRAINED_STEPS, SEQ * PATCH), 1.0, 6.0, ((0, 32),)),
        "noise": centred(keys[1], (N_DP * SLOT_CAPACITY, TRAINED_STEPS, SEQ * PATCH), 1.0, 6.0, ((0, 32),)),
        "behavior_velocity": centred(keys[2], (N_DP * SLOT_CAPACITY, TRAINED_STEPS, SEQ * PATCH), 1.0, 6.0, ((0, 32),)),
        "timestep": set_ends(jax.random.randint(keys[3], (N_DP * SLOT_CAPACITY, TRAINED_STEPS), 0, KSTEPS), jax.random.fold_in(keys[3], 1), 0, KSTEPS - 1).astype(jnp.int32),
        "reward_rank_integer": set_ends(jax.random.randint(keys[4], (N_DP * SLOT_CAPACITY,), 0, 1024), jax.random.fold_in(keys[4], 1), 0, 1023).astype(jnp.int32),
        "surviving_source_index": draw_surviving_source_index(jax.random.fold_in(keys[13], 71), 0),
        "surviving_slot_index": draw_surviving_slot_index(jax.random.fold_in(keys[13], 71), 0),
        "group_kept_count": ragged(keys[7], PROMPTS, SURV, GROUP, 2).astype(jnp.int32),
        "patch_input_weight": centred(keys[8], (PATCH, D), PATCH ** -0.5, 0.75),
        "modulation_lookup": centred(keys[9], (KSTEPS, 3, D), 0.5, 3.0, (), jnp.float32),
        "up_projection_weight": centred(keys[10], (D, FF), D ** -0.5, 0.15625, ((1, 8),)),
        "down_projection_weight": centred(keys[11], (D, FF), FF ** -0.5, 0.0625, ((1, 8),)),
        "velocity_head_weight": centred(keys[12], (D, PATCH), D ** -0.5, 0.15625),
    }


clip_range = 0.2
noise_level = 0.7
norm_eps = 1e-06

def step_ratio(indices, count):
    spacing = 1.0 / count
    level = 1.0 - indices.astype(jnp.float32) * spacing
    return jnp.sqrt(spacing * (1.0 - level + spacing) / level) / noise_level

def layer_norm(values):
    center = values - lax.optimization_barrier(jnp.mean(values, axis=-1, keepdims=True))
    variance = lax.optimization_barrier(jnp.mean(center * center, axis=-1, keepdims=True))
    inverse = lax.rsqrt(variance + norm_eps)
    return (center * inverse, inverse)

def smooth_gate(values):
    return jax.nn.gelu(values, approximate=True)

def membership_matrix(surviving_identifiers, kept_mask):
    group_ends = jnp.cumsum(kept_mask).astype(jnp.int32)
    group_starts = group_ends - kept_mask
    inside_clip_mask = (surviving_identifiers[:, None] >= group_starts[None, :]) & (surviving_identifiers[:, None] < group_ends[None, :])
    return inside_clip_mask.astype(jnp.int32)

def advantages(ranks, member_mask, kept_mask, sums):
    count = lax.optimization_barrier(jnp.sum(member_mask * kept_mask[None, :], axis=1))
    first = lax.optimization_barrier(jnp.sum(member_mask * sums[0][None, :], axis=1))
    second = lax.optimization_barrier(jnp.sum(member_mask * sums[1][None, :], axis=1))
    spread = (count * second - first * first).astype(jnp.float32)
    counts = count.astype(jnp.float32)
    deviation = jnp.sqrt(spread) / counts
    return (ranks.astype(jnp.float32) - first.astype(jnp.float32) / counts) / jnp.maximum(deviation, 1.0)

def reference(latents, noise, behavior_velocity, timestep, reward_rank_integer, surviving_source_index, surviving_slot_index, group_kept_count, patch_input_weight, modulation_lookup, up_projection_weight, down_projection_weight, velocity_head_weight):
    surviving_count = surviving_source_index.shape[0]
    picked_indices = (surviving_source_index * SLOT_CAPACITY + surviving_slot_index).astype(jnp.int32)
    ranks = jnp.take(reward_rank_integer, picked_indices)
    member_mask = membership_matrix(jnp.arange(surviving_count, dtype=jnp.int32), group_kept_count)
    sums = jnp.stack([lax.optimization_barrier(jnp.sum(member_mask * ranks[:, None], axis=0)), lax.optimization_barrier(jnp.sum(member_mask * (ranks * ranks)[:, None], axis=0))]).astype(jnp.int32)
    advantage = advantages(ranks, member_mask, group_kept_count, sums)
    width = patch_input_weight.shape[1]
    hidden_width = up_projection_weight.shape[1]
    contract = (((0,), (0,)), ((), ()))

    def visit_group(carry, index):
        up_weight_gradient, down_weight_gradient, total_count = carry
        pick = picked_indices[index]
        sample = lax.dynamic_index_in_dim(latents, pick, 0, False)
        drawn = lax.dynamic_index_in_dim(noise, pick, 0, False).astype(jnp.float32)
        target = lax.dynamic_index_in_dim(behavior_velocity, pick, 0, False).astype(jnp.float32)
        stamps = lax.dynamic_index_in_dim(timestep, pick, 0, False)
        advantage_gain = advantage[index]
        modulation = jnp.take(modulation_lookup, stamps, axis=0)
        inputs = sample.reshape(TRAINED_STEPS * SEQ, PATCH)
        embedded = jnp.dot(inputs, patch_input_weight, preferred_element_type=jnp.float32).reshape(TRAINED_STEPS, SEQ, width)
        normed, unused_value = layer_norm(embedded)
        modulated = (normed * (1.0 + modulation[:, 1][:, None]) + modulation[:, 0][:, None]).astype(jnp.bfloat16).reshape(TRAINED_STEPS * SEQ, width)
        pre = jnp.dot(modulated, up_projection_weight, preferred_element_type=jnp.float32)
        activated = smooth_gate(pre).astype(jnp.bfloat16)
        projected = lax.dot_general(activated, down_projection_weight, (((1,), (1,)), ((), ())), preferred_element_type=jnp.float32).reshape(TRAINED_STEPS, SEQ, width)
        gates = modulation[:, 2][:, None]
        mixed = embedded + gates * projected
        final, inverse = layer_norm(mixed)
        velocity = jnp.dot(final.astype(jnp.bfloat16).reshape(TRAINED_STEPS * SEQ, width), velocity_head_weight, preferred_element_type=jnp.float32).reshape(TRAINED_STEPS, SEQ * PATCH)
        coeff = step_ratio(stamps, KSTEPS)[:, None]
        error = velocity - target
        terms = coeff * drawn * error + 0.5 * coeff * coeff * error * error
        logratio = -lax.optimization_barrier(jnp.mean(terms, axis=1))
        likelihood_ratio = jnp.exp(logratio)
        clipped = jnp.clip(likelihood_ratio, 1.0 - clip_range, 1.0 + clip_range)
        plain = likelihood_ratio * advantage_gain
        bounded = clipped * advantage_gain
        unit_loss = -jnp.minimum(plain, bounded)
        live_mask = (plain <= bounded).astype(jnp.float32)
        loss_slope = (-advantage_gain * likelihood_ratio * live_mask / (surviving_count * TRAINED_STEPS))[:, None]
        dvelocity = (loss_slope * (-(coeff * drawn + coeff * coeff * error) / (SEQ * PATCH))).astype(jnp.bfloat16).reshape(TRAINED_STEPS * SEQ, PATCH)
        dfinal = lax.dot_general(dvelocity, velocity_head_weight, (((1,), (1,)), ((), ())), preferred_element_type=jnp.float32).reshape(TRAINED_STEPS, SEQ, width)
        dmixed = inverse * (dfinal - lax.optimization_barrier(jnp.mean(dfinal, axis=-1, keepdims=True)) - final * lax.optimization_barrier(jnp.mean(dfinal * final, axis=-1, keepdims=True)))
        upstream = (gates * dmixed).astype(jnp.bfloat16).reshape(TRAINED_STEPS * SEQ, width)
        down_weight_gradient = down_weight_gradient + lax.dot_general(upstream, activated, contract, preferred_element_type=jnp.float32)
        dactivated = jnp.dot(upstream, down_projection_weight, preferred_element_type=jnp.float32)
        unused_value, pull = jax.vjp(smooth_gate, pre)
        dpre = pull(dactivated)[0].astype(jnp.bfloat16)
        up_weight_gradient = up_weight_gradient + lax.dot_general(modulated, dpre, contract, preferred_element_type=jnp.float32)
        return ((up_weight_gradient, down_weight_gradient, total_count + jnp.sum(unit_loss)), None)
    group_start = (jnp.zeros((width, hidden_width), jnp.float32), jnp.zeros((width, hidden_width), jnp.float32), jnp.zeros((), jnp.float32))
    (up_weight_gradient, down_weight_gradient, total_count), unused_value = lax.scan(visit_group, group_start, jnp.arange(surviving_count, dtype=jnp.int32))
    return (up_weight_gradient, down_weight_gradient, total_count / (surviving_count * TRAINED_STEPS))
```

```python
import jax
import jax.numpy as jnp
from jax import lax
from jax.experimental import pallas as pl
from jax.experimental.pallas import tpu as pltpu
from jax.sharding import Mesh
from jax.sharding import PartitionSpec as P

MESH = pl.DeviceIdType.MESH
F32, BF16, I32 = jnp.float32, jnp.bfloat16, jnp.int32
NZ, NX, NY, NC = 8, 4, 4, 2
D, HID, TRAJ, SLOTS = 1536, 1024, 6, 12
UNITS, ROWS, CH = 12, 768, 192
KSTEPS = 10
SURV = 192
EPS = 1e-06
GELU_K = 0.7978845608028654
GELU_C = 0.044715


def tri(s):
    return lax.rem(s * s * s, 5)


def kernel(
    slot_s, src_s, cnt_s, src_v, slot_v, lat, noi, old, rank_v, time_v, wpatch, modl, wv, wup_h, wdn_h,
    out_up, out_dn, out_loss,
    meta, wup, wdn, snd_a, snd_b, rcv_a, rcv_b, meta_l, meta_all, meta_flat, tmp, xs, nz, od,
    mod_s, mod_c, mod_g, coef_u, adv_u, emb, modb, act, dg, dpre, dsend, drecv, pk, ysend, yrecv, pfull,
    fin, finb, inv, ups, mod_t, up_t, gu, gd, zr, xr, s2u, s2d, s2ur, s2dr, loss_own, loss_x, loss_z,
    lsem, ssem, rsem,
):
    z, x, y, c = (lax.axis_index(n) for n in ("z", "x", "y", "c"))
    owner = z * NX + x

    def dev(dz=0, dx=0, dy=0, dc=0):
        return (
            lax.rem(z + (dz + NZ), NZ),
            lax.rem(x + (dx + NX), NX),
            lax.rem(y + (dy + NY), NY),
            lax.rem(c + dc, NC),
        )

    nxt = lax.rem(owner + 1, NZ * NX)
    prv = lax.rem(owner + NZ * NX - 1, NZ * NX)
    next_dev = (nxt // NX, lax.rem(nxt, NX), y, c)
    prev_dev = (prv // NX, lax.rem(prv, NX), y, c)

    ids = {}

    def mid(name):
        return ids.setdefault(name, len(ids))

    sent = []

    def copy(name, src, dst, to):
        i = mid(name) if isinstance(name, str) else name
        return pltpu.make_async_remote_copy(
            src_ref=src, dst_ref=dst, send_sem=ssem.at[i], recv_sem=rsem.at[i],
            device_id=to, device_id_type=MESH,
        )

    def send(name, src, dst, to):
        d = copy(name, src, dst, to)
        d.start()
        sent.append(d)

    def recv(name, dst, to=None):
        copy(name, dst, dst, dev(dc=1) if to is None else to).wait_recv()

    barrier = pltpu.get_barrier_semaphore()
    peers = [dev(dx=i) for i in range(1, NX)] + [dev(dz=i) for i in range(1, NZ)]
    peers += [dev(dy=1), dev(dy=-1), dev(dc=1), next_dev, prev_dev]
    meta[0:1, 0:SLOTS] = rank_v[...]
    meta[1:3, 0:SLOTS] = time_v[...]
    for p in peers:
        pl.semaphore_signal(barrier, inc=1, device_id=p, device_id_type=MESH)
    cp_up = pltpu.make_async_copy(wup_h, wup, lsem.at[0])
    cp_dn = pltpu.make_async_copy(wdn_h, wdn, lsem.at[1])
    cp_up.start()
    cp_dn.start()
    lead_n = jnp.minimum(owner + 1, NZ * NX - 1) * TRAJ
    lead = owner * TRAJ
    for i in range(TRAJ):
        s = slot_s[lead_n + i]
        snd_a[i] = lat[s]
        snd_b[0, i] = noi[s]
        snd_b[1, i] = old[s]
    meta_all[z * NX + x] = meta[...]
    pl.semaphore_wait(barrier, len(peers))

    send("meta_l", meta, meta_l, next_dev)
    send("shift_a", snd_a, rcv_a, next_dev)
    send("shift_b", snd_b, rcv_b, next_dev)
    for i in range(1, NX):
        send(f"meta_x{i}", meta, meta_all.at[z * NX + x], dev(dx=i))

    slots = [slot_s[lead + i] for i in range(TRAJ)]
    lefts = [src_s[lead + i] != owner for i in range(TRAJ)]

    sub = lax.broadcasted_iota(I32, (16, 128), 0)
    lane = lax.broadcasted_iota(I32, (16, 128), 1)
    pos = jnp.zeros((16, 128), I32)
    from_left = jnp.zeros((16, 128), I32)
    for i in range(TRAJ):
        mine = (sub >> 1) == i
        pos = pos + jnp.where(mine, slots[i], 0)
        from_left = from_left + jnp.where(mine, lefts[i].astype(I32), 0)
    recv("meta_l", meta_l)

    def step_row(n):
        wide = [jnp.broadcast_to(m[n : n + 1, :], (16, 128)) for m in (meta_l, meta)]
        return jnp.where(from_left == 1, wide[0], wide[1])

    row = jnp.where((sub & 1) == 0, step_row(1), step_row(2))
    stamp = jnp.sum(jnp.where(lane == pos, row.astype(F32), 0.0), axis=1, keepdims=True)
    level = 1.0 - stamp * (1.0 / KSTEPS)
    coef = jnp.sqrt((1.0 / KSTEPS) * (1.0 - level + (1.0 / KSTEPS)) / level) / 0.7
    coef_u[...] = jnp.broadcast_to(coef, (16, 128))
    for kind, dst in ((0, mod_s), (1, mod_c), (2, mod_g)):
        acc = jnp.zeros((16, D), F32)
        for t in range(KSTEPS):
            acc = jnp.where(stamp == float(t), jnp.broadcast_to(modl[t, pl.ds(kind, 1), :], (16, D)), acc)
        dst[...] = acc + 1.0 if kind == 1 else acc

    def assemble(own, arrived, i):
        v = jnp.where(lefts[i], arrived.astype(F32), own.astype(F32))
        tmp[...] = v
        return tmp[pl.ds(0, 32, stride=2), :], tmp[pl.ds(1, 32, stride=2), :]

    recv("shift_a", rcv_a)
    for i in range(TRAJ):
        for step, v in enumerate(assemble(lat[slots[i]], rcv_a[i], i)):
            u = 2 * i + step
            xs[u // 3, (u % 3) * 32 : (u % 3) * 32 + 32, :] = v

    def spread(pair):
        return jnp.concatenate([pair[:, :64], pltpu.roll(pair, 64, 1)[:, :64]], axis=0)

    cp_up.wait()
    cp_dn.wait()

    def forward(s, carry):
        k = lax.rem(y + 2 + tri(s), NY)
        r0 = pl.multiple_of(k * CH, CH)
        emb[pl.ds(r0, CH), :] = jnp.dot(spread(xs[k]).astype(BF16), wpatch[...], preferred_element_type=F32)

        def norm(b, carry):
            rb = pl.multiple_of(r0 + b * 32, 32)
            u = k * 3 + lax.rem(b, 3)
            v = emb[pl.ds(rb, 32), :]
            v = v - jnp.mean(v, axis=-1, keepdims=True)
            i = lax.rsqrt(jnp.mean(v * v, axis=-1, keepdims=True) + EPS)
            modb[pl.ds(rb, 32), :] = (v * i * mod_c[pl.ds(u, 1), :] + mod_s[pl.ds(u, 1), :]).astype(BF16)
            return carry

        lax.fori_loop(0, 6, norm, 0)

        def up(n, carry):
            cols = pl.ds(pl.multiple_of(n * 512, 512), 512)
            pre = jnp.dot(modb[pl.ds(r0, CH), :], wup[:, cols], preferred_element_type=F32)
            sq = pre * pre
            th = jnp.tanh(GELU_K * (pre + GELU_C * (sq * pre)))
            half = 0.5 * (1.0 + th)
            act[pl.ds(r0, CH), cols] = (pre * half).astype(BF16)
            dg[pl.ds(r0, CH), cols] = half + (0.5 * GELU_K) * pre * (1.0 - th * th) * (1.0 + 3.0 * GELU_C * sq)
            return carry

        lax.fori_loop(0, 2, up, 0)

        def down(n, carry):
            q = pl.multiple_of(n * 768, 768)
            v = lax.dot_general(
                act[pl.ds(r0, CH), :], wdn[pl.ds(q, 768), :], (((1,), (1,)), ((), ())), preferred_element_type=F32
            )

            @pl.when(n == c)
            def _():
                pk[s, 0] = v[:, :384]
                pk[s, 1] = v[:, 384:]

            @pl.when(n != c)
            def _():
                dsend[s, 0] = v[:, :384].astype(BF16)
                dsend[s, 1] = v[:, 384:].astype(BF16)

            return carry

        lax.fori_loop(0, 2, down, 0)
        copy(d2d + s, dsend.at[s], drecv.at[s], dev(dc=1)).start()

        @pl.when(s == 1)
        def _():
            presum(0)
            ysend[0] = pk[0, 0].astype(BF16)
            ysend[1] = pk[0, 1].astype(BF16)
            copy("y1a", ysend.at[0], yrecv.at[0], dev(dy=1)).start()
            copy("y1b", ysend.at[1], yrecv.at[1], dev(dy=-1)).start()

        @pl.when(s == 2)
        def _():
            presum(1)
            ysend[2] = pk[1, 0].astype(BF16)
            copy("y2a", ysend.at[2], yrecv.at[2], dev(dy=-1)).start()

        @pl.when(s == 3)
        def _():
            presum(2)
            ysend[3] = pk[2, 1].astype(BF16)
            copy("y2b", ysend.at[3], yrecv.at[3], dev(dy=1)).start()
            recv("y1b", yrecv.at[1])
            ysend[4] = (pk[1, 1] + yrecv[1].astype(F32)).astype(BF16)
            copy("y3b", ysend.at[4], yrecv.at[4], dev(dy=-1)).start()
            recv("y1a", yrecv.at[0])
            ysend[5] = (pk[2, 0] + yrecv[0].astype(F32)).astype(BF16)
            copy("y3a", ysend.at[5], yrecv.at[5], dev(dy=1)).start()

        return carry

    d2d = mid("d2d0")
    for i in range(1, 4):
        mid(f"d2d{i}")

    def presum(s):
        recv(d2d + s, drecv.at[s])
        for h in range(2):
            pk[s, h] = pk[s, h] + drecv[s, h].astype(F32)

    lax.fori_loop(0, 4, forward, 0)
    for i in range(4):
        sent.append(copy(d2d + i, dsend.at[i], drecv.at[i], dev(dc=1)))
    for i, (n, t) in enumerate((("y1a", 1), ("y1b", -1), ("y2a", -1), ("y2b", 1), ("y3b", -1), ("y3a", 1))):
        sent.append(copy(n, ysend.at[i], yrecv.at[i], dev(dy=t)))

    for i in range(1, NX):
        recv(f"meta_x{i}", meta_all.at[z * NX + lax.rem(x + NX - i, NX)])
    for i in range(1, NZ):
        send(f"meta_z{i}", meta_all.at[pl.ds(z * NX, NX)], meta_all.at[pl.ds(z * NX, NX)], dev(dz=i))

    def transpose_pair(p, src, put):
        tok = pl.ds(pl.multiple_of(p * 384, 384), 384)
        for b in range(4):
            put(b, tok, src[tok, 384 * b : 384 * b + 384].T)

    def put_mod(b, tok, t):
        mod_t[2 * b, :, tok] = t[:192]
        mod_t[2 * b + 1, :, tok] = t[192:]

    def put_up(b, tok, t):
        for zz in range(2):
            for xx in range(NX):
                o = zz * 192 + xx * 48
                up_t[xx, (2 * b + zz) * 48 : (2 * b + zz) * 48 + 48, tok] = t[o : o + 48]

    def both(p, carry):
        transpose_pair(p, modb, put_mod)
        return carry

    presum(3)
    lax.fori_loop(0, 2, both, 0)

    q0 = 2 * c
    recv("y2a", yrecv.at[2])
    recv("y3a", yrecv.at[5])
    pfull[y, q0] = (pk[3, 0] + yrecv[2].astype(F32) + yrecv[5].astype(F32)).astype(BF16)
    send("g_up_a", pfull.at[y, q0], pfull.at[y, q0], dev(dy=1))
    recv("y2b", yrecv.at[3])
    recv("y3b", yrecv.at[4])
    pfull[y, q0 + 1] = (pk[3, 1] + yrecv[3].astype(F32) + yrecv[4].astype(F32)).astype(BF16)
    send("g_dn_b", pfull.at[y, q0 + 1], pfull.at[y, q0 + 1], dev(dy=-1))
    send("g_up_b", pfull.at[y, q0 + 1], pfull.at[y, q0 + 1], dev(dy=1))
    send("g_dn_a", pfull.at[y, q0], pfull.at[y, q0], dev(dy=-1))
    send("c_own", pfull.at[y, pl.ds(q0, 2)], pfull.at[y, pl.ds(q0, 2)], dev(dc=1))

    recv("shift_b", rcv_b)
    for i in range(TRAJ):
        for arr, which, dst in ((noi, 0, nz), (old, 1, od)):
            for step, v in enumerate(assemble(arr[slots[i]], rcv_b[which, i], i)):
                u = 2 * i + step
                dst[u // 3, (u % 3) * 32 : (u % 3) * 32 + 32, :] = v

    for i in range(1, NZ):
        recv(f"meta_z{i}", meta_all.at[pl.ds(lax.rem(z + NZ - i, NZ) * NX, NX)])
    for r in range(NZ * NX):
        meta_flat[r : r + 1, :] = meta_all[r, 0:1, :]
    ranks = meta_flat[...]
    hot = (lax.broadcasted_iota(I32, (NZ * NX, SURV), 0) == src_v[...]).astype(F32).astype(BF16)
    first = (((0,), (0,)), ((), ()))
    hi = lax.dot_general((ranks >> 4).astype(F32).astype(BF16), hot, first, preferred_element_type=F32)[:16]
    lo = lax.dot_general((ranks & 15).astype(F32).astype(BF16), hot, first, preferred_element_type=F32)[:16]
    by_slot = hi * 16.0 + lo
    rank = jnp.sum(
        jnp.where(lax.broadcasted_iota(I32, (16, SURV), 0) == slot_v[...], by_slot, 0.0), axis=0, keepdims=True
    )
    rank_i = rank.astype(I32)
    sq_i = rank_i * rank_i
    sq_hi, sq_lo = (sq_i >> 10).astype(F32), (sq_i & 1023).astype(F32)
    jdx = lax.broadcasted_iota(I32, (1, SURV), 1)

    def bounds(g, carry):
        end = carry[0] + cnt_s[g]
        out = [end]
        for i in range(TRAJ):
            hit = (lead + i >= carry[0]) & (lead + i < end)
            out += [jnp.where(hit, carry[0], carry[1 + 2 * i]), jnp.where(hit, end, carry[2 + 2 * i])]
        return tuple(out)

    ends = lax.fori_loop(0, 48, bounds, (jnp.int32(0),) * (1 + 2 * TRAJ))
    for i in range(TRAJ):
        lo_i, hi_i = ends[1 + 2 * i], ends[2 + 2 * i]
        inside = (jdx >= lo_i) & (jdx < hi_i)

        def total(v):
            return jnp.sum(jnp.where(inside, v, 0.0), axis=1, keepdims=True)

        s1 = total(rank)
        s1_i = s1.astype(I32)
        s2_i = total(sq_hi).astype(I32) * 1024 + total(sq_lo).astype(I32)
        n_i = jnp.full((1, 1), hi_i - lo_i, I32)
        n = n_i.astype(F32)
        r = jnp.sum(jnp.where(jdx == lead + i, rank, 0.0), axis=1, keepdims=True)
        dev_i = jnp.sqrt((n_i * s2_i - s1_i * s1_i).astype(F32)) / n
        a = (r - s1 / n) / jnp.maximum(dev_i, 1.0)
        adv_u[2 * i : 2 * i + 2, :] = jnp.broadcast_to(a, (2, 128))

    loss_own[...] = jnp.zeros((1, 128), F32)

    def head(k):
        r0 = pl.multiple_of(k * CH, CH)

        def mix(b, carry):
            o = pl.multiple_of(b * 32, 32)
            u = k * 3 + lax.rem(b, 3)
            proj = jnp.concatenate([pfull[k, q, pl.ds(o, 32), :] for q in range(4)], axis=1).astype(F32)
            v = emb[pl.ds(pl.multiple_of(r0 + o, 32), 32), :] + mod_g[pl.ds(u, 1), :] * proj
            v = v - jnp.mean(v, axis=-1, keepdims=True)
            i = lax.rsqrt(jnp.mean(v * v, axis=-1, keepdims=True) + EPS)
            v = v * i
            fin[pl.ds(o, 32), :] = v
            finb[pl.ds(o, 32), :] = v.astype(BF16)
            inv[pl.ds(o, 32), :] = jnp.broadcast_to(i, (32, 128))
            return carry

        lax.fori_loop(0, 6, mix, 0)
        velocity = lax.dot_general(finb[...], wv[...], (((1,), (1,)), ((), ())), preferred_element_type=F32)
        drawn, target = spread(nz[k]), spread(od[k])
        err = velocity - target
        dv = [None] * 6
        for j in range(3):
            u = k * 3 + j
            cu = coef_u[pl.ds(u, 1), :][:, :64]
            au = adv_u[pl.ds(u, 1), :][:, :1]
            part = jnp.zeros((32, 64), F32)
            for h in range(2):
                o = h * 96 + j * 32
                e, n = err[o : o + 32], drawn[o : o + 32]
                part = part + cu * n * e + 0.5 * cu * cu * e * e
            logratio = -jnp.sum(jnp.sum(part, axis=0, keepdims=True), axis=1, keepdims=True) * (1.0 / 4096)
            ratio = jnp.exp(logratio)
            plain = ratio * au
            bounded = jnp.clip(ratio, 0.8, 1.2) * au
            loss_own[...] += jnp.broadcast_to(-jnp.minimum(plain, bounded), (1, 128))
            slope = jnp.where(plain <= bounded, -au * ratio * (1.0 / (SURV * 2)), 0.0)
            for h in range(2):
                o = h * 96 + j * 32
                e, n = err[o : o + 32], drawn[o : o + 32]
                dv[h * 3 + j] = slope * (-(cu * n + cu * cu * e) * (1.0 / 4096))
        dvel = jnp.concatenate(dv, axis=0).astype(BF16)
        dfin = jnp.dot(dvel, wv[...], preferred_element_type=F32)
        pk[0, 0], pk[0, 1] = dfin[:, :384], dfin[:, 384:768]
        pk[1, 0], pk[1, 1] = dfin[:, 768:1152], dfin[:, 1152:]

        def back(b, carry):
            o = pl.multiple_of(b * 32, 32)
            u = k * 3 + lax.rem(b, 3)
            g = jnp.concatenate([pk[q // 2, q % 2, pl.ds(o, 32), :] for q in range(4)], axis=1)
            f = fin[pl.ds(o, 32), :]
            m1 = jnp.mean(g, axis=-1, keepdims=True)
            m2 = jnp.mean(g * f, axis=-1, keepdims=True)
            i = inv[pl.ds(o, 32), :][:, :1]
            ups[pl.ds(pl.multiple_of(r0 + o, 32), 32), :] = (
                mod_g[pl.ds(u, 1), :] * (i * (g - m1 - f * m2))
            ).astype(BF16)
            return carry

        lax.fori_loop(0, 6, back, 0)

    def dact(k):
        rows = pl.ds(pl.multiple_of(k * CH, CH), CH)

        def one(n, carry):
            cols = pl.ds(pl.multiple_of(n * 512, 512), 512)
            v = jnp.dot(ups[rows, :], wdn[:, cols], preferred_element_type=F32)
            dpre[rows, cols] = (v * dg[rows, cols]).astype(BF16)
            return carry

        lax.fori_loop(0, 2, one, 0)

    yu, yd, yo = (lax.rem(y + i, NY) for i in (1, 3, 2))
    p0 = 2 - 2 * c

    def fwd_core(name, k, q):
        copy(name, pfull.at[k, q], pfull.at[k, q], dev(dc=1)).start()

    def got(name, k, q):
        recv(name, pfull.at[k, q])

    def visit(h, carry):
        k = lax.rem(y + tri(h), NY)

        @pl.when(h == 0)
        def _():
            recv("c_own", pfull.at[y, pl.ds(p0, 2)])

        @pl.when(h == 1)
        def _():
            got("g_dn_a", yu, q0)
            fwd_core("c_ua", yu, q0)
            got("c_ua", yu, p0)
            got("c_ub", yu, p0 + 1)

        @pl.when(h == 2)
        def _():
            got("g_up_b", yd, q0 + 1)
            fwd_core("c_db", yd, q0 + 1)
            got("c_da", yd, p0)
            got("c_db", yd, p0 + 1)

        @pl.when(h == 3)
        def _():
            got("r_up", yo, q0)
            fwd_core("c_oa", yo, q0)
            got("r_dn", yo, q0 + 1)
            fwd_core("c_ob", yo, q0 + 1)
            got("c_oa", yo, p0)
            got("c_ob", yo, p0 + 1)

        head(k)

        @pl.when(h == 0)
        def _():
            got("g_up_a", yd, q0)
            copy("r_up", pfull.at[yd, q0], pfull.at[yd, q0], dev(dy=1)).start()
            fwd_core("c_da", yd, q0)
            got("g_dn_b", yu, q0 + 1)
            copy("r_dn", pfull.at[yu, q0 + 1], pfull.at[yu, q0 + 1], dev(dy=-1)).start()
            fwd_core("c_ub", yu, q0 + 1)

        dact(k)
        return carry

    lax.fori_loop(0, 4, visit, 0)
    sent.append(copy("r_up", pfull.at[yd, q0], pfull.at[yd, q0], dev(dy=1)))
    sent.append(copy("r_dn", pfull.at[yu, q0 + 1], pfull.at[yu, q0 + 1], dev(dy=-1)))
    for n, k, q in (("c_ua", yu, q0), ("c_ub", yu, q0 + 1), ("c_da", yd, q0), ("c_db", yd, q0 + 1),
                    ("c_oa", yo, q0), ("c_ob", yo, q0 + 1)):
        sent.append(copy(n, pfull.at[k, q], pfull.at[k, q], dev(dc=1)))

    def both_up(p, carry):
        transpose_pair(p, ups, put_up)
        return carry

    lax.fori_loop(0, 2, both_up, 0)

    def grad_dn(k):
        for h in range(2):
            gd[k, h] = jnp.dot(up_t[k], act[:, 512 * h : 512 * h + 512], preferred_element_type=F32).astype(BF16)

    def grad_up(k):
        for h in range(2):
            gu[k, h] = jnp.dot(mod_t[k], dpre[:, 512 * h : 512 * h + 512], preferred_element_type=F32).astype(BF16)

    def at(axis_pos, n, off):
        return lax.rem(axis_pos + (off + n), n)

    xsend = lambda name, off, h, to: copy(name, gd.at[at(x, NX, off), h], xr.at[xi[name]], dev(dx=to))
    xi = {"xa1": 0, "xb1": 1, "xa2": 2, "wb1": 3, "wa1": 4, "wb2": 5}
    xspec = {"xa1": (2, 0, 1), "xb1": (1, 1, 1), "xa2": (1, 0, 1), "wb1": (2, 1, -1), "wa1": (-1, 0, -1), "wb2": (-1, 1, -1)}

    def xgo(name):
        off, h, to = xspec[name]
        xsend(name, off, h, to).start()

    def dn_step(s, carry):
        grad_dn(lax.rem(x + 2 + tri(s), NX))

        @pl.when(s == 0)
        def _():
            xgo("xa1")
            xgo("wb1")

        @pl.when(s == 1)
        def _():
            xgo("wa1")

        @pl.when(s == 2)
        def _():
            xgo("xb1")

        return carry

    zi = {}
    zspec = {}
    for d, sign in (("r", 1), ("l", -1)):
        for h in range(2):
            far = (h == 0) == (sign == 1)
            for s in range(1, 5 if far else 4):
                off = sign * ((5 - s) if far else (4 - s))
                zi[f"z{d}{h}{s}"] = len(zi)
                zspec[f"z{d}{h}{s}"] = (off, h, sign)

    def zcopy(name):
        off, h, to = zspec[name]
        return copy(name, gu.at[at(z, NZ, off), h], zr.at[zi[name]], dev(dz=to))

    def up_step(t, off):
        grad_up(lax.rem(z + off, NZ))

        @pl.when(t == 0)
        def _():
            zcopy("zr01").start()
            zcopy("zl11").start()

        @pl.when(t == 1)
        def _():
            zcopy("zr11").start()

        @pl.when(t == 2)
        def _():
            zcopy("zl01").start()

        return off + (t + 1) * (2 * lax.rem(t, 2) - 1)

    lax.fori_loop(0, 4, dn_step, 0)
    lax.fori_loop(0, 8, up_step, 4)

    for i in range(1, NX):
        send(f"loss_x{i}", loss_own, loss_x.at[i], dev(dx=i))

    def zrelay(prev, name):
        off, h, _ = zspec[name]
        k = at(z, NZ, off)
        recv(prev, zr.at[zi[prev]])
        gu[k, h] = (gu[k, h].astype(F32) + zr[zi[prev]].astype(F32)).astype(BF16)
        zcopy(name).start()

    def xrelay(prev, name):
        off, h, to = xspec[name]
        k = at(x, NX, off)
        recv(prev, xr.at[xi[prev]])
        gd[k, h] = (gd[k, h].astype(F32) + xr[xi[prev]].astype(F32)).astype(BF16)
        xgo(name)

    zrelay("zr01", "zr02")
    zrelay("zl11", "zl12")
    zrelay("zr11", "zr12")
    zrelay("zl01", "zl02")
    xrelay("xa1", "xa2")
    xrelay("wb1", "wb2")
    lsum = loss_own[...]
    for i in range(1, NX):
        recv(f"loss_x{i}", loss_x.at[i])
        lsum = lsum + loss_x[i]
    loss_z[0] = lsum
    for i in range(1, NZ):
        send(f"loss_z{i}", loss_z.at[0], loss_z.at[i], dev(dz=i))
    zrelay("zr02", "zr03")
    zrelay("zl12", "zl13")
    zrelay("zr12", "zr13")
    zrelay("zl02", "zl03")
    zrelay("zr03", "zr04")
    zrelay("zl13", "zl14")

    def finish_x(h, names):
        v = gd[x, h].astype(F32)
        for n in names:
            recv(n, xr.at[xi[n]])
            v = v + xr[xi[n]].astype(F32)
        v = v.astype(BF16)
        for i in range(NZ):
            s2d[i, h] = v[48 * i : 48 * i + 48]

    def finish_z(h, names):
        v = gu[z, h].astype(F32)
        for n in names:
            recv(n, zr.at[zi[n]])
            v = v + zr[zi[n]].astype(F32)
        v = v.astype(BF16)
        for i in range(NX):
            s2u[i, h] = v[48 * i : 48 * i + 48]

    def dcopy(name):
        off, h, to = zspec[name]
        return copy("s" + name, s2d.at[at(z, NZ, off), h], s2dr.at[zi[name]], dev(dz=to))

    def drelay(prev, name):
        off, h, _ = zspec[name]
        k = at(z, NZ, off)
        recv("s" + prev, s2dr.at[zi[prev]])
        s2d[k, h] = (s2d[k, h].astype(F32) + s2dr[zi[prev]].astype(F32)).astype(BF16)
        dcopy(name).start()

    def ucopy(name):
        off, h, to = xspec[name]
        return copy("s" + name, s2u.at[at(x, NX, off), h], s2ur.at[xi[name]], dev(dx=to))

    def urelay(prev, name):
        off, h, _ = xspec[name]
        k = at(x, NX, off)
        recv("s" + prev, s2ur.at[xi[prev]])
        s2u[k, h] = (s2u[k, h].astype(F32) + s2ur[xi[prev]].astype(F32)).astype(BF16)
        ucopy(name).start()

    finish_x(0, ("xa2", "wa1"))
    dcopy("zr01").start()
    dcopy("zl01").start()
    finish_x(1, ("xb1", "wb2"))
    dcopy("zl11").start()
    dcopy("zr11").start()
    finish_z(1, ("zr13", "zl14"))
    ucopy("wb1").start()
    ucopy("xb1").start()
    finish_z(0, ("zr04", "zl03"))
    ucopy("xa1").start()
    ucopy("wa1").start()
    drelay("zr01", "zr02")
    drelay("zl01", "zl02")
    drelay("zl11", "zl12")
    drelay("zr11", "zr12")
    urelay("wb1", "wb2")
    urelay("xa1", "xa2")
    drelay("zr02", "zr03")
    drelay("zl02", "zl03")
    drelay("zl12", "zl13")
    drelay("zr12", "zr13")
    drelay("zr03", "zr04")
    drelay("zl13", "zl14")
    lsum = loss_z[0]
    for i in range(1, NZ):
        recv(f"loss_z{i}", loss_z.at[i])
        lsum = lsum + loss_z[i]
    out_loss[...] = lsum * (1.0 / (SURV * 2))
    for h, names in ((0, ("xa2", "wa1")), (1, ("xb1", "wb2"))):
        v = s2u[x, h].astype(F32)
        for n in names:
            recv("s" + n, s2ur.at[xi[n]])
            v = v + s2ur[xi[n]].astype(F32)
        out_up[:, 512 * h : 512 * h + 512] = v
    for h, names in ((0, ("zr04", "zl03")), (1, ("zr13", "zl14"))):
        v = s2d[z, h].astype(F32)
        for n in names:
            recv("s" + n, s2dr.at[zi[n]])
            v = v + s2dr[zi[n]].astype(F32)
        out_dn[:, 512 * h : 512 * h + 512] = v

    for n in xspec:
        sent.append(xsend(n, *xspec[n]))
        sent.append(ucopy(n))
    for n in zspec:
        sent.append(zcopy(n))
        sent.append(dcopy(n))
    for d in sent:
        d.wait_send()
    assert len(ids) <= NSEM, len(ids)


NSEM = 104


def shards(
    latents, noise, behavior_velocity, timestep, reward_rank_integer, surviving_source_index,
    surviving_slot_index, group_kept_count, patch_input_weight, modulation_lookup,
    up_projection_weight, down_projection_weight, velocity_head_weight,
):
    def pairs(a):
        return a.reshape(SLOTS, 2, 32, 128).transpose(0, 2, 1, 3).reshape(SLOTS, 64, 128)

    smem = pl.BlockSpec(memory_space=pltpu.SMEM)
    vmem = pl.BlockSpec(memory_space=pltpu.VMEM)
    hbm = pl.BlockSpec(memory_space=pl.ANY)
    V = pltpu.VMEM
    piece = (CH, 384)
    scratch = [
        V((8, 128), I32), V((D, HID), BF16), V((D, HID), BF16),
        V((TRAJ, 64, 128), BF16), V((2, TRAJ, 64, 128), BF16), V((TRAJ, 64, 128), BF16), V((2, TRAJ, 64, 128), BF16),
        V((8, 128), I32), V((NZ * NX, 8, 128), I32), V((NZ * NX, 128), I32), V((64, 128), F32),
        V((4, 96, 128), F32), V((4, 96, 128), F32), V((4, 96, 128), F32),
        V((16, D), F32), V((16, D), F32), V((16, D), F32), V((16, 128), F32), V((16, 128), F32),
        V((ROWS, D), F32), V((ROWS, D), BF16), V((ROWS, HID), BF16), V((ROWS, HID), F32), V((ROWS, HID), BF16),
        V((4, 2, *piece), BF16), V((4, 2, *piece), BF16), V((4, 2, *piece), F32),
        V((6, *piece), BF16), V((6, *piece), BF16), V((4, 4, *piece), BF16),
        V((CH, D), F32), V((CH, D), BF16), V((CH, 128), F32), V((ROWS, D), BF16),
        V((NZ, 192, ROWS), BF16), V((NX, 384, ROWS), BF16),
        V((NZ, 2, 192, 512), BF16), V((NX, 2, 384, 512), BF16), V((14, 192, 512), BF16), V((6, 384, 512), BF16),
        V((NX, 2, 48, 512), BF16), V((NZ, 2, 48, 512), BF16), V((6, 48, 512), BF16), V((14, 48, 512), BF16),
        V((1, 128), F32), V((NX, 1, 128), F32), V((NZ, 1, 128), F32),
        pltpu.SemaphoreType.DMA((2,)), pltpu.SemaphoreType.DMA((NSEM,)), pltpu.SemaphoreType.DMA((NSEM,)),
    ]
    up, dn, loss = pl.pallas_call(
        kernel,
        out_shape=(
            jax.ShapeDtypeStruct((48, HID), F32),
            jax.ShapeDtypeStruct((48, HID), F32),
            jax.ShapeDtypeStruct((1, 128), F32),
        ),
        in_specs=[smem] * 3 + [vmem] * 10 + [hbm] * 2,
        out_specs=(vmem,) * 3,
        scratch_shapes=scratch,
        compiler_params=pltpu.CompilerParams(collective_id=0, has_side_effects=True, vmem_limit_bytes=67043328),
    )(
        surviving_slot_index, surviving_source_index, group_kept_count,
        surviving_source_index.reshape(1, SURV), surviving_slot_index.reshape(1, SURV),
        pairs(latents), pairs(noise), pairs(behavior_velocity), reward_rank_integer.reshape(1, SLOTS), timestep.T,
        patch_input_weight, modulation_lookup, velocity_head_weight.T,
        up_projection_weight, down_projection_weight,
    )
    return up, dn, loss[0, 0]


def solution(mesh):
    finer = Mesh(mesh.devices.reshape(NZ, NX, NY, NC), ("z", "x", "y", "c"))
    dp, fs = ("z", "x"), ("y", "c")
    in_specs = (
        P(dp, None, None), P(dp, None, None), P(dp, None, None), P(dp, None), P(dp), P(), P(), P(), P(), P(),
        P(None, fs), P(None, fs), P(),
    )
    out_specs = (P(dp, fs), P(dp, fs), P())
    return jax.shard_map(shards, mesh=finer, in_specs=in_specs, out_specs=out_specs, check_vma=False)
```

```python
import jax
import jax.numpy as jnp
from jax import lax
from jax.experimental import pallas as pl
from jax.experimental.pallas import tpu as pltpu
from jax.sharding import Mesh
from jax.sharding import PartitionSpec as P

MESH = pl.DeviceIdType.MESH
F32, BF16, I32 = jnp.float32, jnp.bfloat16, jnp.int32
NZ, NX, NY, NC = 8, 4, 4, 2
D, HID, TRAJ, SLOTS = 1536, 1024, 6, 12
UNITS, ROWS, CH = 12, 768, 192
KSTEPS = 10
SURV = 192
EPS = 1e-06
GELU_K = 0.7978845608028654
GELU_C = 0.044715


def tri(s):
    return lax.rem(s * s * s, 5)


def kernel(
    slot_s, src_s, cnt_s, rank_v, time_v, src_h, slot_h, lat_h, noi_h, old_h, wpatch_h, modl_h, wv_h, wup_h, wdn_h,
    out_up, out_dn, out_loss,
    src_v, slot_v, lat, noi, old, wpatch, modl, wv, dfin_s, wdn_t, meta, wup, wdn, snd_a, snd_b, rcv_a, rcv_b, meta_l, meta_all, meta_flat, tmp, xs, nz, od,
    mod_s, mod_c, mod_g, coef_u, adv_u, emb, modb, act, dg, dpre, dsend, drecv, pk, ysend, yrecv, pfull,
    fin, finb, inv, ups, mod_t, up_t, gu, gd, zr, xr, s2u, s2d, s2ur, s2dr, loss_own, loss_x, loss_z,
    up_v, dn_v, loss_v, lsem, osem, ssem, rsem,
):
    z, x, y, c = (lax.axis_index(n) for n in ("z", "x", "y", "c"))
    owner = z * NX + x

    def dev(dz=0, dx=0, dy=0, dc=0):
        return (
            lax.rem(z + (dz + NZ), NZ),
            lax.rem(x + (dx + NX), NX),
            lax.rem(y + (dy + NY), NY),
            lax.rem(c + dc, NC),
        )

    nxt = lax.rem(owner + 1, NZ * NX)
    prv = lax.rem(owner + NZ * NX - 1, NZ * NX)
    next_dev = (nxt // NX, lax.rem(nxt, NX), y, c)
    prev_dev = (prv // NX, lax.rem(prv, NX), y, c)

    ids = {}

    def mid(name):
        return ids.setdefault(name, len(ids))

    sent = []

    def copy(name, src, dst, to):
        i = mid(name) if isinstance(name, str) else name
        return pltpu.make_async_remote_copy(
            src_ref=src, dst_ref=dst, send_sem=ssem.at[i], recv_sem=rsem.at[i],
            device_id=to, device_id_type=MESH,
        )

    def send(name, src, dst, to):
        d = copy(name, src, dst, to)
        d.start()
        sent.append(d)

    def recv(name, dst, to=None):
        copy(name, dst, dst, dev(dc=1) if to is None else to).wait_recv()

    barrier = pltpu.get_barrier_semaphore()
    peers = [dev(dx=2), dev(dx=1), dev(dx=-1), dev(dz=1), dev(dz=-1), dev(dy=1), dev(dy=-1), dev(dc=1), next_dev, prev_dev]
    for p in peers:
        pl.semaphore_signal(barrier, inc=1, device_id=p, device_id_type=MESH)
    pairs = (
        (lat_h, lat), (noi_h, noi), (old_h, old), (modl_h, modl), (wpatch_h, wpatch), (wdn_h, wdn), (wup_h, wup), (wv_h, wv),
        (src_h, src_v), (slot_h, slot_v),
    )
    loads = [pltpu.make_async_copy(a, b, lsem.at[i]) for i, (a, b) in enumerate(pairs)]
    for cp in loads:
        cp.start()
    meta[0:1, 0:SLOTS] = rank_v[...]
    meta[1:3, 0:SLOTS] = time_v[...]
    meta_all[z * NX + x] = meta[...]
    lead_n = jnp.minimum(owner + 1, NZ * NX - 1) * TRAJ
    lead = owner * TRAJ
    next_slots = [slot_s[lead_n + i] for i in range(TRAJ)]
    loads[0].wait()
    for i in range(TRAJ):
        snd_a[i] = lat[next_slots[i]]
    pl.semaphore_wait(barrier, len(peers))
    send("meta_l", meta, meta_l, next_dev)
    send("shift_a", snd_a, rcv_a, next_dev)
    loads[1].wait()
    loads[2].wait()
    for i in range(TRAJ):
        snd_b[0, i] = noi[next_slots[i]]
        snd_b[1, i] = old[next_slots[i]]
    send("shift_b", snd_b, rcv_b, next_dev)
    row_of = lambda d: z * NX + lax.rem(x + (d + NX), NX)
    block = lambda d: pl.ds(lax.rem(z + (d + NZ), NZ) * NX, NX)
    for d in (1, -1):
        send(f"meta_x{d}", meta, meta_all.at[row_of(0)], dev(dx=d))

    def meta_step(n):
        if n == 0:
            recv("meta_x1", meta_all.at[row_of(-1)])
            recv("meta_x-1", meta_all.at[row_of(1)])
            copy("meta_xx", meta_all.at[row_of(-1)], meta_all.at[row_of(-1)], dev(dx=1)).start()
            return
        if n == 1:
            recv("meta_xx", meta_all.at[row_of(-2)])
        for d in (1, -1):
            if n > 1 and (d == 1 or n < 5):
                recv(f"meta_z{d}_{n - 1}", meta_all.at[block(-d * (n - 1))])
            if n < 4 or (n == 4 and d == 1):
                b = block(-d * (n - 1))
                copy(f"meta_z{d}_{n}", meta_all.at[b], meta_all.at[b], dev(dz=d)).start()

    def meta_sent():
        sent.append(copy("meta_xx", meta_all.at[row_of(-1)], meta_all.at[row_of(-1)], dev(dx=1)))
        for d, last in ((1, 4), (-1, 3)):
            for n in range(1, last + 1):
                b = block(-d * (n - 1))
                sent.append(copy(f"meta_z{d}_{n}", meta_all.at[b], meta_all.at[b], dev(dz=d)))

    loads[5].wait()
    for b in range(4):
        wdn_t[:, 384 * b : 384 * b + 384] = wdn[384 * b : 384 * b + 384, :].T
    loads[3].wait()

    slots = [slot_s[lead + i] for i in range(TRAJ)]
    lefts = [src_s[lead + i] != owner for i in range(TRAJ)]

    sub = lax.broadcasted_iota(I32, (16, 128), 0)
    lane = lax.broadcasted_iota(I32, (16, 128), 1)
    pos = jnp.zeros((16, 128), I32)
    from_left = jnp.zeros((16, 128), I32)
    for i in range(TRAJ):
        mine = (sub >> 1) == i
        pos = pos + jnp.where(mine, slots[i], 0)
        from_left = from_left + jnp.where(mine, lefts[i].astype(I32), 0)
    recv("meta_l", meta_l)

    def step_row(n):
        wide = [jnp.broadcast_to(m[n : n + 1, :], (16, 128)) for m in (meta_l, meta)]
        return jnp.where(from_left == 1, wide[0], wide[1])

    row = jnp.where((sub & 1) == 0, step_row(1), step_row(2))
    stamp = jnp.sum(jnp.where(lane == pos, row.astype(F32), 0.0), axis=1, keepdims=True)
    level = 1.0 - stamp * (1.0 / KSTEPS)
    coef = jnp.sqrt((1.0 / KSTEPS) * (1.0 - level + (1.0 / KSTEPS)) / level) / 0.7
    coef_u[...] = jnp.broadcast_to(coef, (16, 128))
    for kind, dst in ((0, mod_s), (1, mod_c), (2, mod_g)):
        acc = jnp.zeros((16, D), F32)
        for t in range(KSTEPS):
            acc = jnp.where(stamp == float(t), jnp.broadcast_to(modl[t, pl.ds(kind, 1), :], (16, D)), acc)
        dst[...] = acc + 1.0 if kind == 1 else acc

    def assemble(own, arrived, i):
        v = jnp.where(lefts[i], arrived.astype(F32), own.astype(F32))
        tmp[...] = v
        return tmp[pl.ds(0, 32, stride=2), :], tmp[pl.ds(1, 32, stride=2), :]

    recv("shift_a", rcv_a)
    for i in range(TRAJ):
        for step, v in enumerate(assemble(lat[slots[i]], rcv_a[i], i)):
            u = 2 * i + step
            xs[u // 3, (u % 3) * 32 : (u % 3) * 32 + 32, :] = v

    def spread(pair):
        return jnp.concatenate([pair[:, :64], pltpu.roll(pair, 64, 1)[:, :64]], axis=0)

    for i in (4, 6, 7, 8, 9):
        loads[i].wait()

    chunk_of = [lax.rem(y + i, NY) for i in (2, 3, 1, 0)]

    def embed(s):
        k, r0 = chunk_of[s], s * CH
        emb[r0 : r0 + CH, :] = jnp.dot(spread(xs[k]).astype(BF16), wpatch[...], preferred_element_type=F32)

    def norm(s, blocks):
        for b in blocks:
            rb = s * CH + b * 16
            u = chunk_of[s] * 3 + (b % 6) // 2
            v = emb[rb : rb + 16, :]
            v = v - jnp.mean(v, axis=-1, keepdims=True)
            i = lax.rsqrt(jnp.mean(v * v, axis=-1, keepdims=True) + EPS)
            modb[rb : rb + 16, :] = (v * i * mod_c[pl.ds(u, 1), :] + mod_s[pl.ds(u, 1), :]).astype(BF16)

    def up(s, n):
        rows, cols = slice(s * CH, s * CH + CH), slice(256 * n, 256 * n + 256)
        pre = jnp.dot(modb[rows, :], wup[:, cols], preferred_element_type=F32)
        sq = pre * pre
        th = jnp.tanh(GELU_K * (pre + GELU_C * (sq * pre)))
        half = 0.5 * (1.0 + th)
        act[rows, cols] = (pre * half).astype(BF16)
        dg[rows, cols] = half + (0.5 * GELU_K) * pre * (1.0 - th * th) * (1.0 + 3.0 * GELU_C * sq)

    def down(s):
        rows = slice(s * CH, s * CH + CH)
        for j in range(2):
            q = pl.multiple_of((1 - c if j == 0 else c) * 768, 768)
            v = jnp.dot(act[rows, :], wdn_t[:, pl.ds(q, 768)], preferred_element_type=F32)
            for h in range(2):
                if j == 0:
                    dsend[s, h] = v[:, 384 * h : 384 * h + 384].astype(BF16)
                else:
                    pk[s, h] = v[:, 384 * h : 384 * h + 384]
            if j == 0:
                send(f"d2d{s}", dsend.at[s], drecv.at[s], dev(dc=1))

    def presum(s):
        recv(f"d2d{s}", drecv.at[s])
        for h in range(2):
            pk[s, h] = pk[s, h] + drecv[s, h].astype(F32)

    def ygo(name, i, v, d):
        ysend[i] = v.astype(BF16)
        send(name, ysend.at[i], yrecv.at[i], dev(dy=d))

    def yphase(s):
        if s == 1:
            presum(0)
            ygo("y1a", 0, pk[0, 0], 1)
            ygo("y1b", 1, pk[0, 1], -1)
        elif s == 2:
            presum(1)
            ygo("y2a", 2, pk[1, 0], -1)
        elif s == 3:
            presum(2)
            ygo("y2b", 3, pk[2, 1], 1)

    embed(0)
    norm(0, range(12))
    for s in range(4):
        if s < 3:
            embed(s + 1)
        for n in range(4):
            up(s, n)
            if s < 3:
                norm(s + 1, range(3 * n, 3 * n + 3))
        yphase(s)
        down(s)
        meta_step(s)
    recv("y1a", yrecv.at[0])
    ygo("y3a", 5, pk[2, 0] + yrecv[0].astype(F32), 1)
    recv("y1b", yrecv.at[1])
    ygo("y3b", 4, pk[1, 1] + yrecv[1].astype(F32), -1)

    def transpose_pair(p, src, put):
        tok = slice(p * 384, p * 384 + 384)
        for b in range(4):
            put(b, tok, src[tok, 384 * b : 384 * b + 384].T)

    def put_up(b, tok, t):
        up_t[2 * b, :, tok] = t[:192]
        up_t[2 * b + 1, :, tok] = t[192:]

    def put_mod(b, tok, t):
        for zz in range(2):
            for xx in range(NX):
                o = zz * 192 + xx * 48
                mod_t[xx, (2 * b + zz) * 48 : (2 * b + zz) * 48 + 48, tok] = t[o : o + 48]

    presum(3)
    for p in range(2):
        transpose_pair(p, modb, put_mod)

    q0 = 2 * c
    recv("y2a", yrecv.at[2])
    recv("y3a", yrecv.at[5])
    pfull[y, q0] = (pk[3, 0] + yrecv[2].astype(F32) + yrecv[5].astype(F32)).astype(BF16)
    send("g_up_a", pfull.at[y, q0], pfull.at[y, q0], dev(dy=1))
    recv("y2b", yrecv.at[3])
    recv("y3b", yrecv.at[4])
    pfull[y, q0 + 1] = (pk[3, 1] + yrecv[3].astype(F32) + yrecv[4].astype(F32)).astype(BF16)
    send("g_dn_b", pfull.at[y, q0 + 1], pfull.at[y, q0 + 1], dev(dy=-1))
    send("g_up_b", pfull.at[y, q0 + 1], pfull.at[y, q0 + 1], dev(dy=1))
    send("g_dn_a", pfull.at[y, q0], pfull.at[y, q0], dev(dy=-1))
    send("c_own", pfull.at[y, pl.ds(q0, 2)], pfull.at[y, pl.ds(q0, 2)], dev(dc=1))

    meta_step(4)
    recv("shift_b", rcv_b)
    for i in range(TRAJ):
        for arr, which, dst in ((noi, 0, nz), (old, 1, od)):
            for step, v in enumerate(assemble(arr[slots[i]], rcv_b[which, i], i)):
                u = 2 * i + step
                dst[u // 3, (u % 3) * 32 : (u % 3) * 32 + 32, :] = v

    meta_step(5)
    meta_sent()
    for r in range(NZ * NX):
        meta_flat[r : r + 1, :] = meta_all[r, 0:1, :]
    ranks = meta_flat[...]
    hot = (lax.broadcasted_iota(I32, (NZ * NX, SURV), 0) == src_v[...]).astype(F32).astype(BF16)
    first = (((0,), (0,)), ((), ()))
    hi = lax.dot_general((ranks >> 4).astype(F32).astype(BF16), hot, first, preferred_element_type=F32)[:16]
    lo = lax.dot_general((ranks & 15).astype(F32).astype(BF16), hot, first, preferred_element_type=F32)[:16]
    by_slot = hi * 16.0 + lo
    rank = jnp.sum(
        jnp.where(lax.broadcasted_iota(I32, (16, SURV), 0) == slot_v[...], by_slot, 0.0), axis=0, keepdims=True
    )
    rank_i = rank.astype(I32)
    sq_i = rank_i * rank_i
    sq_hi, sq_lo = (sq_i >> 10).astype(F32), (sq_i & 1023).astype(F32)
    jdx = lax.broadcasted_iota(I32, (1, SURV), 1)

    def bounds(g, carry):
        end = carry[0] + cnt_s[g]
        out = [end]
        for i in range(TRAJ):
            hit = (lead + i >= carry[0]) & (lead + i < end)
            out += [jnp.where(hit, carry[0], carry[1 + 2 * i]), jnp.where(hit, end, carry[2 + 2 * i])]
        return tuple(out)

    ends = lax.fori_loop(0, 48, bounds, (jnp.int32(0),) * (1 + 2 * TRAJ))
    for i in range(TRAJ):
        lo_i, hi_i = ends[1 + 2 * i], ends[2 + 2 * i]
        inside = (jdx >= lo_i) & (jdx < hi_i)

        def total(v):
            return jnp.sum(jnp.where(inside, v, 0.0), axis=1, keepdims=True)

        s1 = total(rank)
        s1_i = s1.astype(I32)
        s2_i = total(sq_hi).astype(I32) * 1024 + total(sq_lo).astype(I32)
        n_i = jnp.full((1, 1), hi_i - lo_i, I32)
        n = n_i.astype(F32)
        r = jnp.sum(jnp.where(jdx == lead + i, rank, 0.0), axis=1, keepdims=True)
        dev_i = jnp.sqrt((n_i * s2_i - s1_i * s1_i).astype(F32)) / n
        a = (r - s1 / n) / jnp.maximum(dev_i, 1.0)
        adv_u[2 * i : 2 * i + 2, :] = jnp.broadcast_to(a, (2, 128))

    loss_own[...] = jnp.zeros((1, 128), F32)

    def head(k, r0, behind):

        def mix(t, carry):
            for b in range(6):
                o = pl.multiple_of(t * 96 + b * 16, 16)
                u = k * 3 + b // 2
                proj = jnp.concatenate([pfull[k, q, pl.ds(o, 16), :] for q in range(4)], axis=1).astype(F32)
                v = emb[pl.ds(pl.multiple_of(r0 + o, 16), 16), :] + mod_g[pl.ds(u, 1), :] * proj
                v = v - jnp.mean(v, axis=-1, keepdims=True)
                i = lax.rsqrt(jnp.mean(v * v, axis=-1, keepdims=True) + EPS)
                v = v * i
                fin[pl.ds(o, 16), :] = v
                finb[pl.ds(o, 16), :] = v.astype(BF16)
                inv[pl.ds(o, 16), :] = jnp.broadcast_to(i, (16, 128))
            if behind is not None:
                dact(behind, pl.multiple_of(t * 512, 512))
            return carry

        lax.fori_loop(0, 2, mix, 0)
        velocity = lax.dot_general(finb[...], wv[...], (((1,), (1,)), ((), ())), preferred_element_type=F32)
        drawn, target = spread(nz[k]), spread(od[k])
        err = velocity - target
        dv = [None] * 6
        for j in range(3):
            u = k * 3 + j
            cu = coef_u[pl.ds(u, 1), :][:, :64]
            au = adv_u[pl.ds(u, 1), :][:, :1]
            part = jnp.zeros((32, 64), F32)
            for h in range(2):
                o = h * 96 + j * 32
                e, n = err[o : o + 32], drawn[o : o + 32]
                part = part + cu * n * e + 0.5 * cu * cu * e * e
            logratio = -jnp.sum(jnp.sum(part, axis=0, keepdims=True), axis=1, keepdims=True) * (1.0 / 4096)
            ratio = jnp.exp(logratio)
            plain = ratio * au
            bounded = jnp.clip(ratio, 0.8, 1.2) * au
            loss_own[...] += jnp.broadcast_to(-jnp.minimum(plain, bounded), (1, 128))
            slope = jnp.where(plain <= bounded, -au * ratio * (1.0 / (SURV * 2)), 0.0)
            for h in range(2):
                o = h * 96 + j * 32
                e, n = err[o : o + 32], drawn[o : o + 32]
                dv[h * 3 + j] = slope * (-(cu * n + cu * cu * e) * (1.0 / 4096))
        dvel = jnp.concatenate(dv, axis=0).astype(BF16)
        dfin = jnp.dot(dvel, wv[...], preferred_element_type=F32)
        dfin_s[...] = dfin

        def back(t, carry):
            for b in range(6):
                o = pl.multiple_of(t * 96 + b * 16, 16)
                u = k * 3 + b // 2
                g = dfin_s[pl.ds(o, 16), :]
                f = fin[pl.ds(o, 16), :]
                m1 = jnp.mean(g, axis=-1, keepdims=True)
                m2 = jnp.mean(g * f, axis=-1, keepdims=True)
                i = inv[pl.ds(o, 16), :][:, :1]
                ups[pl.ds(pl.multiple_of(r0 + o, 16), 16), :] = (
                    mod_g[pl.ds(u, 1), :] * (i * (g - m1 - f * m2))
                ).astype(BF16)
            return carry

        lax.fori_loop(0, 2, back, 0)

    def dact(r0, lo):
        rows, cols = slice(r0, r0 + CH), pl.ds(lo, 512)
        v = jnp.dot(ups[rows, :], wdn[:, cols], preferred_element_type=F32)
        dpre[rows, cols] = (v * dg[rows, cols]).astype(BF16)

    yu, yd, yo = (lax.rem(y + i, NY) for i in (1, 3, 2))
    p0 = 2 - 2 * c

    def fwd_core(name, k, q):
        send(name, pfull.at[k, q], pfull.at[k, q], dev(dc=1))

    def got(name, k, q):
        recv(name, pfull.at[k, q])

    recv("c_own", pfull.at[y, pl.ds(p0, 2)])
    head(y, 3 * CH, None)
    got("g_up_a", yd, q0)
    send("r_up", pfull.at[yd, q0], pfull.at[yd, q0], dev(dy=1))
    fwd_core("c_da", yd, q0)
    got("g_dn_b", yu, q0 + 1)
    send("r_dn", pfull.at[yu, q0 + 1], pfull.at[yu, q0 + 1], dev(dy=-1))
    fwd_core("c_ub", yu, q0 + 1)
    got("g_dn_a", yu, q0)
    fwd_core("c_ua", yu, q0)
    got("g_up_b", yd, q0 + 1)
    fwd_core("c_db", yd, q0 + 1)
    got("c_ua", yu, p0)
    got("c_ub", yu, p0 + 1)
    head(yu, 2 * CH, 3 * CH)
    got("r_up", yo, q0)
    fwd_core("c_oa", yo, q0)
    got("r_dn", yo, q0 + 1)
    fwd_core("c_ob", yo, q0 + 1)
    got("c_da", yd, p0)
    got("c_db", yd, p0 + 1)
    head(yd, CH, 2 * CH)
    transpose_pair(1, ups, put_up)
    got("c_oa", yo, p0)
    got("c_ob", yo, p0 + 1)
    head(yo, 0, CH)
    transpose_pair(0, ups, put_up)

    def grad_x(off):
        k = at(x, NX, off)
        for h in range(2):
            v = jnp.dot(mod_t[k], dpre[:, 512 * h : 512 * h + 512], preferred_element_type=F32).astype(BF16)
            gd[k, 2 * h], gd[k, 2 * h + 1] = v[:, :256], v[:, 256:]

    def grad_z(off):
        k = at(z, NZ, off)
        for h in range(2):
            v = jnp.dot(up_t[k], act[:, 512 * h : 512 * h + 512], preferred_element_type=F32).astype(BF16)
            gu[k, 2 * h], gu[k, 2 * h + 1] = v[:, :256], v[:, 256:]

    def at(axis_pos, n, off):
        return lax.rem(axis_pos + (off + n), n)

    def ring(n):
        spec = {}
        for d in (1, -1):
            for h in range(2):
                far = (h == 0) == (d == 1)
                last = n // 2 if far else n // 2 - 1
                for i in range(1, last + 1):
                    spec[d, h, i] = (d * (last + 1 - i), h, d)
        return spec, {m: i for i, m in enumerate(spec)}

    zspec, zi = ring(NZ)
    xspec, xi = ring(NX)

    class Stream:
        def __init__(self, tag, axis, buf, land):
            self.tag, self.axis, self.buf, self.land = tag, axis, buf, land
            self.spec, self.idx = (zspec, zi) if axis == "z" else (xspec, xi)
            self.pos, self.n = (z, NZ) if axis == "z" else (x, NX)

        def slot(self, b, m):
            return self.land.at[b * len(self.spec) + self.idx[m]]

        def go(self, b, *m):
            off, h, d = self.spec[m]
            to = dev(dz=d) if self.axis == "z" else dev(dx=d)
            send(f"{self.tag}{b}{m}", self.buf.at[at(self.pos, self.n, off), 2 * b + h], self.slot(b, m), to)

        def got(self, b, m):
            recv(f"{self.tag}{b}{m}", self.slot(b, m))
            return self.land[b * len(self.spec) + self.idx[m]].astype(F32)

        def relay(self, b, d, h, i):
            off = self.spec[d, h, i][0]
            k = at(self.pos, self.n, off)
            v = self.got(b, (d, h, i - 1))
            self.buf[k, 2 * b + h] = (self.buf[k, 2 * b + h].astype(F32) + v).astype(BF16)
            self.go(b, d, h, i)

        def far(self, b, i):
            self.relay(b, 1, 0, i)
            self.relay(b, -1, 1, i)

        def near(self, b, i):
            self.relay(b, 1, 1, i)
            self.relay(b, -1, 0, i)

        def total(self, b, h):
            v = self.buf[at(self.pos, self.n, 0), 2 * b + h].astype(F32)
            for d in (1, -1):
                last = max(i for e, g, i in self.spec if (e, g) == (d, h))
                v = v + self.got(b, (d, h, last))
            return v

        def first(self, b):
            self.go(b, 1, 0, 1)
            self.go(b, -1, 1, 1)

    Z1 = Stream("z", "z", gu, zr)
    X1 = Stream("x", "x", gd, xr)
    X2 = Stream("s", "z", s2d, s2dr)

    def finish_x(b):
        for h in range(2):
            v = X1.total(b, h).astype(BF16)
            for i in range(NZ):
                s2d[i, 2 * b + h] = v[48 * i : 48 * i + 48]
        X2.first(b)
        X2.go(b, 1, 1, 1)
        X2.go(b, -1, 0, 1)

    def hop(b, i):
        X2.far(b, i)
        if i < 4:
            X2.near(b, i)

    def done_x(b):
        for h in range(2):
            up_v[b, :, 256 * h : 256 * h + 256] = X2.total(b, h)
        store(f"up{b}", up_v.at[b], out_up.at[:, pl.ds(512 * b, 512)])

    def finish_z(b):
        for h in range(2):
            v = Z1.total(b, h).astype(BF16)
            for i in range(NX):
                s2u[b, i, :, 256 * h : 256 * h + 256] = v[48 * i : 48 * i + 48]
        for i in (2, 1, 3):
            send(f"t{b}{i}", s2u.at[b, at(x, NX, i)], s2ur.at[b, i], dev(dx=i))

    def done_z(b):
        v = s2u[b, x].astype(F32)
        for i in (1, 3, 2):
            recv(f"t{b}{i}", s2ur.at[b, i])
            v = v + s2ur[b, i].astype(F32)
        dn_v[b] = v
        store(f"dn{b}", dn_v.at[b], out_dn.at[:, pl.ds(512 * b, 512)])

    stores = []

    def store(name, src, dst):
        d = pltpu.make_async_copy(src, dst, osem.at[len(stores)])
        d.start()
        stores.append(d)

    def loss_step(n):
        if n == 0:
            for d in (1, -1):
                send(f"loss_x{d}", loss_own, loss_x.at[d % 4], dev(dx=d))
        elif n == 1:
            recv("loss_x1", loss_x.at[1])
            recv("loss_x-1", loss_x.at[3])
            send("loss_xx", loss_x.at[1], loss_x.at[2], dev(dx=1))
        elif n == 2:
            recv("loss_xx", loss_x.at[2])
            loss_z[0] = loss_own[...] + loss_x[1] + loss_x[2] + loss_x[3]
        if n >= 2:
            for d in (1, -1):
                if n > 2 and (d == 1 or n < 6):
                    recv(f"loss_z{d}_{n - 1}", loss_z.at[(d * (n - 2)) % NZ])
                if n < 5 or (n == 5 and d == 1):
                    send(f"loss_z{d}_{n}", loss_z.at[(d * (n - 2)) % NZ], loss_z.at[(d * (n - 1)) % NZ], dev(dz=d))

    grad_z(4)
    Z1.first(0)
    grad_z(3)
    Z1.go(0, 1, 1, 1)
    grad_z(-3)
    Z1.go(0, -1, 0, 1)
    for lo in (0, 512):
        dact(0, lo)
    grad_x(2)
    X1.first(0)
    Z1.first(1)
    loss_step(0)
    grad_x(-1)
    X1.go(0, -1, 0, 1)
    grad_x(1)
    X1.go(0, 1, 1, 1)
    Z1.far(0, 2)
    loss_step(1)
    grad_z(2)
    grad_z(-2)
    Z1.go(1, 1, 1, 1)
    Z1.go(1, -1, 0, 1)
    Z1.near(0, 2)
    X1.far(0, 2)
    grad_z(1)
    grad_z(-1)
    X1.first(1)
    loss_step(2)
    Z1.far(0, 3)
    grad_z(0)
    grad_x(0)
    Z1.far(1, 2)
    X1.go(1, 1, 1, 1)
    X1.go(1, -1, 0, 1)
    Z1.near(0, 3)
    loss_step(3)
    Z1.near(1, 2)
    Z1.far(0, 4)
    finish_x(0)
    X1.far(1, 2)
    loss_step(4)
    Z1.far(1, 3)
    hop(0, 2)
    finish_z(0)
    Z1.near(1, 3)
    loss_step(5)
    hop(0, 3)
    Z1.far(1, 4)
    finish_x(1)
    hop(0, 4)
    loss_step(6)
    v = loss_z[0]
    for i in range(1, NZ):
        v = v + loss_z[i]
    loss_v[...] = v * (1.0 / (SURV * 2))
    store("loss", loss_v, out_loss)
    hop(1, 2)
    done_x(0)
    done_z(0)
    finish_z(1)
    hop(1, 3)
    hop(1, 4)
    done_z(1)
    done_x(1)
    for d in stores:
        d.wait()
    for d in sent:
        d.wait_send()
    assert len(ids) <= NSEM, len(ids)


NSEM = 136


def shards(
    latents, noise, behavior_velocity, timestep, reward_rank_integer, surviving_source_index,
    surviving_slot_index, group_kept_count, patch_input_weight, modulation_lookup,
    up_projection_weight, down_projection_weight, velocity_head_weight,
):
    def pairs(a):
        return a.reshape(SLOTS, 2, 32, 128).transpose(0, 2, 1, 3).reshape(SLOTS, 64, 128)

    smem = pl.BlockSpec(memory_space=pltpu.SMEM)
    vmem = pl.BlockSpec(memory_space=pltpu.VMEM)
    hbm = pl.BlockSpec(memory_space=pl.ANY)
    V = pltpu.VMEM
    piece = (CH, 384)
    scratch = [
        V((1, SURV), I32), V((1, SURV), I32),
        V((SLOTS, 64, 128), BF16), V((SLOTS, 64, 128), BF16), V((SLOTS, 64, 128), BF16), V((64, D), BF16),
        V((KSTEPS, 3, D), F32), V((64, D), BF16), V((CH, D), F32), V((HID, D), BF16),
        V((8, 128), I32), V((D, HID), BF16), V((D, HID), BF16),
        V((TRAJ, 64, 128), BF16), V((2, TRAJ, 64, 128), BF16), V((TRAJ, 64, 128), BF16), V((2, TRAJ, 64, 128), BF16),
        V((8, 128), I32), V((NZ * NX, 8, 128), I32), V((NZ * NX, 128), I32), V((64, 128), F32),
        V((4, 96, 128), F32), V((4, 96, 128), F32), V((4, 96, 128), F32),
        V((16, D), F32), V((16, D), F32), V((16, D), F32), V((16, 128), F32), V((16, 128), F32),
        V((ROWS, D), F32), V((ROWS, D), BF16), V((ROWS, HID), BF16), V((ROWS, HID), F32), V((ROWS, HID), BF16),
        V((4, 2, *piece), BF16), V((4, 2, *piece), BF16), V((4, 2, *piece), F32),
        V((6, *piece), BF16), V((6, *piece), BF16), V((4, 4, *piece), BF16),
        V((CH, D), F32), V((CH, D), BF16), V((CH, 128), F32), V((ROWS, D), BF16),
        V((NX, 384, ROWS), BF16), V((NZ, 192, ROWS), BF16),
        V((NZ, 4, 192, 256), BF16), V((NX, 4, 384, 256), BF16), V((28, 192, 256), BF16), V((12, 384, 256), BF16),
        V((2, NX, 48, 512), BF16), V((NZ, 4, 48, 256), BF16), V((2, NX, 48, 512), BF16), V((28, 48, 256), BF16),
        V((1, 128), F32), V((NX, 1, 128), F32), V((NZ, 1, 128), F32),
        V((2, 48, 512), F32), V((2, 48, 512), F32), V((1, 128), F32),
        pltpu.SemaphoreType.DMA((10,)), pltpu.SemaphoreType.DMA((5,)), pltpu.SemaphoreType.DMA((NSEM,)), pltpu.SemaphoreType.DMA((NSEM,)),
    ]
    up, dn, loss = pl.pallas_call(
        kernel,
        out_shape=(
            jax.ShapeDtypeStruct((48, HID), F32),
            jax.ShapeDtypeStruct((48, HID), F32),
            jax.ShapeDtypeStruct((1, 128), F32),
        ),
        in_specs=[smem] * 3 + [vmem] * 2 + [hbm] * 10,
        out_specs=(hbm,) * 3,
        scratch_shapes=scratch,
        compiler_params=pltpu.CompilerParams(collective_id=0, has_side_effects=True, vmem_limit_bytes=67043328),
    )(
        surviving_slot_index, surviving_source_index, group_kept_count,
        reward_rank_integer.reshape(1, SLOTS), timestep.T,
        surviving_source_index.reshape(1, SURV), surviving_slot_index.reshape(1, SURV), pairs(latents), pairs(noise), pairs(behavior_velocity),
        patch_input_weight, modulation_lookup, velocity_head_weight.T,
        up_projection_weight, down_projection_weight,
    )
    return up, dn, loss[0, 0]


def solution(mesh):
    finer = Mesh(mesh.devices.reshape(NZ, NX, NY, NC), ("z", "x", "y", "c"))
    dp, fs = ("z", "x"), ("y", "c")
    in_specs = (
        P(dp, None, None), P(dp, None, None), P(dp, None, None), P(dp, None), P(dp), P(), P(), P(), P(), P(),
        P(None, fs), P(None, fs), P(),
    )
    out_specs = (P(dp, fs), P(dp, fs), P())
    return jax.shard_map(shards, mesh=finer, in_specs=in_specs, out_specs=out_specs, check_vma=False)
```

```python
import jax
import jax.numpy as jnp
from jax import lax
from jax.experimental import pallas as pl
from jax.experimental.pallas import tpu as pltpu
from jax.sharding import Mesh
from jax.sharding import PartitionSpec as P

MESH = pl.DeviceIdType.MESH
F32, BF16, I32 = jnp.float32, jnp.bfloat16, jnp.int32
NZ, NX, NY, NC = 8, 4, 4, 2
D, HID, TRAJ, SLOTS = 1536, 1024, 6, 12
UNITS, ROWS, CH = 12, 768, 192
KSTEPS = 10
SURV = 192
EPS = 1e-06
GELU_K = 0.7978845608028654
GELU_C = 0.044715


def tri(s):
    return lax.rem(s * s * s, 5)


def kernel(
    slot_s, src_s, cnt_s, rank_v, time_v, src_h, slot_h, lat_h, noi_h, old_h, wpatch_h, modl_h, wv_h, wup_h, wdn_h,
    out_up, out_dn, out_loss,
    src_v, slot_v, lat, noi, old, wpatch, modl, wv, dfin_s, wdn_t, meta, wup, wdn, snd_a, snd_b, rcv_a, rcv_b, meta_l, meta_all, meta_flat, tmp, xs, nz, od,
    mod_s, mod_c, mod_g, coef_u, adv_u, emb, modb, act, dg, dpre, dsend, drecv, pk, ysend, yrecv, pfull,
    fin, finb, inv, ups, mod_t, up_t, gu, gd, zr, xr, s2u, s2d, s2ur, s2dr, loss_own, loss_x, loss_z,
    up_v, dn_v, loss_v, lsem, osem, ssem, rsem,
):
    z, x, y, c = (lax.axis_index(n) for n in ("z", "x", "y", "c"))
    owner = z * NX + x

    def dev(dz=0, dx=0, dy=0, dc=0):
        return (
            lax.rem(z + (dz + NZ), NZ),
            lax.rem(x + (dx + NX), NX),
            lax.rem(y + (dy + NY), NY),
            lax.rem(c + dc, NC),
        )

    nxt = lax.rem(owner + 1, NZ * NX)
    prv = lax.rem(owner + NZ * NX - 1, NZ * NX)
    next_dev = (nxt // NX, lax.rem(nxt, NX), y, c)
    prev_dev = (prv // NX, lax.rem(prv, NX), y, c)

    ids = {}

    def mid(name):
        return ids.setdefault(name, len(ids))

    sent = []

    def copy(name, src, dst, to):
        i = mid(name) if isinstance(name, str) else name
        return pltpu.make_async_remote_copy(
            src_ref=src, dst_ref=dst, send_sem=ssem.at[i], recv_sem=rsem.at[i],
            device_id=to, device_id_type=MESH,
        )

    def send(name, src, dst, to):
        d = copy(name, src, dst, to)
        d.start()
        sent.append(d)

    def recv(name, dst, to=None):
        copy(name, dst, dst, dev(dc=1) if to is None else to).wait_recv()

    barrier = pltpu.get_barrier_semaphore()
    peers = [dev(dx=2), dev(dx=1), dev(dx=-1), dev(dz=1), dev(dz=-1), dev(dy=1), dev(dy=-1), dev(dc=1), next_dev, prev_dev]
    for p in peers:
        pl.semaphore_signal(barrier, inc=1, device_id=p, device_id_type=MESH)
    pairs = (
        (lat_h, lat), (noi_h, noi), (old_h, old), (modl_h, modl), (wpatch_h, wpatch), (wdn_h, wdn), (wup_h, wup), (wv_h, wv),
        (src_h, src_v), (slot_h, slot_v),
    )
    loads = [pltpu.make_async_copy(a, b, lsem.at[i]) for i, (a, b) in enumerate(pairs)]
    for cp in loads:
        cp.start()
    meta[0:1, 0:SLOTS] = rank_v[...]
    meta[1:3, 0:SLOTS] = time_v[...]
    meta_all[z * NX + x] = meta[...]
    lead_n = jnp.minimum(owner + 1, NZ * NX - 1) * TRAJ
    lead = owner * TRAJ
    next_slots = [slot_s[lead_n + i] for i in range(TRAJ)]
    loads[0].wait()
    for i in range(TRAJ):
        snd_a[i] = lat[next_slots[i]]
    pl.semaphore_wait(barrier, len(peers))
    send("meta_l", meta, meta_l, next_dev)
    send("shift_a", snd_a, rcv_a, next_dev)
    loads[1].wait()
    loads[2].wait()
    for i in range(TRAJ):
        snd_b[0, i] = noi[next_slots[i]]
        snd_b[1, i] = old[next_slots[i]]
    send("shift_b", snd_b, rcv_b, next_dev)
    row_of = lambda d: z * NX + lax.rem(x + (d + NX), NX)
    block = lambda d: pl.ds(lax.rem(z + (d + NZ), NZ) * NX, NX)
    for d in (1, -1):
        send(f"meta_x{d}", meta, meta_all.at[row_of(0)], dev(dx=d))

    def meta_step(n):
        if n == 0:
            recv("meta_x1", meta_all.at[row_of(-1)])
            recv("meta_x-1", meta_all.at[row_of(1)])
            copy("meta_xx", meta_all.at[row_of(-1)], meta_all.at[row_of(-1)], dev(dx=1)).start()
            return
        if n == 1:
            recv("meta_xx", meta_all.at[row_of(-2)])
        for d in (1, -1):
            if n > 1 and (d == 1 or n < 5):
                recv(f"meta_z{d}_{n - 1}", meta_all.at[block(-d * (n - 1))])
            if n < 4 or (n == 4 and d == 1):
                b = block(-d * (n - 1))
                copy(f"meta_z{d}_{n}", meta_all.at[b], meta_all.at[b], dev(dz=d)).start()

    def meta_sent():
        sent.append(copy("meta_xx", meta_all.at[row_of(-1)], meta_all.at[row_of(-1)], dev(dx=1)))
        for d, last in ((1, 4), (-1, 3)):
            for n in range(1, last + 1):
                b = block(-d * (n - 1))
                sent.append(copy(f"meta_z{d}_{n}", meta_all.at[b], meta_all.at[b], dev(dz=d)))

    loads[5].wait()
    for b in range(4):
        wdn_t[:, 384 * b : 384 * b + 384] = wdn[384 * b : 384 * b + 384, :].T
    loads[3].wait()

    slots = [slot_s[lead + i] for i in range(TRAJ)]
    lefts = [src_s[lead + i] != owner for i in range(TRAJ)]

    sub = lax.broadcasted_iota(I32, (16, 128), 0)
    lane = lax.broadcasted_iota(I32, (16, 128), 1)
    pos = jnp.zeros((16, 128), I32)
    from_left = jnp.zeros((16, 128), I32)
    for i in range(TRAJ):
        mine = (sub >> 1) == i
        pos = pos + jnp.where(mine, slots[i], 0)
        from_left = from_left + jnp.where(mine, lefts[i].astype(I32), 0)
    recv("meta_l", meta_l)

    def step_row(n):
        wide = [jnp.broadcast_to(m[n : n + 1, :], (16, 128)) for m in (meta_l, meta)]
        return jnp.where(from_left == 1, wide[0], wide[1])

    row = jnp.where((sub & 1) == 0, step_row(1), step_row(2))
    stamp = jnp.sum(jnp.where(lane == pos, row.astype(F32), 0.0), axis=1, keepdims=True)
    level = 1.0 - stamp * (1.0 / KSTEPS)
    coef = jnp.sqrt((1.0 / KSTEPS) * (1.0 - level + (1.0 / KSTEPS)) / level) / 0.7
    coef_u[...] = jnp.broadcast_to(coef, (16, 128))
    for kind, dst in ((0, mod_s), (1, mod_c), (2, mod_g)):
        acc = jnp.zeros((16, D), F32)
        for t in range(KSTEPS):
            acc = jnp.where(stamp == float(t), jnp.broadcast_to(modl[t, pl.ds(kind, 1), :], (16, D)), acc)
        dst[...] = acc + 1.0 if kind == 1 else acc

    def assemble(own, arrived, i):
        v = jnp.where(lefts[i], arrived.astype(F32), own.astype(F32))
        tmp[...] = v
        return tmp[pl.ds(0, 32, stride=2), :], tmp[pl.ds(1, 32, stride=2), :]

    recv("shift_a", rcv_a)
    for i in range(TRAJ):
        for step, v in enumerate(assemble(lat[slots[i]], rcv_a[i], i)):
            u = 2 * i + step
            xs[u // 3, (u % 3) * 32 : (u % 3) * 32 + 32, :] = v

    def spread(pair):
        return jnp.concatenate([pair[:, :64], pltpu.roll(pair, 64, 1)[:, :64]], axis=0)

    for i in (4, 6, 7, 8, 9):
        loads[i].wait()

    yu, yd, yo = (lax.rem(y + i, NY) for i in (1, 3, 2))
    held = ((yo, yo), (yd, yu), (yu, yd), (y, y))

    def embed(s):
        even, odd = (xs[k] for k in held[s])
        rows = jnp.concatenate([even[:, :64], pltpu.roll(odd, 64, 1)[:, :64]], axis=0)
        emb[s * CH : s * CH + CH, :] = jnp.dot(rows.astype(BF16), wpatch[...], preferred_element_type=F32)

    def norm(s, blocks):
        for b in blocks:
            rb = s * CH + b * 16
            u = held[s][b // 6] * 3 + (b % 6) // 2
            v = emb[rb : rb + 16, :]
            v = v - jnp.mean(v, axis=-1, keepdims=True)
            i = lax.rsqrt(jnp.mean(v * v, axis=-1, keepdims=True) + EPS)
            modb[rb : rb + 16, :] = (v * i * mod_c[pl.ds(u, 1), :] + mod_s[pl.ds(u, 1), :]).astype(BF16)

    def up(s, n):
        rows, cols = slice(s * CH, s * CH + CH), slice(256 * n, 256 * n + 256)
        pre = jnp.dot(modb[rows, :], wup[:, cols], preferred_element_type=F32)
        sq = pre * pre
        th = jnp.tanh(GELU_K * (pre + GELU_C * (sq * pre)))
        half = 0.5 * (1.0 + th)
        act[rows, cols] = (pre * half).astype(BF16)
        dg[rows, cols] = half + (0.5 * GELU_K) * pre * (1.0 - th * th) * (1.0 + 3.0 * GELU_C * sq)

    def down(s):
        rows = slice(s * CH, s * CH + CH)
        for j in range(2):
            q = pl.multiple_of((1 - c if j == 0 else c) * 768, 768)
            v = jnp.dot(act[rows, :], wdn_t[:, pl.ds(q, 768)], preferred_element_type=F32)
            for h in range(2):
                if j == 0:
                    dsend[s, h] = v[96 * h : 96 * h + 96].astype(BF16)
                else:
                    pk[s, h] = v[96 * h : 96 * h + 96]
            if j == 0:
                send(f"d2d{s}", dsend.at[s], drecv.at[s], dev(dc=1))

    def presum(s):
        recv(f"d2d{s}", drecv.at[s])
        for h in range(2):
            pk[s, h] = pk[s, h] + drecv[s, h].astype(F32)

    def ygo(name, i, v, d):
        ysend[i] = v.astype(BF16)
        send(name, ysend.at[i], yrecv.at[i], dev(dy=d))

    def yphase(s):
        if s == 1:
            presum(0)
            ygo("y1a", 0, pk[0, 0], 1)
            ygo("y1b", 1, pk[0, 1], -1)
        elif s == 2:
            presum(1)
            ygo("y2a", 2, pk[1, 0], -1)
            ygo("y2b", 3, pk[1, 1], 1)
        elif s == 3:
            presum(2)
            recv("y1a", yrecv.at[0])
            ygo("y3a", 5, pk[2, 0] + yrecv[0].astype(F32), 1)
            recv("y1b", yrecv.at[1])
            ygo("y3b", 4, pk[2, 1] + yrecv[1].astype(F32), -1)

    embed(0)
    norm(0, range(12))
    for s in range(4):
        if s < 3:
            embed(s + 1)
        for n in range(4):
            up(s, n)
            if s < 3:
                norm(s + 1, range(3 * n, 3 * n + 3))
        yphase(s)
        down(s)
        meta_step(s)
    def transpose_pair(p, src, put):
        tok = slice(p * 384, p * 384 + 384)
        for b in range(4):
            put(b, tok, src[tok, 384 * b : 384 * b + 384].T)

    def put_up(b, tok, t):
        up_t[2 * b, :, tok] = t[:192]
        up_t[2 * b + 1, :, tok] = t[192:]

    def put_mod(b, tok, t):
        for zz in range(2):
            for xx in range(NX):
                o = zz * 192 + xx * 48
                mod_t[xx, (2 * b + zz) * 48 : (2 * b + zz) * 48 + 48, tok] = t[o : o + 48]

    presum(3)
    for p in range(2):
        transpose_pair(p, modb, put_mod)

    part = lambda k, h: pfull.at[k, c, h]
    recv("y2a", yrecv.at[2])
    recv("y3a", yrecv.at[5])
    pfull[y, c, 0] = (pk[3, 0] + yrecv[2].astype(F32) + yrecv[5].astype(F32)).astype(BF16)
    send("g_up_a", part(y, 0), part(y, 0), dev(dy=1))
    recv("y2b", yrecv.at[3])
    recv("y3b", yrecv.at[4])
    pfull[y, c, 1] = (pk[3, 1] + yrecv[3].astype(F32) + yrecv[4].astype(F32)).astype(BF16)
    send("g_dn_b", part(y, 1), part(y, 1), dev(dy=-1))
    send("g_up_b", part(y, 1), part(y, 1), dev(dy=1))
    send("g_dn_a", part(y, 0), part(y, 0), dev(dy=-1))
    send("c_own", pfull.at[y, c], pfull.at[y, c], dev(dc=1))

    loss_own[...] = jnp.zeros((1, 128), F32)

    def mix(w, k, t, r0, behind=()):
        for b in range(6):
            o = t * 96 + b * 16
            u = k * 3 + b // 2
            proj = jnp.concatenate([pfull[k, q, t, b * 16 : b * 16 + 16, :] for q in range(2)], axis=1).astype(F32)
            v = emb[r0 + b * 16 : r0 + b * 16 + 16, :] + mod_g[pl.ds(u, 1), :] * proj
            v = v - jnp.mean(v, axis=-1, keepdims=True)
            i = lax.rsqrt(jnp.mean(v * v, axis=-1, keepdims=True) + EPS)
            v = v * i
            fin[w, o : o + 16, :] = v
            finb[w, o : o + 16, :] = v.astype(BF16)
            inv[w, o : o + 16, :] = jnp.broadcast_to(i, (16, 128))
        for slot, lo in behind:
            dact(slot * CH, lo)

    def rest(w, k, offs):
        velocity = lax.dot_general(finb[w], wv[...], (((1,), (1,)), ((), ())), preferred_element_type=F32)
        drawn, target = spread(nz[k]), spread(od[k])
        err = velocity - target
        dv = [None] * 6
        for j in range(3):
            u = k * 3 + j
            cu = coef_u[pl.ds(u, 1), :][:, :64]
            au = adv_u[pl.ds(u, 1), :][:, :1]
            part = jnp.zeros((32, 64), F32)
            for h in range(2):
                o = h * 96 + j * 32
                e, n = err[o : o + 32], drawn[o : o + 32]
                part = part + cu * n * e + 0.5 * cu * cu * e * e
            logratio = -jnp.sum(jnp.sum(part, axis=0, keepdims=True), axis=1, keepdims=True) * (1.0 / 4096)
            ratio = jnp.exp(logratio)
            plain = ratio * au
            bounded = jnp.clip(ratio, 0.8, 1.2) * au
            loss_own[...] += jnp.broadcast_to(-jnp.minimum(plain, bounded), (1, 128))
            slope = jnp.where(plain <= bounded, -au * ratio * (1.0 / (SURV * 2)), 0.0)
            for h in range(2):
                o = h * 96 + j * 32
                e, n = err[o : o + 32], drawn[o : o + 32]
                dv[h * 3 + j] = slope * (-(cu * n + cu * cu * e) * (1.0 / 4096))
        dvel = jnp.concatenate(dv, axis=0).astype(BF16)
        dfin = jnp.dot(dvel, wv[...], preferred_element_type=F32)
        dfin_s[...] = dfin

        for t in range(2):
            for b in range(6):
                o = t * 96 + b * 16
                u = k * 3 + b // 2
                g = dfin_s[o : o + 16, :]
                f = fin[w, o : o + 16, :]
                m1 = jnp.mean(g, axis=-1, keepdims=True)
                m2 = jnp.mean(g * f, axis=-1, keepdims=True)
                i = inv[w, o : o + 16, :][:, :1]
                r = offs[t] + b * 16
                ups[r : r + 16, :] = (mod_g[pl.ds(u, 1), :] * (i * (g - m1 - f * m2))).astype(BF16)

    def dact(r0, lo):
        rows, cols = slice(r0, r0 + CH), slice(lo, lo + 512)
        v = jnp.dot(ups[rows, :], wdn[:, cols], preferred_element_type=F32)
        dpre[rows, cols] = (v * dg[rows, cols]).astype(BF16)

    def fwd_core(name, k, h):
        send(name, part(k, h), part(k, h), dev(dc=1))

    def got(name, k, h):
        recv(name, part(k, h))

    def core(name, k, h):
        recv(name, pfull.at[k, 1 - c, h])

    recv("shift_b", rcv_b)
    for i in range(TRAJ):
        for arr, which, dst in ((noi, 0, nz), (old, 1, od)):
            for step, v in enumerate(assemble(arr[slots[i]], rcv_b[which, i], i)):
                u = 2 * i + step
                dst[u // 3, (u % 3) * 32 : (u % 3) * 32 + 32, :] = v

    recv("c_own", pfull.at[y, 1 - c])
    own = (3 * CH, 3 * CH + 96)
    for t in range(2):
        mix(0, y, t, own[t])
    meta_step(4)
    meta_step(5)
    meta_sent()
    for r in range(NZ * NX):
        meta_flat[r : r + 1, :] = meta_all[r, 0:1, :]
    ranks = meta_flat[...]
    hot = (lax.broadcasted_iota(I32, (NZ * NX, SURV), 0) == src_v[...]).astype(F32).astype(BF16)
    first = (((0,), (0,)), ((), ()))
    hi = lax.dot_general((ranks >> 4).astype(F32).astype(BF16), hot, first, preferred_element_type=F32)[:16]
    lo = lax.dot_general((ranks & 15).astype(F32).astype(BF16), hot, first, preferred_element_type=F32)[:16]
    by_slot = hi * 16.0 + lo
    rank = jnp.sum(
        jnp.where(lax.broadcasted_iota(I32, (16, SURV), 0) == slot_v[...], by_slot, 0.0), axis=0, keepdims=True
    )
    rank_i = rank.astype(I32)
    sq_i = rank_i * rank_i
    sq_hi, sq_lo = (sq_i >> 10).astype(F32), (sq_i & 1023).astype(F32)
    jdx = lax.broadcasted_iota(I32, (1, SURV), 1)

    def bounds(g, carry):
        end = carry[0] + cnt_s[g]
        out = [end]
        for i in range(TRAJ):
            hit = (lead + i >= carry[0]) & (lead + i < end)
            out += [jnp.where(hit, carry[0], carry[1 + 2 * i]), jnp.where(hit, end, carry[2 + 2 * i])]
        return tuple(out)

    ends = lax.fori_loop(0, 48, bounds, (jnp.int32(0),) * (1 + 2 * TRAJ))
    for i in range(TRAJ):
        lo_i, hi_i = ends[1 + 2 * i], ends[2 + 2 * i]
        inside = (jdx >= lo_i) & (jdx < hi_i)

        def total(v):
            return jnp.sum(jnp.where(inside, v, 0.0), axis=1, keepdims=True)

        s1 = total(rank)
        s1_i = s1.astype(I32)
        s2_i = total(sq_hi).astype(I32) * 1024 + total(sq_lo).astype(I32)
        n_i = jnp.full((1, 1), hi_i - lo_i, I32)
        n = n_i.astype(F32)
        r = jnp.sum(jnp.where(jdx == lead + i, rank, 0.0), axis=1, keepdims=True)
        dev_i = jnp.sqrt((n_i * s2_i - s1_i * s1_i).astype(F32)) / n
        a = (r - s1 / n) / jnp.maximum(dev_i, 1.0)
        adv_u[2 * i : 2 * i + 2, :] = jnp.broadcast_to(a, (2, 128))

    rest(0, y, own)
    got("g_up_a", yd, 0)
    send("r_up", part(yd, 0), part(yd, 0), dev(dy=1))
    fwd_core("c_da", yd, 0)
    got("g_dn_b", yu, 1)
    send("r_dn", part(yu, 1), part(yu, 1), dev(dy=-1))
    fwd_core("c_ub", yu, 1)
    core("c_da", yd, 0)
    core("c_ub", yu, 1)
    mix(0, yu, 1, CH + 96, [(3, 0)])
    mix(1, yd, 0, CH, [(3, 512)])
    got("g_dn_a", yu, 0)
    fwd_core("c_ua", yu, 0)
    got("g_up_b", yd, 1)
    fwd_core("c_db", yd, 1)
    core("c_ua", yu, 0)
    mix(0, yu, 0, 2 * CH)
    rest(0, yu, (2 * CH, CH + 96))
    core("c_db", yd, 1)
    mix(1, yd, 1, 2 * CH + 96)
    got("r_up", yo, 0)
    fwd_core("c_oa", yo, 0)
    got("r_dn", yo, 1)
    fwd_core("c_ob", yo, 1)
    rest(1, yd, (CH, 2 * CH + 96))
    transpose_pair(1, ups, put_up)
    core("c_oa", yo, 0)
    core("c_ob", yo, 1)
    mix(0, yo, 0, 0, [(1, 0), (1, 512)])
    mix(0, yo, 1, 96, [(2, 0), (2, 512)])
    rest(0, yo, (0, 96))
    transpose_pair(0, ups, put_up)

    def grad_x(off):
        k = at(x, NX, off)
        for h in range(2):
            v = jnp.dot(mod_t[k], dpre[:, 512 * h : 512 * h + 512], preferred_element_type=F32).astype(BF16)
            gd[k, 2 * h], gd[k, 2 * h + 1] = v[:, :256], v[:, 256:]

    def grad_z(off):
        k = at(z, NZ, off)
        for h in range(2):
            v = jnp.dot(up_t[k], act[:, 512 * h : 512 * h + 512], preferred_element_type=F32).astype(BF16)
            gu[k, 2 * h], gu[k, 2 * h + 1] = v[:, :256], v[:, 256:]

    def at(axis_pos, n, off):
        return lax.rem(axis_pos + (off + n), n)

    def ring(n):
        spec = {}
        for d in (1, -1):
            for h in range(2):
                far = (h == 0) == (d == 1)
                last = n // 2 if far else n // 2 - 1
                for i in range(1, last + 1):
                    spec[d, h, i] = (d * (last + 1 - i), h, d)
        return spec, {m: i for i, m in enumerate(spec)}

    zspec, zi = ring(NZ)
    xspec, xi = ring(NX)

    class Stream:
        def __init__(self, tag, axis, buf, land):
            self.tag, self.axis, self.buf, self.land = tag, axis, buf, land
            self.spec, self.idx = (zspec, zi) if axis == "z" else (xspec, xi)
            self.pos, self.n = (z, NZ) if axis == "z" else (x, NX)

        def slot(self, b, m):
            return self.land.at[b * len(self.spec) + self.idx[m]]

        def go(self, b, *m):
            off, h, d = self.spec[m]
            to = dev(dz=d) if self.axis == "z" else dev(dx=d)
            send(f"{self.tag}{b}{m}", self.buf.at[at(self.pos, self.n, off), 2 * b + h], self.slot(b, m), to)

        def got(self, b, m):
            recv(f"{self.tag}{b}{m}", self.slot(b, m))
            return self.land[b * len(self.spec) + self.idx[m]].astype(F32)

        def relay(self, b, d, h, i):
            off = self.spec[d, h, i][0]
            k = at(self.pos, self.n, off)
            v = self.got(b, (d, h, i - 1))
            self.buf[k, 2 * b + h] = (self.buf[k, 2 * b + h].astype(F32) + v).astype(BF16)
            self.go(b, d, h, i)

        def far(self, b, i):
            self.relay(b, 1, 0, i)
            self.relay(b, -1, 1, i)

        def near(self, b, i):
            self.relay(b, 1, 1, i)
            self.relay(b, -1, 0, i)

        def total(self, b, h):
            v = self.buf[at(self.pos, self.n, 0), 2 * b + h].astype(F32)
            for d in (1, -1):
                last = max(i for e, g, i in self.spec if (e, g) == (d, h))
                v = v + self.got(b, (d, h, last))
            return v

        def first(self, b):
            self.go(b, 1, 0, 1)
            self.go(b, -1, 1, 1)

    Z1 = Stream("z", "z", gu, zr)
    X1 = Stream("x", "x", gd, xr)
    X2 = Stream("s", "z", s2d, s2dr)

    def finish_x(b):
        for h in range(2):
            v = X1.total(b, h).astype(BF16)
            for i in range(NZ):
                s2d[i, 2 * b + h] = v[48 * i : 48 * i + 48]
        X2.first(b)
        X2.go(b, 1, 1, 1)
        X2.go(b, -1, 0, 1)

    def hop(b, i):
        X2.far(b, i)
        if i < 4:
            X2.near(b, i)

    def done_x(b):
        for h in range(2):
            up_v[b, :, 256 * h : 256 * h + 256] = X2.total(b, h)
        store(f"up{b}", up_v.at[b], out_up.at[:, pl.ds(512 * b, 512)])

    def finish_z(b):
        for h in range(2):
            v = Z1.total(b, h).astype(BF16)
            for i in range(NX):
                s2u[b, i, :, 256 * h : 256 * h + 256] = v[48 * i : 48 * i + 48]
        for i in (2, 1, 3):
            send(f"t{b}{i}", s2u.at[b, at(x, NX, i)], s2ur.at[b, i], dev(dx=i))

    def done_z(b):
        v = s2u[b, x].astype(F32)
        for i in (1, 3, 2):
            recv(f"t{b}{i}", s2ur.at[b, i])
            v = v + s2ur[b, i].astype(F32)
        dn_v[b] = v
        store(f"dn{b}", dn_v.at[b], out_dn.at[:, pl.ds(512 * b, 512)])

    stores = []

    def store(name, src, dst):
        d = pltpu.make_async_copy(src, dst, osem.at[len(stores)])
        d.start()
        stores.append(d)

    def loss_step(n):
        if n == 0:
            for d in (1, -1):
                send(f"loss_x{d}", loss_own, loss_x.at[d % 4], dev(dx=d))
        elif n == 1:
            recv("loss_x1", loss_x.at[1])
            recv("loss_x-1", loss_x.at[3])
            send("loss_xx", loss_x.at[1], loss_x.at[2], dev(dx=1))
        elif n == 2:
            recv("loss_xx", loss_x.at[2])
            loss_z[0] = loss_own[...] + loss_x[1] + loss_x[2] + loss_x[3]
        if n >= 2:
            for d in (1, -1):
                if n > 2 and (d == 1 or n < 6):
                    recv(f"loss_z{d}_{n - 1}", loss_z.at[(d * (n - 2)) % NZ])
                if n < 5 or (n == 5 and d == 1):
                    send(f"loss_z{d}_{n}", loss_z.at[(d * (n - 2)) % NZ], loss_z.at[(d * (n - 1)) % NZ], dev(dz=d))

    grad_z(4)
    Z1.first(0)
    Z1.first(1)
    for lo in (0, 512):
        dact(0, lo)
    grad_x(2)
    X1.first(0)
    grad_z(3)
    Z1.go(0, 1, 1, 1)
    Z1.go(1, 1, 1, 1)
    grad_z(-3)
    Z1.go(0, -1, 0, 1)
    Z1.go(1, -1, 0, 1)
    loss_step(0)
    grad_x(-1)
    X1.go(0, -1, 0, 1)
    grad_x(1)
    X1.go(0, 1, 1, 1)
    Z1.far(0, 2)
    grad_z(2)
    grad_z(-2)
    Z1.far(1, 2)
    grad_z(1)
    grad_z(-1)
    X1.first(1)
    Z1.near(0, 2)
    X1.far(0, 2)
    grad_z(0)
    grad_x(0)
    Z1.near(1, 2)
    loss_step(1)
    X1.go(1, 1, 1, 1)
    X1.go(1, -1, 0, 1)
    Z1.far(0, 3)
    Z1.far(1, 3)
    loss_step(2)
    Z1.near(0, 3)
    finish_x(0)
    Z1.near(1, 3)
    loss_step(3)
    X1.far(1, 2)
    Z1.far(0, 4)
    hop(0, 2)
    Z1.far(1, 4)
    loss_step(4)
    hop(0, 3)
    finish_x(1)
    finish_z(0)
    loss_step(5)
    hop(0, 4)
    hop(1, 2)
    finish_z(1)
    loss_step(6)
    v = loss_z[0]
    for i in range(1, NZ):
        v = v + loss_z[i]
    loss_v[...] = v * (1.0 / (SURV * 2))
    store("loss", loss_v, out_loss)
    done_x(0)
    hop(1, 3)
    done_z(0)
    hop(1, 4)
    done_z(1)
    done_x(1)
    for d in stores:
        d.wait()
    for d in sent:
        d.wait_send()
    assert len(ids) <= NSEM, len(ids)


NSEM = 136


def shards(
    latents, noise, behavior_velocity, timestep, reward_rank_integer, surviving_source_index,
    surviving_slot_index, group_kept_count, patch_input_weight, modulation_lookup,
    up_projection_weight, down_projection_weight, velocity_head_weight,
):
    def pairs(a):
        return a.reshape(SLOTS, 2, 32, 128).transpose(0, 2, 1, 3).reshape(SLOTS, 64, 128)

    smem = pl.BlockSpec(memory_space=pltpu.SMEM)
    vmem = pl.BlockSpec(memory_space=pltpu.VMEM)
    hbm = pl.BlockSpec(memory_space=pl.ANY)
    V = pltpu.VMEM
    piece = (CH // 2, 768)
    scratch = [
        V((1, SURV), I32), V((1, SURV), I32),
        V((SLOTS, 64, 128), BF16), V((SLOTS, 64, 128), BF16), V((SLOTS, 64, 128), BF16), V((64, D), BF16),
        V((KSTEPS, 3, D), F32), V((64, D), BF16), V((CH, D), F32), V((HID, D), BF16),
        V((8, 128), I32), V((D, HID), BF16), V((D, HID), BF16),
        V((TRAJ, 64, 128), BF16), V((2, TRAJ, 64, 128), BF16), V((TRAJ, 64, 128), BF16), V((2, TRAJ, 64, 128), BF16),
        V((8, 128), I32), V((NZ * NX, 8, 128), I32), V((NZ * NX, 128), I32), V((64, 128), F32),
        V((4, 96, 128), F32), V((4, 96, 128), F32), V((4, 96, 128), F32),
        V((16, D), F32), V((16, D), F32), V((16, D), F32), V((16, 128), F32), V((16, 128), F32),
        V((ROWS, D), F32), V((ROWS, D), BF16), V((ROWS, HID), BF16), V((ROWS, HID), F32), V((ROWS, HID), BF16),
        V((4, 2, *piece), BF16), V((4, 2, *piece), BF16), V((4, 2, *piece), F32),
        V((6, *piece), BF16), V((6, *piece), BF16), V((4, 2, 2, *piece), BF16),
        V((2, CH, D), F32), V((2, CH, D), BF16), V((2, CH, 128), F32), V((ROWS, D), BF16),
        V((NX, 384, ROWS), BF16), V((NZ, 192, ROWS), BF16),
        V((NZ, 4, 192, 256), BF16), V((NX, 4, 384, 256), BF16), V((28, 192, 256), BF16), V((12, 384, 256), BF16),
        V((2, NX, 48, 512), BF16), V((NZ, 4, 48, 256), BF16), V((2, NX, 48, 512), BF16), V((28, 48, 256), BF16),
        V((1, 128), F32), V((NX, 1, 128), F32), V((NZ, 1, 128), F32),
        V((2, 48, 512), F32), V((2, 48, 512), F32), V((1, 128), F32),
        pltpu.SemaphoreType.DMA((10,)), pltpu.SemaphoreType.DMA((5,)), pltpu.SemaphoreType.DMA((NSEM,)), pltpu.SemaphoreType.DMA((NSEM,)),
    ]
    up, dn, loss = pl.pallas_call(
        kernel,
        out_shape=(
            jax.ShapeDtypeStruct((48, HID), F32),
            jax.ShapeDtypeStruct((48, HID), F32),
            jax.ShapeDtypeStruct((1, 128), F32),
        ),
        in_specs=[smem] * 3 + [vmem] * 2 + [hbm] * 10,
        out_specs=(hbm,) * 3,
        scratch_shapes=scratch,
        compiler_params=pltpu.CompilerParams(collective_id=0, has_side_effects=True, vmem_limit_bytes=67043328),
    )(
        surviving_slot_index, surviving_source_index, group_kept_count,
        reward_rank_integer.reshape(1, SLOTS), timestep.T,
        surviving_source_index.reshape(1, SURV), surviving_slot_index.reshape(1, SURV), pairs(latents), pairs(noise), pairs(behavior_velocity),
        patch_input_weight, modulation_lookup, velocity_head_weight.T,
        up_projection_weight, down_projection_weight,
    )
    return up, dn, loss[0, 0]


def solution(mesh):
    finer = Mesh(mesh.devices.reshape(NZ, NX, NY, NC), ("z", "x", "y", "c"))
    dp, fs = ("z", "x"), ("y", "c")
    in_specs = (
        P(dp, None, None), P(dp, None, None), P(dp, None, None), P(dp, None), P(dp), P(), P(), P(), P(), P(),
        P(None, fs), P(None, fs), P(),
    )
    out_specs = (P(dp, fs), P(dp, fs), P())
    return jax.shard_map(shards, mesh=finer, in_specs=in_specs, out_specs=out_specs, check_vma=False)
```

```python
import jax
import jax.numpy as jnp
from jax import lax
from jax.experimental import pallas as pl
from jax.experimental.pallas import tpu as pltpu
from jax.sharding import Mesh
from jax.sharding import PartitionSpec as P

MESH = pl.DeviceIdType.MESH
F32, BF16, I32 = jnp.float32, jnp.bfloat16, jnp.int32
NZ, NX, NY, NC = 8, 4, 4, 2
D, HID, TRAJ, SLOTS = 1536, 1024, 6, 12
UNITS, ROWS, CH = 12, 768, 192
KSTEPS = 10
SURV = 192
EPS = 1e-06
GELU_K = 0.7978845608028654
GELU_C = 0.044715


def tri(s):
    return lax.rem(s * s * s, 5)


def kernel(
    slot_s, src_s, cnt_s, rank_v, time_v, src_h, slot_h, lat_h, noi_h, old_h, wpatch_h, modl_h, wv_h, wup_h, wdn_h,
    out, out_loss,
    src_v, slot_v, lat, noi, old, wpatch, modl, wv, dfin_s, wdn_t, meta, wup, wdn, snd_a, snd_b, rcv_a, rcv_b, meta_l, meta_all, meta_flat, tmp, xs, nz, od,
    mod_s, mod_c, mod_g, coef_u, adv_u, emb, modb, act, dg, dpre, dsend, drecv, pk, ysend, yrecv, pfull,
    fin, finb, inv, ups, mod_t, up_t, gu, gd, zr, xr, s2u, s2d, s2ur, s2dr, loss_own, loss_x, loss_z,
    up_v, dn_v, loss_v, lsem, osem, ssem, rsem,
):
    z, x, y, c = (lax.axis_index(n) for n in ("z", "x", "y", "c"))
    owner = z * NX + x

    def dev(dz=0, dx=0, dy=0, dc=0):
        return (
            lax.rem(z + (dz + NZ), NZ),
            lax.rem(x + (dx + NX), NX),
            lax.rem(y + (dy + NY), NY),
            lax.rem(c + dc, NC),
        )

    nxt = lax.rem(owner + 1, NZ * NX)
    prv = lax.rem(owner + NZ * NX - 1, NZ * NX)
    next_dev = (nxt // NX, lax.rem(nxt, NX), y, c)
    prev_dev = (prv // NX, lax.rem(prv, NX), y, c)

    ids = {}

    def mid(name):
        return ids.setdefault(name, len(ids))

    sent = []

    def copy(name, src, dst, to):
        i = mid(name) if isinstance(name, str) else name
        return pltpu.make_async_remote_copy(
            src_ref=src, dst_ref=dst, send_sem=ssem.at[i], recv_sem=rsem.at[i],
            device_id=to, device_id_type=MESH,
        )

    def send(name, src, dst, to):
        d = copy(name, src, dst, to)
        d.start()
        sent.append(d)

    def recv(name, dst, to=None):
        copy(name, dst, dst, dev(dc=1) if to is None else to).wait_recv()

    barrier = pltpu.get_barrier_semaphore()
    peers = [dev(dx=2), dev(dx=1), dev(dx=-1), dev(dz=1), dev(dz=-1), dev(dy=1), dev(dy=-1), dev(dc=1), next_dev, prev_dev]
    for p in peers:
        pl.semaphore_signal(barrier, inc=1, device_id=p, device_id_type=MESH)
    pairs = (
        (lat_h, lat), (noi_h, noi), (old_h, old), (modl_h, modl), (wpatch_h, wpatch), (wdn_h, wdn), (wup_h, wup), (wv_h, wv),
        (src_h, src_v), (slot_h, slot_v),
    )
    loads = [pltpu.make_async_copy(a, b, lsem.at[i]) for i, (a, b) in enumerate(pairs)]
    for cp in loads:
        cp.start()
    meta[0:1, 0:SLOTS] = rank_v[...]
    meta[1:3, 0:SLOTS] = time_v[...]
    meta_all[z * NX + x] = meta[...]
    lead_n = jnp.minimum(owner + 1, NZ * NX - 1) * TRAJ
    lead = owner * TRAJ
    next_slots = [slot_s[lead_n + i] for i in range(TRAJ)]
    loads[0].wait()
    for i in range(TRAJ):
        snd_a[i] = lat[next_slots[i]]
    pl.semaphore_wait(barrier, len(peers))
    send("meta_l", meta, meta_l, next_dev)
    send("shift_a", snd_a, rcv_a, next_dev)
    loads[1].wait()
    loads[2].wait()
    for i in range(TRAJ):
        snd_b[0, i] = noi[next_slots[i]]
        snd_b[1, i] = old[next_slots[i]]
    send("shift_b", snd_b, rcv_b, next_dev)
    row_of = lambda d: z * NX + lax.rem(x + (d + NX), NX)
    block = lambda d: pl.ds(lax.rem(z + (d + NZ), NZ) * NX, NX)
    for d in (1, -1):
        send(f"meta_x{d}", meta, meta_all.at[row_of(0)], dev(dx=d))

    def meta_step(n):
        if n == 0:
            recv("meta_x1", meta_all.at[row_of(-1)])
            recv("meta_x-1", meta_all.at[row_of(1)])
            copy("meta_xx", meta_all.at[row_of(-1)], meta_all.at[row_of(-1)], dev(dx=1)).start()
            return
        if n == 1:
            recv("meta_xx", meta_all.at[row_of(-2)])
        for d in (1, -1):
            if n > 1 and (d == 1 or n < 5):
                recv(f"meta_z{d}_{n - 1}", meta_all.at[block(-d * (n - 1))])
            if n < 4 or (n == 4 and d == 1):
                b = block(-d * (n - 1))
                copy(f"meta_z{d}_{n}", meta_all.at[b], meta_all.at[b], dev(dz=d)).start()

    def meta_sent():
        sent.append(copy("meta_xx", meta_all.at[row_of(-1)], meta_all.at[row_of(-1)], dev(dx=1)))
        for d, last in ((1, 4), (-1, 3)):
            for n in range(1, last + 1):
                b = block(-d * (n - 1))
                sent.append(copy(f"meta_z{d}_{n}", meta_all.at[b], meta_all.at[b], dev(dz=d)))

    loads[5].wait()
    for b in range(4):
        wdn_t[:, 384 * b : 384 * b + 384] = wdn[384 * b : 384 * b + 384, :].T
    loads[3].wait()

    slots = [slot_s[lead + i] for i in range(TRAJ)]
    lefts = [src_s[lead + i] != owner for i in range(TRAJ)]

    sub = lax.broadcasted_iota(I32, (16, 128), 0)
    lane = lax.broadcasted_iota(I32, (16, 128), 1)
    pos = jnp.zeros((16, 128), I32)
    from_left = jnp.zeros((16, 128), I32)
    for i in range(TRAJ):
        mine = (sub >> 1) == i
        pos = pos + jnp.where(mine, slots[i], 0)
        from_left = from_left + jnp.where(mine, lefts[i].astype(I32), 0)
    recv("meta_l", meta_l)

    def step_row(n):
        wide = [jnp.broadcast_to(m[n : n + 1, :], (16, 128)) for m in (meta_l, meta)]
        return jnp.where(from_left == 1, wide[0], wide[1])

    row = jnp.where((sub & 1) == 0, step_row(1), step_row(2))
    stamp = jnp.sum(jnp.where(lane == pos, row.astype(F32), 0.0), axis=1, keepdims=True)
    level = 1.0 - stamp * (1.0 / KSTEPS)
    coef = jnp.sqrt((1.0 / KSTEPS) * (1.0 - level + (1.0 / KSTEPS)) / level) / 0.7
    coef_u[...] = jnp.broadcast_to(coef, (16, 128))
    for kind, dst in ((0, mod_s), (1, mod_c), (2, mod_g)):
        acc = jnp.zeros((16, D), F32)
        for t in range(KSTEPS):
            acc = jnp.where(stamp == float(t), jnp.broadcast_to(modl[t, pl.ds(kind, 1), :], (16, D)), acc)
        dst[...] = acc + 1.0 if kind == 1 else acc

    def assemble(own, arrived, i):
        v = jnp.where(lefts[i], arrived.astype(F32), own.astype(F32))
        tmp[...] = v
        return tmp[pl.ds(0, 32, stride=2), :], tmp[pl.ds(1, 32, stride=2), :]

    recv("shift_a", rcv_a)
    for i in range(TRAJ):
        for step, v in enumerate(assemble(lat[slots[i]], rcv_a[i], i)):
            u = 2 * i + step
            xs[u // 3, (u % 3) * 32 : (u % 3) * 32 + 32, :] = v

    def spread(pair):
        return jnp.concatenate([pair[:, :64], pltpu.roll(pair, 64, 1)[:, :64]], axis=0)

    for i in (4, 6, 7, 8, 9):
        loads[i].wait()

    yu, yd, yo = (lax.rem(y + i, NY) for i in (1, 3, 2))
    held = ((yo, yo), (yd, yu), (yu, yd), (y, y))

    def embed(s):
        even, odd = (xs[k] for k in held[s])
        rows = jnp.concatenate([even[:, :64], pltpu.roll(odd, 64, 1)[:, :64]], axis=0)
        emb[s * CH : s * CH + CH, :] = jnp.dot(rows.astype(BF16), wpatch[...], preferred_element_type=F32)

    def norm(s, blocks):
        for b in blocks:
            rb = s * CH + b * 16
            u = held[s][b // 6] * 3 + (b % 6) // 2
            v = emb[rb : rb + 16, :]
            v = v - jnp.mean(v, axis=-1, keepdims=True)
            i = lax.rsqrt(jnp.mean(v * v, axis=-1, keepdims=True) + EPS)
            modb[rb : rb + 16, :] = (v * i * mod_c[pl.ds(u, 1), :] + mod_s[pl.ds(u, 1), :]).astype(BF16)

    def up(s, n):
        rows, cols = slice(s * CH, s * CH + CH), slice(256 * n, 256 * n + 256)
        pre = jnp.dot(modb[rows, :], wup[:, cols], preferred_element_type=F32)
        sq = pre * pre
        th = jnp.tanh(GELU_K * (pre + GELU_C * (sq * pre)))
        half = 0.5 * (1.0 + th)
        act[rows, cols] = (pre * half).astype(BF16)
        dg[rows, cols] = half + (0.5 * GELU_K) * pre * (1.0 - th * th) * (1.0 + 3.0 * GELU_C * sq)

    def down(s):
        rows = slice(s * CH, s * CH + CH)
        for j in range(2):
            q = pl.multiple_of((1 - c if j == 0 else c) * 768, 768)
            v = jnp.dot(act[rows, :], wdn_t[:, pl.ds(q, 768)], preferred_element_type=F32)
            for h in range(2):
                if j == 0:
                    dsend[s, h] = v[96 * h : 96 * h + 96].astype(BF16)
                else:
                    pk[s, h] = v[96 * h : 96 * h + 96]
            if j == 0:
                send(f"d2d{s}", dsend.at[s], drecv.at[s], dev(dc=1))

    def presum(s):
        recv(f"d2d{s}", drecv.at[s])
        for h in range(2):
            pk[s, h] = pk[s, h] + drecv[s, h].astype(F32)

    def ygo(name, i, v, d):
        ysend[i] = v.astype(BF16)
        send(name, ysend.at[i], yrecv.at[i], dev(dy=d))

    def yphase(s):
        if s == 1:
            presum(0)
            ygo("y1a", 0, pk[0, 0], 1)
            ygo("y1b", 1, pk[0, 1], -1)
        elif s == 2:
            presum(1)
            ygo("y2a", 2, pk[1, 0], -1)
            ygo("y2b", 3, pk[1, 1], 1)
        elif s == 3:
            presum(2)
            recv("y1a", yrecv.at[0])
            ygo("y3a", 5, pk[2, 0] + yrecv[0].astype(F32), 1)
            recv("y1b", yrecv.at[1])
            ygo("y3b", 4, pk[2, 1] + yrecv[1].astype(F32), -1)

    embed(0)
    norm(0, range(12))
    for s in range(4):
        if s < 3:
            embed(s + 1)
        for n in range(4):
            up(s, n)
            if s < 3:
                norm(s + 1, range(3 * n, 3 * n + 3))
        yphase(s)
        down(s)
        meta_step(s)
    def transpose_pair(p, src, put):
        tok = slice(p * 384, p * 384 + 384)
        for b in range(4):
            put(b, tok, src[tok, 384 * b : 384 * b + 384].T)

    def put_up(b, tok, t):
        up_t[2 * b, :, tok] = t[:192]
        up_t[2 * b + 1, :, tok] = t[192:]

    def put_mod(b, tok, t):
        for zz in range(2):
            for xx in range(NX):
                o = zz * 192 + xx * 48
                mod_t[xx, (2 * b + zz) * 48 : (2 * b + zz) * 48 + 48, tok] = t[o : o + 48]

    presum(3)
    part = lambda k, h: pfull.at[k, c, h]
    recv("y2a", yrecv.at[2])
    recv("y3a", yrecv.at[5])
    pfull[y, c, 0] = (pk[3, 0] + yrecv[2].astype(F32) + yrecv[5].astype(F32)).astype(BF16)
    send("g_up_a", part(y, 0), part(y, 0), dev(dy=1))
    recv("y2b", yrecv.at[3])
    recv("y3b", yrecv.at[4])
    pfull[y, c, 1] = (pk[3, 1] + yrecv[3].astype(F32) + yrecv[4].astype(F32)).astype(BF16)
    send("g_dn_b", part(y, 1), part(y, 1), dev(dy=-1))
    send("g_up_b", part(y, 1), part(y, 1), dev(dy=1))
    send("g_dn_a", part(y, 0), part(y, 0), dev(dy=-1))
    send("c_own", pfull.at[y, c], pfull.at[y, c], dev(dc=1))

    loss_own[...] = jnp.zeros((1, 128), F32)

    def mix(w, k, t, r0, behind=()):
        for b in range(6):
            o = t * 96 + b * 16
            u = k * 3 + b // 2
            proj = jnp.concatenate([pfull[k, q, t, b * 16 : b * 16 + 16, :] for q in range(2)], axis=1).astype(F32)
            v = emb[r0 + b * 16 : r0 + b * 16 + 16, :] + mod_g[pl.ds(u, 1), :] * proj
            v = v - jnp.mean(v, axis=-1, keepdims=True)
            i = lax.rsqrt(jnp.mean(v * v, axis=-1, keepdims=True) + EPS)
            v = v * i
            fin[w, o : o + 16, :] = v
            finb[w, o : o + 16, :] = v.astype(BF16)
            inv[w, o : o + 16, :] = jnp.broadcast_to(i, (16, 128))
        for slot, lo in behind:
            dact(slot * CH, lo)

    def rest(w, k, offs):
        velocity = lax.dot_general(finb[w], wv[...], (((1,), (1,)), ((), ())), preferred_element_type=F32)
        drawn, target = spread(nz[k]), spread(od[k])
        err = velocity - target
        dv = [None] * 6
        for j in range(3):
            u = k * 3 + j
            cu = coef_u[pl.ds(u, 1), :][:, :64]
            au = adv_u[pl.ds(u, 1), :][:, :1]
            part = jnp.zeros((32, 64), F32)
            for h in range(2):
                o = h * 96 + j * 32
                e, n = err[o : o + 32], drawn[o : o + 32]
                part = part + cu * n * e + 0.5 * cu * cu * e * e
            logratio = -jnp.sum(jnp.sum(part, axis=0, keepdims=True), axis=1, keepdims=True) * (1.0 / 4096)
            ratio = jnp.exp(logratio)
            plain = ratio * au
            bounded = jnp.clip(ratio, 0.8, 1.2) * au
            loss_own[...] += jnp.broadcast_to(-jnp.minimum(plain, bounded), (1, 128))
            slope = jnp.where(plain <= bounded, -au * ratio * (1.0 / (SURV * 2)), 0.0)
            for h in range(2):
                o = h * 96 + j * 32
                e, n = err[o : o + 32], drawn[o : o + 32]
                dv[h * 3 + j] = slope * (-(cu * n + cu * cu * e) * (1.0 / 4096))
        dvel = jnp.concatenate(dv, axis=0).astype(BF16)
        dfin = jnp.dot(dvel, wv[...], preferred_element_type=F32)
        dfin_s[...] = dfin

        for t in range(2):
            for b in range(6):
                o = t * 96 + b * 16
                u = k * 3 + b // 2
                g = dfin_s[o : o + 16, :]
                f = fin[w, o : o + 16, :]
                m1 = jnp.mean(g, axis=-1, keepdims=True)
                m2 = jnp.mean(g * f, axis=-1, keepdims=True)
                i = inv[w, o : o + 16, :][:, :1]
                r = offs[t] + b * 16
                ups[r : r + 16, :] = (mod_g[pl.ds(u, 1), :] * (i * (g - m1 - f * m2))).astype(BF16)

    def dact(r0, lo):
        rows, cols = slice(r0, r0 + CH), slice(lo, lo + 512)
        v = jnp.dot(ups[rows, :], wdn[:, cols], preferred_element_type=F32)
        dpre[rows, cols] = (v * dg[rows, cols]).astype(BF16)

    def fwd_core(name, k, h):
        send(name, part(k, h), part(k, h), dev(dc=1))

    def got(name, k, h):
        recv(name, part(k, h))

    def core(name, k, h):
        recv(name, pfull.at[k, 1 - c, h])

    recv("shift_b", rcv_b)
    for i in range(TRAJ):
        for arr, which, dst in ((noi, 0, nz), (old, 1, od)):
            for step, v in enumerate(assemble(arr[slots[i]], rcv_b[which, i], i)):
                u = 2 * i + step
                dst[u // 3, (u % 3) * 32 : (u % 3) * 32 + 32, :] = v

    meta_step(4)

    def bounds(g, carry):
        end = carry[0] + cnt_s[g]
        out = [end]
        for i in range(TRAJ):
            hit = (lead + i >= carry[0]) & (lead + i < end)
            out += [jnp.where(hit, carry[0], carry[1 + 2 * i]), jnp.where(hit, end, carry[2 + 2 * i])]
        return tuple(out)

    ends = lax.fori_loop(0, 48, bounds, (jnp.int32(0),) * (1 + 2 * TRAJ))
    recv("c_own", pfull.at[y, 1 - c])
    own = (3 * CH, 3 * CH + 96)
    for t in range(2):
        mix(0, y, t, own[t])
    meta_step(5)
    meta_sent()
    for r in range(NZ * NX):
        meta_flat[r : r + 1, :] = meta_all[r, 0:1, :]
    ranks = meta_flat[...]
    hot = (lax.broadcasted_iota(I32, (NZ * NX, SURV), 0) == src_v[...]).astype(F32).astype(BF16)
    first = (((0,), (0,)), ((), ()))
    hi = lax.dot_general((ranks >> 4).astype(F32).astype(BF16), hot, first, preferred_element_type=F32)[:16]
    lo = lax.dot_general((ranks & 15).astype(F32).astype(BF16), hot, first, preferred_element_type=F32)[:16]
    by_slot = hi * 16.0 + lo
    rank = jnp.sum(
        jnp.where(lax.broadcasted_iota(I32, (16, SURV), 0) == slot_v[...], by_slot, 0.0), axis=0, keepdims=True
    )
    rank_i = rank.astype(I32)
    sq_i = rank_i * rank_i
    sq_hi, sq_lo = (sq_i >> 10).astype(F32), (sq_i & 1023).astype(F32)
    jdx = lax.broadcasted_iota(I32, (1, SURV), 1)

    for i in range(TRAJ):
        lo_i, hi_i = ends[1 + 2 * i], ends[2 + 2 * i]
        inside = (jdx >= lo_i) & (jdx < hi_i)

        def total(v):
            return jnp.sum(jnp.where(inside, v, 0.0), axis=1, keepdims=True)

        s1 = total(rank)
        s1_i = s1.astype(I32)
        s2_i = total(sq_hi).astype(I32) * 1024 + total(sq_lo).astype(I32)
        n_i = jnp.full((1, 1), hi_i - lo_i, I32)
        n = n_i.astype(F32)
        r = jnp.sum(jnp.where(jdx == lead + i, rank, 0.0), axis=1, keepdims=True)
        dev_i = jnp.sqrt((n_i * s2_i - s1_i * s1_i).astype(F32)) / n
        a = (r - s1 / n) / jnp.maximum(dev_i, 1.0)
        adv_u[2 * i : 2 * i + 2, :] = jnp.broadcast_to(a, (2, 128))

    got("g_up_a", yd, 0)
    send("r_up", part(yd, 0), part(yd, 0), dev(dy=1))
    fwd_core("c_da", yd, 0)
    got("g_dn_b", yu, 1)
    send("r_dn", part(yu, 1), part(yu, 1), dev(dy=-1))
    fwd_core("c_ub", yu, 1)
    rest(0, y, own)
    for p in range(2):
        transpose_pair(p, modb, put_mod)

    core("c_da", yd, 0)
    core("c_ub", yu, 1)
    mix(0, yu, 1, CH + 96, [(3, 0)])
    mix(1, yd, 0, CH, [(3, 512)])
    got("g_dn_a", yu, 0)
    fwd_core("c_ua", yu, 0)
    got("g_up_b", yd, 1)
    fwd_core("c_db", yd, 1)
    core("c_ua", yu, 0)
    mix(0, yu, 0, 2 * CH)
    rest(0, yu, (2 * CH, CH + 96))
    core("c_db", yd, 1)
    mix(1, yd, 1, 2 * CH + 96)
    got("r_up", yo, 0)
    fwd_core("c_oa", yo, 0)
    got("r_dn", yo, 1)
    fwd_core("c_ob", yo, 1)
    rest(1, yd, (CH, 2 * CH + 96))
    transpose_pair(1, ups, put_up)
    core("c_oa", yo, 0)
    core("c_ob", yo, 1)
    mix(0, yo, 0, 0, [(1, 0), (1, 512)])
    mix(0, yo, 1, 96, [(2, 0), (2, 512)])
    rest(0, yo, (0, 96))
    transpose_pair(0, ups, put_up)

    def grad_x(off, b):
        k = at(x, NX, off)
        v = jnp.dot(mod_t[k], dpre[:, 512 * b : 512 * b + 512], preferred_element_type=F32).astype(BF16)
        gd[k, 2 * b], gd[k, 2 * b + 1] = v[:, :256], v[:, 256:]

    def grad_z(off, b):
        k = at(z, NZ, off)
        v = jnp.dot(up_t[k], act[:, 512 * b : 512 * b + 512], preferred_element_type=F32).astype(BF16)
        gu[k, 2 * b], gu[k, 2 * b + 1] = v[:, :256], v[:, 256:]

    def at(axis_pos, n, off):
        return lax.rem(axis_pos + (off + n), n)

    def ring(n):
        spec = {}
        for d in (1, -1):
            for h in range(2):
                far = (h == 0) == (d == 1)
                last = n // 2 if far else n // 2 - 1
                for i in range(1, last + 1):
                    spec[d, h, i] = (d * (last + 1 - i), h, d)
        return spec, {m: i for i, m in enumerate(spec)}

    zspec, zi = ring(NZ)
    xspec, xi = ring(NX)

    class Stream:
        def __init__(self, tag, axis, buf, land):
            self.tag, self.axis, self.buf, self.land = tag, axis, buf, land
            self.spec, self.idx = (zspec, zi) if axis == "z" else (xspec, xi)
            self.pos, self.n = (z, NZ) if axis == "z" else (x, NX)

        def slot(self, b, m):
            return self.land.at[b * len(self.spec) + self.idx[m]]

        def go(self, b, *m):
            off, h, d = self.spec[m]
            to = dev(dz=d) if self.axis == "z" else dev(dx=d)
            send(f"{self.tag}{b}{m}", self.buf.at[at(self.pos, self.n, off), 2 * b + h], self.slot(b, m), to)

        def got(self, b, m):
            recv(f"{self.tag}{b}{m}", self.slot(b, m))
            return self.land[b * len(self.spec) + self.idx[m]].astype(F32)

        def relay(self, b, d, h, i):
            off = self.spec[d, h, i][0]
            k = at(self.pos, self.n, off)
            v = self.got(b, (d, h, i - 1))
            self.buf[k, 2 * b + h] = (self.buf[k, 2 * b + h].astype(F32) + v).astype(BF16)
            self.go(b, d, h, i)

        def far(self, b, i):
            self.relay(b, 1, 0, i)
            self.relay(b, -1, 1, i)

        def near(self, b, i):
            self.relay(b, 1, 1, i)
            self.relay(b, -1, 0, i)

        def total(self, b, h):
            v = self.buf[at(self.pos, self.n, 0), 2 * b + h].astype(F32)
            for d in (1, -1):
                last = max(i for e, g, i in self.spec if (e, g) == (d, h))
                v = v + self.got(b, (d, h, last))
            return v

        def first(self, b):
            self.go(b, 1, 0, 1)
            self.go(b, -1, 1, 1)

    Z1 = Stream("z", "z", gu, zr)
    X1 = Stream("x", "x", gd, xr)
    X2 = Stream("s", "z", s2d, s2dr)

    def finish_x(b):
        for h in range(2):
            v = X1.total(b, h).astype(BF16)
            for i in range(NZ):
                s2d[i, 2 * b + h] = v[48 * i : 48 * i + 48]
        X2.first(b)
        X2.go(b, 1, 1, 1)
        X2.go(b, -1, 0, 1)

    def hop(b, i):
        X2.far(b, i)
        if i < 4:
            X2.near(b, i)

    def done_x(b):
        for h in range(2):
            up_v[b, :, 256 * h : 256 * h + 256] = X2.total(b, h)
        store(f"up{b}", up_v.at[b], out.at[0, :, pl.ds(512 * b, 512)])

    def finish_z(b):
        for h in range(2):
            v = Z1.total(b, h).astype(BF16)
            for i in range(NX):
                s2u[b, i, :, 256 * h : 256 * h + 256] = v[48 * i : 48 * i + 48]
        for i in (2, 1, 3):
            send(f"t{b}{i}", s2u.at[b, at(x, NX, i)], s2ur.at[b, i], dev(dx=i))

    def done_z(b):
        v = s2u[b, x].astype(F32)
        for i in (1, 3, 2):
            recv(f"t{b}{i}", s2ur.at[b, i])
            v = v + s2ur[b, i].astype(F32)
        dn_v[b] = v
        store(f"dn{b}", dn_v.at[b], out.at[1, :, pl.ds(512 * b, 512)])

    stores = []

    def store(name, src, dst):
        d = pltpu.make_async_copy(src, dst, osem.at[len(stores)])
        d.start()
        stores.append(d)

    def loss_step(n):
        if n == 0:
            for d in (1, -1):
                send(f"loss_x{d}", loss_own, loss_x.at[d % 4], dev(dx=d))
        elif n == 1:
            recv("loss_x1", loss_x.at[1])
            recv("loss_x-1", loss_x.at[3])
            send("loss_xx", loss_x.at[1], loss_x.at[2], dev(dx=1))
        elif n == 2:
            recv("loss_xx", loss_x.at[2])
            loss_z[0] = loss_own[...] + loss_x[1] + loss_x[2] + loss_x[3]
        if n >= 2:
            for d in (1, -1):
                if n > 2 and (d == 1 or n < 6):
                    recv(f"loss_z{d}_{n - 1}", loss_z.at[(d * (n - 2)) % NZ])
                if n < 5 or (n == 5 and d == 1):
                    send(f"loss_z{d}_{n}", loss_z.at[(d * (n - 2)) % NZ], loss_z.at[(d * (n - 1)) % NZ], dev(dz=d))

    grad_z(4, 0)
    Z1.first(0)
    dact(0, 0)
    grad_x(2, 0)
    X1.first(0)
    grad_z(4, 1)
    Z1.first(1)
    grad_z(3, 0)
    Z1.go(0, 1, 1, 1)
    grad_z(-3, 0)
    Z1.go(0, -1, 0, 1)
    dact(0, 512)
    grad_x(-1, 0)
    X1.go(0, -1, 0, 1)
    grad_x(1, 0)
    X1.go(0, 1, 1, 1)
    loss_step(0)
    Z1.far(0, 2)
    grad_z(3, 1)
    Z1.go(1, 1, 1, 1)
    grad_z(-3, 1)
    Z1.go(1, -1, 0, 1)
    grad_z(2, 0)
    grad_z(-2, 0)
    Z1.far(1, 2)
    grad_z(2, 1)
    grad_z(-2, 1)
    Z1.near(0, 2)
    X1.far(0, 2)
    grad_x(2, 1)
    grad_z(1, 0)
    grad_z(-1, 0)
    grad_z(0, 0)
    grad_x(0, 0)
    Z1.near(1, 2)
    loss_step(1)
    Z1.far(0, 3)
    X1.first(1)
    grad_x(-1, 1)
    grad_x(1, 1)
    grad_z(1, 1)
    grad_z(-1, 1)
    Z1.far(1, 3)
    loss_step(2)
    Z1.near(0, 3)
    X1.go(1, 1, 1, 1)
    X1.go(1, -1, 0, 1)
    finish_x(0)
    grad_z(0, 1)
    grad_x(0, 1)
    X1.far(1, 2)
    Z1.near(1, 3)
    loss_step(3)
    Z1.far(0, 4)
    hop(0, 2)
    Z1.far(1, 4)
    loss_step(4)
    finish_x(1)
    hop(0, 3)
    finish_z(0)
    loss_step(5)
    hop(1, 2)
    hop(0, 4)
    loss_step(6)
    v = loss_z[0]
    for i in range(1, NZ):
        v = v + loss_z[i]
    loss_v[...] = v * (1.0 / (SURV * 2))
    store("loss", loss_v, out_loss)
    hop(1, 3)
    finish_z(1)
    done_x(0)
    done_z(0)
    hop(1, 4)
    done_z(1)
    done_x(1)
    for d in stores:
        d.wait()
    for d in sent:
        d.wait_send()
    assert len(ids) <= NSEM, len(ids)


NSEM = 136


def shards(
    latents, noise, behavior_velocity, timestep, reward_rank_integer, surviving_source_index,
    surviving_slot_index, group_kept_count, patch_input_weight, modulation_lookup,
    up_projection_weight, down_projection_weight, velocity_head_weight,
):
    def pairs(a):
        return a.reshape(SLOTS, 2, 32, 128).transpose(0, 2, 1, 3).reshape(SLOTS, 64, 128)

    smem = pl.BlockSpec(memory_space=pltpu.SMEM)
    vmem = pl.BlockSpec(memory_space=pltpu.VMEM)
    hbm = pl.BlockSpec(memory_space=pl.ANY)
    V = pltpu.VMEM
    piece = (CH // 2, 768)
    scratch = [
        V((1, SURV), I32), V((1, SURV), I32),
        V((SLOTS, 64, 128), BF16), V((SLOTS, 64, 128), BF16), V((SLOTS, 64, 128), BF16), V((64, D), BF16),
        V((KSTEPS, 3, D), F32), V((64, D), BF16), V((CH, D), F32), V((HID, D), BF16),
        V((8, 128), I32), V((D, HID), BF16), V((D, HID), BF16),
        V((TRAJ, 64, 128), BF16), V((2, TRAJ, 64, 128), BF16), V((TRAJ, 64, 128), BF16), V((2, TRAJ, 64, 128), BF16),
        V((8, 128), I32), V((NZ * NX, 8, 128), I32), V((NZ * NX, 128), I32), V((64, 128), F32),
        V((4, 96, 128), F32), V((4, 96, 128), F32), V((4, 96, 128), F32),
        V((16, D), F32), V((16, D), F32), V((16, D), F32), V((16, 128), F32), V((16, 128), F32),
        V((ROWS, D), F32), V((ROWS, D), BF16), V((ROWS, HID), BF16), V((ROWS, HID), F32), V((ROWS, HID), BF16),
        V((4, 2, *piece), BF16), V((4, 2, *piece), BF16), V((4, 2, *piece), F32),
        V((6, *piece), BF16), V((6, *piece), BF16), V((4, 2, 2, *piece), BF16),
        V((2, CH, D), F32), V((2, CH, D), BF16), V((2, CH, 128), F32), V((ROWS, D), BF16),
        V((NX, 384, ROWS), BF16), V((NZ, 192, ROWS), BF16),
        V((NZ, 4, 192, 256), BF16), V((NX, 4, 384, 256), BF16), V((28, 192, 256), BF16), V((12, 384, 256), BF16),
        V((2, NX, 48, 512), BF16), V((NZ, 4, 48, 256), BF16), V((2, NX, 48, 512), BF16), V((28, 48, 256), BF16),
        V((1, 128), F32), V((NX, 1, 128), F32), V((NZ, 1, 128), F32),
        V((2, 48, 512), F32), V((2, 48, 512), F32), V((1, 128), F32),
        pltpu.SemaphoreType.DMA((10,)), pltpu.SemaphoreType.DMA((5,)), pltpu.SemaphoreType.DMA((NSEM,)), pltpu.SemaphoreType.DMA((NSEM,)),
    ]
    grads, loss = pl.pallas_call(
        kernel,
        out_shape=(
            jax.ShapeDtypeStruct((2, 48, HID), F32),
            jax.ShapeDtypeStruct((1, 128), F32),
        ),
        in_specs=[smem] * 3 + [vmem] * 2 + [hbm] * 10,
        out_specs=(hbm,) * 2,
        scratch_shapes=scratch,
        compiler_params=pltpu.CompilerParams(collective_id=0, has_side_effects=True, vmem_limit_bytes=67043328),
    )(
        surviving_slot_index, surviving_source_index, group_kept_count,
        reward_rank_integer.reshape(1, SLOTS), timestep.T,
        surviving_source_index.reshape(1, SURV), surviving_slot_index.reshape(1, SURV), pairs(latents), pairs(noise), pairs(behavior_velocity),
        patch_input_weight, modulation_lookup, velocity_head_weight.T,
        up_projection_weight, down_projection_weight,
    )
    return grads[0], grads[1], loss[0, 0]


def solution(mesh):
    finer = Mesh(mesh.devices.reshape(NZ, NX, NY, NC), ("z", "x", "y", "c"))
    dp, fs = ("z", "x"), ("y", "c")
    in_specs = (
        P(dp, None, None), P(dp, None, None), P(dp, None, None), P(dp, None), P(dp), P(), P(), P(), P(), P(),
        P(None, fs), P(None, fs), P(),
    )
    out_specs = (P(dp, fs), P(dp, fs), P())
    return jax.shard_map(shards, mesh=finer, in_specs=in_specs, out_specs=out_specs, check_vma=False)
```

```python
import jax
import jax.numpy as jnp
from jax import lax
from jax.experimental import pallas as pl
from jax.experimental.pallas import tpu as pltpu
from jax.sharding import Mesh
from jax.sharding import PartitionSpec as P

MESH = pl.DeviceIdType.MESH
F32, BF16, I32 = jnp.float32, jnp.bfloat16, jnp.int32
NZ, NX, NY, NC = 8, 4, 4, 2
D, HID, TRAJ, SLOTS = 1536, 1024, 6, 12
UNITS, ROWS, CH = 12, 768, 192
KSTEPS = 10
SURV = 192
EPS = 1e-06
GELU_K = 0.7978845608028654
GELU_C = 0.044715


def tri(s):
    return lax.rem(s * s * s, 5)


def kernel(
    slot_s, src_s, cnt_s, rank_v, time_v, src_h, slot_h, lat_h, noi_h, old_h, wpatch_h, modl_h, wv_h, wup_h, wdn_h,
    out, out_loss,
    src_v, slot_v, lat, noi, old, wpatch, modl, wv, dfin_s, wdn_t, meta, wup, wdn, snd_a, snd_b, rcv_a, rcv_b, meta_l, meta_all, meta_flat, tmp, xs, nz, od,
    mod_s, mod_c, mod_g, coef_u, adv_u, emb, modb, act, dg, dpre, dsend, drecv, pk, ysend, yrecv, pfull,
    fin, finb, inv, ups, mod_t, up_t, gu, gd, zr, xr, s2u, s2d, s2ur, s2dr, loss_own, loss_x, loss_z,
    up_v, dn_v, loss_v, lsem, osem, ssem, rsem,
):
    z, x, y, c = (lax.axis_index(n) for n in ("z", "x", "y", "c"))
    owner = z * NX + x

    def dev(dz=0, dx=0, dy=0, dc=0):
        return (
            lax.rem(z + (dz + NZ), NZ),
            lax.rem(x + (dx + NX), NX),
            lax.rem(y + (dy + NY), NY),
            lax.rem(c + dc, NC),
        )

    nxt = lax.rem(owner + 1, NZ * NX)
    prv = lax.rem(owner + NZ * NX - 1, NZ * NX)
    next_dev = (nxt // NX, lax.rem(nxt, NX), y, c)
    prev_dev = (prv // NX, lax.rem(prv, NX), y, c)

    ids = {}

    def mid(name):
        return ids.setdefault(name, len(ids))

    sent = []

    def copy(name, src, dst, to):
        i = mid(name) if isinstance(name, str) else name
        return pltpu.make_async_remote_copy(
            src_ref=src, dst_ref=dst, send_sem=ssem.at[i], recv_sem=rsem.at[i],
            device_id=to, device_id_type=MESH,
        )

    def send(name, src, dst, to):
        d = copy(name, src, dst, to)
        d.start()
        sent.append(d)

    def recv(name, dst, to=None):
        copy(name, dst, dst, dev(dc=1) if to is None else to).wait_recv()

    barrier = pltpu.get_barrier_semaphore()
    peers = [dev(dx=2), dev(dx=1), dev(dx=-1), dev(dz=1), dev(dz=-1), dev(dy=1), dev(dy=-1), dev(dc=1), next_dev, prev_dev]
    for p in peers:
        pl.semaphore_signal(barrier, inc=1, device_id=p, device_id_type=MESH)
    pairs = (
        (lat_h, lat), (noi_h, noi), (old_h, old), (modl_h, modl), (wpatch_h, wpatch), (wdn_h, wdn), (wup_h, wup), (wv_h, wv),
        (src_h, src_v), (slot_h, slot_v),
    )
    loads = [pltpu.make_async_copy(a, b, lsem.at[i]) for i, (a, b) in enumerate(pairs)]
    for cp in loads:
        cp.start()
    meta[0:1, 0:SLOTS] = rank_v[...]
    meta[1:3, 0:SLOTS] = time_v[...]
    meta_all[z * NX + x] = meta[...]
    lead_n = jnp.minimum(owner + 1, NZ * NX - 1) * TRAJ
    lead = owner * TRAJ
    next_slots = [slot_s[lead_n + i] for i in range(TRAJ)]
    loads[0].wait()
    for i in range(TRAJ):
        snd_a[i] = lat[next_slots[i]]
    pl.semaphore_wait(barrier, len(peers))
    send("meta_l", meta, meta_l, next_dev)
    send("shift_a", snd_a, rcv_a, next_dev)
    loads[1].wait()
    loads[2].wait()
    for i in range(TRAJ):
        snd_b[0, i] = noi[next_slots[i]]
        snd_b[1, i] = old[next_slots[i]]
    send("shift_b", snd_b, rcv_b, next_dev)
    row_of = lambda d: z * NX + lax.rem(x + (d + NX), NX)
    block = lambda d: pl.ds(lax.rem(z + (d + NZ), NZ) * NX, NX)
    for d in (1, -1):
        send(f"meta_x{d}", meta, meta_all.at[row_of(0)], dev(dx=d))

    def meta_step(n):
        if n == 0:
            recv("meta_x1", meta_all.at[row_of(-1)])
            recv("meta_x-1", meta_all.at[row_of(1)])
            copy("meta_xx", meta_all.at[row_of(-1)], meta_all.at[row_of(-1)], dev(dx=1)).start()
            return
        if n == 1:
            recv("meta_xx", meta_all.at[row_of(-2)])
        for d in (1, -1):
            if n > 1 and (d == 1 or n < 5):
                recv(f"meta_z{d}_{n - 1}", meta_all.at[block(-d * (n - 1))])
            if n < 4 or (n == 4 and d == 1):
                b = block(-d * (n - 1))
                copy(f"meta_z{d}_{n}", meta_all.at[b], meta_all.at[b], dev(dz=d)).start()

    def meta_sent():
        sent.append(copy("meta_xx", meta_all.at[row_of(-1)], meta_all.at[row_of(-1)], dev(dx=1)))
        for d, last in ((1, 4), (-1, 3)):
            for n in range(1, last + 1):
                b = block(-d * (n - 1))
                sent.append(copy(f"meta_z{d}_{n}", meta_all.at[b], meta_all.at[b], dev(dz=d)))

    loads[5].wait()
    for b in range(4):
        wdn_t[:, 384 * b : 384 * b + 384] = wdn[384 * b : 384 * b + 384, :].T
    loads[3].wait()

    slots = [slot_s[lead + i] for i in range(TRAJ)]
    lefts = [src_s[lead + i] != owner for i in range(TRAJ)]

    sub = lax.broadcasted_iota(I32, (16, 128), 0)
    lane = lax.broadcasted_iota(I32, (16, 128), 1)
    pos = jnp.zeros((16, 128), I32)
    from_left = jnp.zeros((16, 128), I32)
    for i in range(TRAJ):
        mine = (sub >> 1) == i
        pos = pos + jnp.where(mine, slots[i], 0)
        from_left = from_left + jnp.where(mine, lefts[i].astype(I32), 0)
    recv("meta_l", meta_l)

    def step_row(n):
        wide = [jnp.broadcast_to(m[n : n + 1, :], (16, 128)) for m in (meta_l, meta)]
        return jnp.where(from_left == 1, wide[0], wide[1])

    row = jnp.where((sub & 1) == 0, step_row(1), step_row(2))
    stamp = jnp.sum(jnp.where(lane == pos, row.astype(F32), 0.0), axis=1, keepdims=True)
    level = 1.0 - stamp * (1.0 / KSTEPS)
    coef = jnp.sqrt((1.0 / KSTEPS) * (1.0 - level + (1.0 / KSTEPS)) / level) / 0.7
    coef_u[...] = jnp.broadcast_to(coef, (16, 128))
    for kind, dst in ((0, mod_s), (1, mod_c), (2, mod_g)):
        acc = jnp.zeros((16, D), F32)
        for t in range(KSTEPS):
            acc = jnp.where(stamp == float(t), jnp.broadcast_to(modl[t, pl.ds(kind, 1), :], (16, D)), acc)
        dst[...] = acc + 1.0 if kind == 1 else acc

    def assemble(own, arrived, i):
        v = jnp.where(lefts[i], arrived.astype(F32), own.astype(F32))
        tmp[...] = v
        return tmp[pl.ds(0, 32, stride=2), :], tmp[pl.ds(1, 32, stride=2), :]

    recv("shift_a", rcv_a)
    for i in range(TRAJ):
        for step, v in enumerate(assemble(lat[slots[i]], rcv_a[i], i)):
            u = 2 * i + step
            xs[u // 3, (u % 3) * 32 : (u % 3) * 32 + 32, :] = v

    def spread(pair):
        return jnp.concatenate([pair[:, :64], pltpu.roll(pair, 64, 1)[:, :64]], axis=0)

    for i in (4, 6, 7, 8, 9):
        loads[i].wait()

    yu, yd, yo = (lax.rem(y + i, NY) for i in (1, 3, 2))
    held = ((yo, yo), (yd, yu), (yu, yd), (y, y))

    def embed(s):
        even, odd = (xs[k] for k in held[s])
        rows = jnp.concatenate([even[:, :64], pltpu.roll(odd, 64, 1)[:, :64]], axis=0)
        emb[s * CH : s * CH + CH, :] = jnp.dot(rows.astype(BF16), wpatch[...], preferred_element_type=F32)

    def norm(s, blocks):
        for b in blocks:
            rb = s * CH + b * 16
            u = held[s][b // 6] * 3 + (b % 6) // 2
            v = emb[rb : rb + 16, :]
            v = v - jnp.mean(v, axis=-1, keepdims=True)
            i = lax.rsqrt(jnp.mean(v * v, axis=-1, keepdims=True) + EPS)
            modb[rb : rb + 16, :] = (v * i * mod_c[pl.ds(u, 1), :] + mod_s[pl.ds(u, 1), :]).astype(BF16)

    def up(s, n):
        rows, cols = slice(s * CH, s * CH + CH), slice(256 * n, 256 * n + 256)
        pre = jnp.dot(modb[rows, :], wup[:, cols], preferred_element_type=F32)
        th = jnp.tanh(GELU_K * (pre + GELU_C * (pre * pre * pre)))
        act[rows, cols] = (pre * (0.5 * (1.0 + th))).astype(BF16)
        dg[rows, cols] = pre

    def slope_of(s):
        rows = slice(s * CH, s * CH + CH)
        for n in range(4):
            cols = slice(256 * n, 256 * n + 256)
            pre = dg[rows, cols]
            sq = pre * pre
            th = jnp.tanh(GELU_K * (pre + GELU_C * (sq * pre)))
            dg[rows, cols] = 0.5 * (1.0 + th) + (0.5 * GELU_K) * pre * (1.0 - th * th) * (1.0 + 3.0 * GELU_C * sq)

    def down(s):
        rows = slice(s * CH, s * CH + CH)
        for j in range(2):
            q = pl.multiple_of((1 - c if j == 0 else c) * 768, 768)
            v = jnp.dot(act[rows, :], wdn_t[:, pl.ds(q, 768)], preferred_element_type=F32)
            for h in range(2):
                if j == 0:
                    dsend[s, h] = v[96 * h : 96 * h + 96].astype(BF16)
                else:
                    pk[s, h] = v[96 * h : 96 * h + 96]
            if j == 0:
                send(f"d2d{s}", dsend.at[s], drecv.at[s], dev(dc=1))

    def presum(s):
        recv(f"d2d{s}", drecv.at[s])
        for h in range(2):
            pk[s, h] = pk[s, h] + drecv[s, h].astype(F32)

    def ygo(name, i, v, d):
        ysend[i] = v.astype(BF16)
        send(name, ysend.at[i], yrecv.at[i], dev(dy=d))

    def yphase(s):
        if s == 1:
            presum(0)
            ygo("y1a", 0, pk[0, 0], 1)
            ygo("y1b", 1, pk[0, 1], -1)
        elif s == 2:
            presum(1)
            ygo("y2a", 2, pk[1, 0], -1)
            ygo("y2b", 3, pk[1, 1], 1)
        elif s == 3:
            presum(2)
            recv("y1a", yrecv.at[0])
            ygo("y3a", 5, pk[2, 0] + yrecv[0].astype(F32), 1)
            recv("y1b", yrecv.at[1])
            ygo("y3b", 4, pk[2, 1] + yrecv[1].astype(F32), -1)

    embed(0)
    norm(0, range(12))
    for s in range(4):
        if s < 3:
            embed(s + 1)
        for n in range(4):
            up(s, n)
            if s < 3:
                norm(s + 1, range(3 * n, 3 * n + 3))
        yphase(s)
        down(s)
        meta_step(s)
    def transpose_pair(p, src, put):
        tok = slice(p * 384, p * 384 + 384)
        for b in range(4):
            put(b, tok, src[tok, 384 * b : 384 * b + 384].T)

    def put_up(b, tok, t):
        up_t[2 * b, :, tok] = t[:192]
        up_t[2 * b + 1, :, tok] = t[192:]

    def put_mod(b, tok, t):
        for zz in range(2):
            for xx in range(NX):
                o = zz * 192 + xx * 48
                mod_t[xx, (2 * b + zz) * 48 : (2 * b + zz) * 48 + 48, tok] = t[o : o + 48]

    presum(3)
    part = lambda k, h: pfull.at[k, c, h]
    recv("y2a", yrecv.at[2])
    recv("y3a", yrecv.at[5])
    pfull[y, c, 0] = (pk[3, 0] + yrecv[2].astype(F32) + yrecv[5].astype(F32)).astype(BF16)
    send("g_up_a", part(y, 0), part(y, 0), dev(dy=1))
    recv("y2b", yrecv.at[3])
    recv("y3b", yrecv.at[4])
    pfull[y, c, 1] = (pk[3, 1] + yrecv[3].astype(F32) + yrecv[4].astype(F32)).astype(BF16)
    send("g_dn_b", part(y, 1), part(y, 1), dev(dy=-1))
    send("g_up_b", part(y, 1), part(y, 1), dev(dy=1))
    send("g_dn_a", part(y, 0), part(y, 0), dev(dy=-1))
    send("c_own", pfull.at[y, c], pfull.at[y, c], dev(dc=1))

    loss_own[...] = jnp.zeros((1, 128), F32)

    def mix(w, k, t, r0, behind=()):
        for b in range(6):
            o = t * 96 + b * 16
            u = k * 3 + b // 2
            proj = jnp.concatenate([pfull[k, q, t, b * 16 : b * 16 + 16, :] for q in range(2)], axis=1).astype(F32)
            v = emb[r0 + b * 16 : r0 + b * 16 + 16, :] + mod_g[pl.ds(u, 1), :] * proj
            v = v - jnp.mean(v, axis=-1, keepdims=True)
            i = lax.rsqrt(jnp.mean(v * v, axis=-1, keepdims=True) + EPS)
            v = v * i
            fin[w, o : o + 16, :] = v
            finb[w, o : o + 16, :] = v.astype(BF16)
            inv[w, o : o + 16, :] = jnp.broadcast_to(i, (16, 128))
        for slot, lo in behind:
            dact(slot * CH, lo)

    def rest(w, k, offs):
        velocity = lax.dot_general(finb[w], wv[...], (((1,), (1,)), ((), ())), preferred_element_type=F32)
        drawn, target = spread(nz[k]), spread(od[k])
        err = velocity - target
        dv = [None] * 6
        for j in range(3):
            u = k * 3 + j
            cu = coef_u[pl.ds(u, 1), :][:, :64]
            au = adv_u[pl.ds(u, 1), :][:, :1]
            part = jnp.zeros((32, 64), F32)
            for h in range(2):
                o = h * 96 + j * 32
                e, n = err[o : o + 32], drawn[o : o + 32]
                part = part + cu * n * e + 0.5 * cu * cu * e * e
            logratio = -jnp.sum(jnp.sum(part, axis=0, keepdims=True), axis=1, keepdims=True) * (1.0 / 4096)
            ratio = jnp.exp(logratio)
            plain = ratio * au
            bounded = jnp.clip(ratio, 0.8, 1.2) * au
            loss_own[...] += jnp.broadcast_to(-jnp.minimum(plain, bounded), (1, 128))
            slope = jnp.where(plain <= bounded, -au * ratio * (1.0 / (SURV * 2)), 0.0)
            for h in range(2):
                o = h * 96 + j * 32
                e, n = err[o : o + 32], drawn[o : o + 32]
                dv[h * 3 + j] = slope * (-(cu * n + cu * cu * e) * (1.0 / 4096))
        dvel = jnp.concatenate(dv, axis=0).astype(BF16)
        dfin = jnp.dot(dvel, wv[...], preferred_element_type=F32)
        dfin_s[...] = dfin

        for t in range(2):
            for b in range(6):
                o = t * 96 + b * 16
                u = k * 3 + b // 2
                g = dfin_s[o : o + 16, :]
                f = fin[w, o : o + 16, :]
                m1 = jnp.mean(g, axis=-1, keepdims=True)
                m2 = jnp.mean(g * f, axis=-1, keepdims=True)
                i = inv[w, o : o + 16, :][:, :1]
                r = offs[t] + b * 16
                ups[r : r + 16, :] = (mod_g[pl.ds(u, 1), :] * (i * (g - m1 - f * m2))).astype(BF16)

    def dact(r0, lo):
        rows, cols = slice(r0, r0 + CH), slice(lo, lo + 512)
        v = jnp.dot(ups[rows, :], wdn[:, cols], preferred_element_type=F32)
        dpre[rows, cols] = (v * dg[rows, cols]).astype(BF16)

    def fwd_core(name, k, h):
        send(name, part(k, h), part(k, h), dev(dc=1))

    def got(name, k, h):
        recv(name, part(k, h))

    def core(name, k, h):
        recv(name, pfull.at[k, 1 - c, h])

    recv("shift_b", rcv_b)
    for i in range(TRAJ):
        for arr, which, dst in ((noi, 0, nz), (old, 1, od)):
            for step, v in enumerate(assemble(arr[slots[i]], rcv_b[which, i], i)):
                u = 2 * i + step
                dst[u // 3, (u % 3) * 32 : (u % 3) * 32 + 32, :] = v

    meta_step(4)

    def bounds(g, carry):
        end = carry[0] + cnt_s[g]
        out = [end]
        for i in range(TRAJ):
            hit = (lead + i >= carry[0]) & (lead + i < end)
            out += [jnp.where(hit, carry[0], carry[1 + 2 * i]), jnp.where(hit, end, carry[2 + 2 * i])]
        return tuple(out)

    ends = lax.fori_loop(0, 48, bounds, (jnp.int32(0),) * (1 + 2 * TRAJ))
    recv("c_own", pfull.at[y, 1 - c])
    own = (3 * CH, 3 * CH + 96)
    for t in range(2):
        mix(0, y, t, own[t])
    meta_step(5)
    meta_sent()
    for r in range(NZ * NX):
        meta_flat[r : r + 1, :] = meta_all[r, 0:1, :]
    ranks = meta_flat[...]
    hot = (lax.broadcasted_iota(I32, (NZ * NX, SURV), 0) == src_v[...]).astype(F32).astype(BF16)
    first = (((0,), (0,)), ((), ()))
    hi = lax.dot_general((ranks >> 4).astype(F32).astype(BF16), hot, first, preferred_element_type=F32)[:16]
    lo = lax.dot_general((ranks & 15).astype(F32).astype(BF16), hot, first, preferred_element_type=F32)[:16]
    by_slot = hi * 16.0 + lo
    rank = jnp.sum(
        jnp.where(lax.broadcasted_iota(I32, (16, SURV), 0) == slot_v[...], by_slot, 0.0), axis=0, keepdims=True
    )
    rank_i = rank.astype(I32)
    sq_i = rank_i * rank_i
    sq_hi, sq_lo = (sq_i >> 10).astype(F32), (sq_i & 1023).astype(F32)
    jdx = lax.broadcasted_iota(I32, (1, SURV), 1)

    for i in range(TRAJ):
        lo_i, hi_i = ends[1 + 2 * i], ends[2 + 2 * i]
        inside = (jdx >= lo_i) & (jdx < hi_i)

        def total(v):
            return jnp.sum(jnp.where(inside, v, 0.0), axis=1, keepdims=True)

        s1 = total(rank)
        s1_i = s1.astype(I32)
        s2_i = total(sq_hi).astype(I32) * 1024 + total(sq_lo).astype(I32)
        n_i = jnp.full((1, 1), hi_i - lo_i, I32)
        n = n_i.astype(F32)
        r = jnp.sum(jnp.where(jdx == lead + i, rank, 0.0), axis=1, keepdims=True)
        dev_i = jnp.sqrt((n_i * s2_i - s1_i * s1_i).astype(F32)) / n
        a = (r - s1 / n) / jnp.maximum(dev_i, 1.0)
        adv_u[2 * i : 2 * i + 2, :] = jnp.broadcast_to(a, (2, 128))

    slope_of(0)
    got("g_up_a", yd, 0)
    send("r_up", part(yd, 0), part(yd, 0), dev(dy=1))
    fwd_core("c_da", yd, 0)
    got("g_dn_b", yu, 1)
    send("r_dn", part(yu, 1), part(yu, 1), dev(dy=-1))
    fwd_core("c_ub", yu, 1)
    rest(0, y, own)
    slope_of(3)
    for p in range(2):
        transpose_pair(p, modb, put_mod)

    core("c_da", yd, 0)
    core("c_ub", yu, 1)
    mix(0, yu, 1, CH + 96, [(3, 0)])
    mix(1, yd, 0, CH, [(3, 512)])
    got("g_dn_a", yu, 0)
    fwd_core("c_ua", yu, 0)
    got("g_up_b", yd, 1)
    fwd_core("c_db", yd, 1)
    slope_of(1)
    slope_of(2)
    core("c_ua", yu, 0)
    mix(0, yu, 0, 2 * CH)
    rest(0, yu, (2 * CH, CH + 96))
    core("c_db", yd, 1)
    mix(1, yd, 1, 2 * CH + 96)
    got("r_up", yo, 0)
    fwd_core("c_oa", yo, 0)
    got("r_dn", yo, 1)
    fwd_core("c_ob", yo, 1)
    rest(1, yd, (CH, 2 * CH + 96))
    transpose_pair(1, ups, put_up)
    core("c_oa", yo, 0)
    core("c_ob", yo, 1)
    mix(0, yo, 0, 0, [(1, 0), (1, 512)])
    mix(0, yo, 1, 96, [(2, 0), (2, 512)])
    rest(0, yo, (0, 96))
    transpose_pair(0, ups, put_up)

    def grad_x(off, b):
        k = at(x, NX, off)
        v = jnp.dot(mod_t[k], dpre[:, 512 * b : 512 * b + 512], preferred_element_type=F32).astype(BF16)
        gd[k, 2 * b], gd[k, 2 * b + 1] = v[:, :256], v[:, 256:]

    def grad_z(off, b):
        k = at(z, NZ, off)
        v = jnp.dot(up_t[k], act[:, 512 * b : 512 * b + 512], preferred_element_type=F32).astype(BF16)
        gu[k, 2 * b], gu[k, 2 * b + 1] = v[:, :256], v[:, 256:]

    def at(axis_pos, n, off):
        return lax.rem(axis_pos + (off + n), n)

    def ring(n):
        spec = {}
        for d in (1, -1):
            for h in range(2):
                far = (h == 0) == (d == 1)
                last = n // 2 if far else n // 2 - 1
                for i in range(1, last + 1):
                    spec[d, h, i] = (d * (last + 1 - i), h, d)
        return spec, {m: i for i, m in enumerate(spec)}

    zspec, zi = ring(NZ)
    xspec, xi = ring(NX)

    class Stream:
        def __init__(self, tag, axis, buf, land):
            self.tag, self.axis, self.buf, self.land = tag, axis, buf, land
            self.spec, self.idx = (zspec, zi) if axis == "z" else (xspec, xi)
            self.pos, self.n = (z, NZ) if axis == "z" else (x, NX)

        def slot(self, b, m):
            return self.land.at[b * len(self.spec) + self.idx[m]]

        def go(self, b, *m):
            off, h, d = self.spec[m]
            to = dev(dz=d) if self.axis == "z" else dev(dx=d)
            send(f"{self.tag}{b}{m}", self.buf.at[at(self.pos, self.n, off), 2 * b + h], self.slot(b, m), to)

        def got(self, b, m):
            recv(f"{self.tag}{b}{m}", self.slot(b, m))
            return self.land[b * len(self.spec) + self.idx[m]].astype(F32)

        def relay(self, b, d, h, i):
            off = self.spec[d, h, i][0]
            k = at(self.pos, self.n, off)
            v = self.got(b, (d, h, i - 1))
            self.buf[k, 2 * b + h] = (self.buf[k, 2 * b + h].astype(F32) + v).astype(BF16)
            self.go(b, d, h, i)

        def far(self, b, i):
            self.relay(b, 1, 0, i)
            self.relay(b, -1, 1, i)

        def near(self, b, i):
            self.relay(b, 1, 1, i)
            self.relay(b, -1, 0, i)

        def total(self, b, h):
            v = self.buf[at(self.pos, self.n, 0), 2 * b + h].astype(F32)
            for d in (1, -1):
                last = max(i for e, g, i in self.spec if (e, g) == (d, h))
                v = v + self.got(b, (d, h, last))
            return v

        def first(self, b):
            self.go(b, 1, 0, 1)
            self.go(b, -1, 1, 1)

    Z1 = Stream("z", "z", gu, zr)
    X1 = Stream("x", "x", gd, xr)
    X2 = Stream("s", "z", s2d, s2dr)

    def finish_x(b):
        for h in range(2):
            v = X1.total(b, h).astype(BF16)
            for i in range(NZ):
                s2d[i, 2 * b + h] = v[48 * i : 48 * i + 48]
        X2.first(b)
        X2.go(b, 1, 1, 1)
        X2.go(b, -1, 0, 1)

    def hop(b, i):
        X2.far(b, i)
        if i < 4:
            X2.near(b, i)

    def done_x(b):
        for h in range(2):
            up_v[b, :, 256 * h : 256 * h + 256] = X2.total(b, h)
        store(f"up{b}", up_v.at[b], out.at[0, :, pl.ds(512 * b, 512)])

    def finish_z(b):
        for h in range(2):
            v = Z1.total(b, h).astype(BF16)
            for i in range(NX):
                s2u[b, i, :, 256 * h : 256 * h + 256] = v[48 * i : 48 * i + 48]
        for i in (2, 1, 3):
            send(f"t{b}{i}", s2u.at[b, at(x, NX, i)], s2ur.at[b, i], dev(dx=i))

    def done_z(b):
        v = s2u[b, x].astype(F32)
        for i in (1, 3, 2):
            recv(f"t{b}{i}", s2ur.at[b, i])
            v = v + s2ur[b, i].astype(F32)
        dn_v[b] = v
        store(f"dn{b}", dn_v.at[b], out.at[1, :, pl.ds(512 * b, 512)])

    stores = []

    def store(name, src, dst):
        d = pltpu.make_async_copy(src, dst, osem.at[len(stores)])
        d.start()
        stores.append(d)

    def loss_step(n):
        if n == 0:
            for d in (1, -1):
                send(f"loss_x{d}", loss_own, loss_x.at[d % 4], dev(dx=d))
        elif n == 1:
            recv("loss_x1", loss_x.at[1])
            recv("loss_x-1", loss_x.at[3])
            send("loss_xx", loss_x.at[1], loss_x.at[2], dev(dx=1))
        elif n == 2:
            recv("loss_xx", loss_x.at[2])
            loss_z[0] = loss_own[...] + loss_x[1] + loss_x[2] + loss_x[3]
        if n >= 2:
            for d in (1, -1):
                if n > 2 and (d == 1 or n < 6):
                    recv(f"loss_z{d}_{n - 1}", loss_z.at[(d * (n - 2)) % NZ])
                if n < 5 or (n == 5 and d == 1):
                    send(f"loss_z{d}_{n}", loss_z.at[(d * (n - 2)) % NZ], loss_z.at[(d * (n - 1)) % NZ], dev(dz=d))

    grad_z(4, 0)
    Z1.first(0)
    dact(0, 0)
    grad_x(2, 0)
    X1.first(0)
    grad_z(4, 1)
    Z1.first(1)
    grad_z(3, 0)
    Z1.go(0, 1, 1, 1)
    grad_z(-3, 0)
    Z1.go(0, -1, 0, 1)
    dact(0, 512)
    grad_x(-1, 0)
    X1.go(0, -1, 0, 1)
    grad_x(1, 0)
    X1.go(0, 1, 1, 1)
    loss_step(0)
    Z1.far(0, 2)
    grad_z(3, 1)
    Z1.go(1, 1, 1, 1)
    grad_z(-3, 1)
    Z1.go(1, -1, 0, 1)
    grad_z(2, 0)
    grad_z(-2, 0)
    Z1.far(1, 2)
    grad_z(2, 1)
    grad_z(-2, 1)
    Z1.near(0, 2)
    X1.far(0, 2)
    grad_x(2, 1)
    grad_z(1, 0)
    grad_z(-1, 0)
    grad_z(0, 0)
    grad_x(0, 0)
    Z1.near(1, 2)
    loss_step(1)
    Z1.far(0, 3)
    X1.first(1)
    grad_x(-1, 1)
    grad_x(1, 1)
    grad_z(1, 1)
    grad_z(-1, 1)
    Z1.far(1, 3)
    loss_step(2)
    Z1.near(0, 3)
    X1.go(1, 1, 1, 1)
    X1.go(1, -1, 0, 1)
    finish_x(0)
    grad_z(0, 1)
    grad_x(0, 1)
    X1.far(1, 2)
    Z1.near(1, 3)
    loss_step(3)
    Z1.far(0, 4)
    hop(0, 2)
    finish_x(1)
    Z1.far(1, 4)
    loss_step(4)
    hop(0, 3)
    hop(1, 2)
    finish_z(0)
    loss_step(5)
    hop(0, 4)
    hop(1, 3)
    finish_z(1)
    loss_step(6)
    v = loss_z[0]
    for i in range(1, NZ):
        v = v + loss_z[i]
    loss_v[...] = v * (1.0 / (SURV * 2))
    store("loss", loss_v, out_loss)
    hop(1, 4)
    done_x(0)
    done_z(0)
    done_x(1)
    done_z(1)
    for d in stores:
        d.wait()
    for d in sent:
        d.wait_send()
    assert len(ids) <= NSEM, len(ids)


NSEM = 136


def shards(
    latents, noise, behavior_velocity, timestep, reward_rank_integer, surviving_source_index,
    surviving_slot_index, group_kept_count, patch_input_weight, modulation_lookup,
    up_projection_weight, down_projection_weight, velocity_head_weight,
):
    def pairs(a):
        return a.reshape(SLOTS, 2, 32, 128).transpose(0, 2, 1, 3).reshape(SLOTS, 64, 128)

    smem = pl.BlockSpec(memory_space=pltpu.SMEM)
    vmem = pl.BlockSpec(memory_space=pltpu.VMEM)
    hbm = pl.BlockSpec(memory_space=pl.ANY)
    V = pltpu.VMEM
    piece = (CH // 2, 768)
    scratch = [
        V((1, SURV), I32), V((1, SURV), I32),
        V((SLOTS, 64, 128), BF16), V((SLOTS, 64, 128), BF16), V((SLOTS, 64, 128), BF16), V((64, D), BF16),
        V((KSTEPS, 3, D), F32), V((64, D), BF16), V((CH, D), F32), V((HID, D), BF16),
        V((8, 128), I32), V((D, HID), BF16), V((D, HID), BF16),
        V((TRAJ, 64, 128), BF16), V((2, TRAJ, 64, 128), BF16), V((TRAJ, 64, 128), BF16), V((2, TRAJ, 64, 128), BF16),
        V((8, 128), I32), V((NZ * NX, 8, 128), I32), V((NZ * NX, 128), I32), V((64, 128), F32),
        V((4, 96, 128), F32), V((4, 96, 128), F32), V((4, 96, 128), F32),
        V((16, D), F32), V((16, D), F32), V((16, D), F32), V((16, 128), F32), V((16, 128), F32),
        V((ROWS, D), F32), V((ROWS, D), BF16), V((ROWS, HID), BF16), V((ROWS, HID), F32), V((ROWS, HID), BF16),
        V((4, 2, *piece), BF16), V((4, 2, *piece), BF16), V((4, 2, *piece), F32),
        V((6, *piece), BF16), V((6, *piece), BF16), V((4, 2, 2, *piece), BF16),
        V((2, CH, D), F32), V((2, CH, D), BF16), V((2, CH, 128), F32), V((ROWS, D), BF16),
        V((NX, 384, ROWS), BF16), V((NZ, 192, ROWS), BF16),
        V((NZ, 4, 192, 256), BF16), V((NX, 4, 384, 256), BF16), V((28, 192, 256), BF16), V((12, 384, 256), BF16),
        V((2, NX, 48, 512), BF16), V((NZ, 4, 48, 256), BF16), V((2, NX, 48, 512), BF16), V((28, 48, 256), BF16),
        V((1, 128), F32), V((NX, 1, 128), F32), V((NZ, 1, 128), F32),
        V((2, 48, 512), F32), V((2, 48, 512), F32), V((1, 128), F32),
        pltpu.SemaphoreType.DMA((10,)), pltpu.SemaphoreType.DMA((5,)), pltpu.SemaphoreType.DMA((NSEM,)), pltpu.SemaphoreType.DMA((NSEM,)),
    ]
    grads, loss = pl.pallas_call(
        kernel,
        out_shape=(
            jax.ShapeDtypeStruct((2, 48, HID), F32),
            jax.ShapeDtypeStruct((1, 128), F32),
        ),
        in_specs=[smem] * 3 + [vmem] * 2 + [hbm] * 10,
        out_specs=(hbm,) * 2,
        scratch_shapes=scratch,
        compiler_params=pltpu.CompilerParams(collective_id=0, has_side_effects=True, vmem_limit_bytes=67043328),
    )(
        surviving_slot_index, surviving_source_index, group_kept_count,
        reward_rank_integer.reshape(1, SLOTS), timestep.T,
        surviving_source_index.reshape(1, SURV), surviving_slot_index.reshape(1, SURV), pairs(latents), pairs(noise), pairs(behavior_velocity),
        patch_input_weight, modulation_lookup, velocity_head_weight.T,
        up_projection_weight, down_projection_weight,
    )
    return grads[0], grads[1], loss[0, 0]


def solution(mesh):
    finer = Mesh(mesh.devices.reshape(NZ, NX, NY, NC), ("z", "x", "y", "c"))
    dp, fs = ("z", "x"), ("y", "c")
    in_specs = (
        P(dp, None, None), P(dp, None, None), P(dp, None, None), P(dp, None), P(dp), P(), P(), P(), P(), P(),
        P(None, fs), P(None, fs), P(),
    )
    out_specs = (P(dp, fs), P(dp, fs), P())
    return jax.shard_map(shards, mesh=finer, in_specs=in_specs, out_specs=out_specs, check_vma=False)
```

```python
import jax
import jax.numpy as jnp
from jax import lax
from jax.experimental import pallas as pl
from jax.experimental.pallas import tpu as pltpu
from jax.sharding import Mesh
from jax.sharding import PartitionSpec as P

MESH = pl.DeviceIdType.MESH
F32, BF16, I32 = jnp.float32, jnp.bfloat16, jnp.int32
NZ, NX, NY, NC = 8, 4, 4, 2
D, HID, TRAJ, SLOTS = 1536, 1024, 6, 12
UNITS, ROWS, CH = 12, 768, 192
KSTEPS = 10
SURV = 192
EPS = 1e-06
GELU_K = 0.7978845608028654
GELU_C = 0.044715


def tri(s):
    return lax.rem(s * s * s, 5)


def kernel(
    slot_s, src_s, cnt_s, rank_v, time_v, src_h, slot_h, lat_h, noi_h, old_h, wpatch_h, modl_h, wv_h, wup_h, wdn_h,
    out, out_loss,
    src_v, slot_v, lat, noi, old, wpatch, modl, wv, dfin_s, wdn_t, meta, wup, wdn, snd_a, snd_b, rcv_a, rcv_b, meta_l, meta_all, meta_flat, tmp, xs, nz, od,
    mod_s, mod_c, mod_g, coef_u, adv_u, emb, modb, act, dg, dpre, dsend, drecv, pk, ysend, yrecv, pfull,
    fin, finb, inv, ups, mod_t, up_t, gu, gd, zr, xr, s2u, s2d, s2ur, s2dr, loss_own, loss_x, loss_z,
    up_v, dn_v, loss_v, lsem, osem, ssem, rsem,
):
    z, x, y, c = (lax.axis_index(n) for n in ("z", "x", "y", "c"))
    owner = z * NX + x

    def dev(dz=0, dx=0, dy=0, dc=0):
        return (
            lax.rem(z + (dz + NZ), NZ),
            lax.rem(x + (dx + NX), NX),
            lax.rem(y + (dy + NY), NY),
            lax.rem(c + dc, NC),
        )

    nxt = lax.rem(owner + 1, NZ * NX)
    prv = lax.rem(owner + NZ * NX - 1, NZ * NX)
    next_dev = (nxt // NX, lax.rem(nxt, NX), y, c)
    prev_dev = (prv // NX, lax.rem(prv, NX), y, c)

    ids = {}

    def mid(name):
        return ids.setdefault(name, len(ids))

    sent = []

    def copy(name, src, dst, to):
        i = mid(name) if isinstance(name, str) else name
        return pltpu.make_async_remote_copy(
            src_ref=src, dst_ref=dst, send_sem=ssem.at[i], recv_sem=rsem.at[i],
            device_id=to, device_id_type=MESH,
        )

    def send(name, src, dst, to):
        d = copy(name, src, dst, to)
        d.start()
        sent.append(d)

    def recv(name, dst, to=None):
        copy(name, dst, dst, dev(dc=1) if to is None else to).wait_recv()

    barrier = pltpu.get_barrier_semaphore()
    peers = [dev(dx=2), dev(dx=1), dev(dx=-1), dev(dz=1), dev(dz=-1), dev(dy=1), dev(dy=-1), dev(dc=1), next_dev, prev_dev]
    for p in peers:
        pl.semaphore_signal(barrier, inc=1, device_id=p, device_id_type=MESH)
    pairs = (
        (lat_h, lat), (noi_h, noi), (old_h, old), (modl_h, modl), (wpatch_h, wpatch), (wdn_h, wdn), (wup_h, wup), (wv_h, wv),
        (src_h, src_v), (slot_h, slot_v),
    )
    loads = [pltpu.make_async_copy(a, b, lsem.at[i]) for i, (a, b) in enumerate(pairs)]
    for cp in loads:
        cp.start()
    meta[0:1, 0:SLOTS] = rank_v[...]
    meta[1:3, 0:SLOTS] = time_v[...]
    meta_all[z * NX + x] = meta[...]
    lead_n = jnp.minimum(owner + 1, NZ * NX - 1) * TRAJ
    lead = owner * TRAJ
    next_slots = [slot_s[lead_n + i] for i in range(TRAJ)]
    loads[0].wait()
    for i in range(TRAJ):
        snd_a[i] = lat[next_slots[i]]
    pl.semaphore_wait(barrier, len(peers))
    send("meta_l", meta, meta_l, next_dev)
    send("shift_a", snd_a, rcv_a, next_dev)
    loads[1].wait()
    loads[2].wait()
    for i in range(TRAJ):
        snd_b[0, i] = noi[next_slots[i]]
        snd_b[1, i] = old[next_slots[i]]
    send("shift_b", snd_b, rcv_b, next_dev)
    row_of = lambda d: z * NX + lax.rem(x + (d + NX), NX)
    block = lambda d: pl.ds(lax.rem(z + (d + NZ), NZ) * NX, NX)
    for d in (1, -1):
        send(f"meta_x{d}", meta, meta_all.at[row_of(0)], dev(dx=d))

    def meta_step(n):
        if n == 0:
            recv("meta_x1", meta_all.at[row_of(-1)])
            recv("meta_x-1", meta_all.at[row_of(1)])
            copy("meta_xx", meta_all.at[row_of(-1)], meta_all.at[row_of(-1)], dev(dx=1)).start()
            return
        if n == 1:
            recv("meta_xx", meta_all.at[row_of(-2)])
        for d in (1, -1):
            if n > 1 and (d == 1 or n < 5):
                recv(f"meta_z{d}_{n - 1}", meta_all.at[block(-d * (n - 1))])
            if n < 4 or (n == 4 and d == 1):
                b = block(-d * (n - 1))
                copy(f"meta_z{d}_{n}", meta_all.at[b], meta_all.at[b], dev(dz=d)).start()

    def meta_sent():
        sent.append(copy("meta_xx", meta_all.at[row_of(-1)], meta_all.at[row_of(-1)], dev(dx=1)))
        for d, last in ((1, 4), (-1, 3)):
            for n in range(1, last + 1):
                b = block(-d * (n - 1))
                sent.append(copy(f"meta_z{d}_{n}", meta_all.at[b], meta_all.at[b], dev(dz=d)))

    loads[5].wait()
    for b in range(4):
        wdn_t[:, 384 * b : 384 * b + 384] = wdn[384 * b : 384 * b + 384, :].T
    loads[3].wait()

    slots = [slot_s[lead + i] for i in range(TRAJ)]
    lefts = [src_s[lead + i] != owner for i in range(TRAJ)]

    sub = lax.broadcasted_iota(I32, (16, 128), 0)
    lane = lax.broadcasted_iota(I32, (16, 128), 1)
    pos = jnp.zeros((16, 128), I32)
    from_left = jnp.zeros((16, 128), I32)
    for i in range(TRAJ):
        mine = (sub >> 1) == i
        pos = pos + jnp.where(mine, slots[i], 0)
        from_left = from_left + jnp.where(mine, lefts[i].astype(I32), 0)
    recv("meta_l", meta_l)

    def step_row(n):
        wide = [jnp.broadcast_to(m[n : n + 1, :], (16, 128)) for m in (meta_l, meta)]
        return jnp.where(from_left == 1, wide[0], wide[1])

    row = jnp.where((sub & 1) == 0, step_row(1), step_row(2))
    stamp = jnp.sum(jnp.where(lane == pos, row.astype(F32), 0.0), axis=1, keepdims=True)
    level = 1.0 - stamp * (1.0 / KSTEPS)
    coef = jnp.sqrt((1.0 / KSTEPS) * (1.0 - level + (1.0 / KSTEPS)) / level) / 0.7
    coef_u[...] = jnp.broadcast_to(coef, (16, 128))
    for kind, dst in ((0, mod_s), (1, mod_c), (2, mod_g)):
        acc = jnp.zeros((16, D), F32)
        for t in range(KSTEPS):
            acc = jnp.where(stamp == float(t), jnp.broadcast_to(modl[t, pl.ds(kind, 1), :], (16, D)), acc)
        dst[...] = acc + 1.0 if kind == 1 else acc

    def assemble(own, arrived, i):
        v = jnp.where(lefts[i], arrived.astype(F32), own.astype(F32))
        tmp[...] = v
        return tmp[pl.ds(0, 32, stride=2), :], tmp[pl.ds(1, 32, stride=2), :]

    recv("shift_a", rcv_a)
    for i in range(TRAJ):
        for step, v in enumerate(assemble(lat[slots[i]], rcv_a[i], i)):
            u = 2 * i + step
            xs[u // 3, (u % 3) * 32 : (u % 3) * 32 + 32, :] = v

    def spread(pair):
        return jnp.concatenate([pair[:, :64], pltpu.roll(pair, 64, 1)[:, :64]], axis=0)

    for i in (4, 6, 7, 8, 9):
        loads[i].wait()

    yu, yd, yo = (lax.rem(y + i, NY) for i in (1, 3, 2))
    held = ((yo, yo), (yd, yu), (yu, yd), (y, y))

    def embed(s):
        even, odd = (xs[k] for k in held[s])
        rows = jnp.concatenate([even[:, :64], pltpu.roll(odd, 64, 1)[:, :64]], axis=0)
        emb[s * CH : s * CH + CH, :] = jnp.dot(rows.astype(BF16), wpatch[...], preferred_element_type=F32)

    def norm(s, blocks):
        for b in blocks:
            rb = s * CH + b * 16
            u = held[s][b // 6] * 3 + (b % 6) // 2
            v = emb[rb : rb + 16, :]
            v = v - jnp.mean(v, axis=-1, keepdims=True)
            i = lax.rsqrt(jnp.mean(v * v, axis=-1, keepdims=True) + EPS)
            modb[rb : rb + 16, :] = (v * i * mod_c[pl.ds(u, 1), :] + mod_s[pl.ds(u, 1), :]).astype(BF16)

    def up(s, n):
        rows, cols = slice(s * CH, s * CH + CH), slice(256 * n, 256 * n + 256)
        pre = jnp.dot(modb[rows, :], wup[:, cols], preferred_element_type=F32)
        th = jnp.tanh(GELU_K * (pre + GELU_C * (pre * pre * pre)))
        act[rows, cols] = (pre * (0.5 * (1.0 + th))).astype(BF16)
        dg[rows, cols] = pre

    def slope_of(s):
        rows = slice(s * CH, s * CH + CH)
        for n in range(4):
            cols = slice(256 * n, 256 * n + 256)
            pre = dg[rows, cols]
            sq = pre * pre
            th = jnp.tanh(GELU_K * (pre + GELU_C * (sq * pre)))
            dg[rows, cols] = 0.5 * (1.0 + th) + (0.5 * GELU_K) * pre * (1.0 - th * th) * (1.0 + 3.0 * GELU_C * sq)

    def down(s):
        rows = slice(s * CH, s * CH + CH)
        for j in range(2):
            q = pl.multiple_of((1 - c if j == 0 else c) * 768, 768)
            v = jnp.dot(act[rows, :], wdn_t[:, pl.ds(q, 768)], preferred_element_type=F32)
            for h in range(2):
                if j == 0:
                    dsend[s, h] = v[96 * h : 96 * h + 96].astype(BF16)
                else:
                    pk[s, h] = v[96 * h : 96 * h + 96]
            if j == 0:
                send(f"d2d{s}", dsend.at[s], drecv.at[s], dev(dc=1))

    def presum(s):
        recv(f"d2d{s}", drecv.at[s])
        for h in range(2):
            pk[s, h] = pk[s, h] + drecv[s, h].astype(F32)

    def ygo(name, i, v, d):
        ysend[i] = v.astype(BF16)
        send(name, ysend.at[i], yrecv.at[i], dev(dy=d))

    def yphase(s):
        if s == 1:
            presum(0)
            ygo("y1a", 0, pk[0, 0], 1)
            ygo("y1b", 1, pk[0, 1], -1)
        elif s == 2:
            presum(1)
            ygo("y2a", 2, pk[1, 0], -1)
            ygo("y2b", 3, pk[1, 1], 1)
        elif s == 3:
            presum(2)
            recv("y1a", yrecv.at[0])
            ygo("y3a", 5, pk[2, 0] + yrecv[0].astype(F32), 1)
            recv("y1b", yrecv.at[1])
            ygo("y3b", 4, pk[2, 1] + yrecv[1].astype(F32), -1)

    embed(0)
    norm(0, range(12))
    for s in range(4):
        if s < 3:
            embed(s + 1)
        for n in range(4):
            up(s, n)
            if s < 3:
                norm(s + 1, range(3 * n, 3 * n + 3))
        yphase(s)
        down(s)
        meta_step(s)
    def transpose_pair(p, src, put):
        tok = slice(p * 384, p * 384 + 384)
        for b in range(4):
            put(b, tok, src[tok, 384 * b : 384 * b + 384].T)

    def put_up(b, tok, t):
        up_t[2 * b, :, tok] = t[:192]
        up_t[2 * b + 1, :, tok] = t[192:]

    def put_mod(b, tok, t):
        for zz in range(2):
            for xx in range(NX):
                o = zz * 192 + xx * 48
                mod_t[xx, (2 * b + zz) * 48 : (2 * b + zz) * 48 + 48, tok] = t[o : o + 48]

    presum(3)
    part = lambda k, h: pfull.at[k, c, h]
    recv("y2a", yrecv.at[2])
    recv("y3a", yrecv.at[5])
    pfull[y, c, 0] = (pk[3, 0] + yrecv[2].astype(F32) + yrecv[5].astype(F32)).astype(BF16)
    send("g_up_a", part(y, 0), part(y, 0), dev(dy=1))
    recv("y2b", yrecv.at[3])
    recv("y3b", yrecv.at[4])
    pfull[y, c, 1] = (pk[3, 1] + yrecv[3].astype(F32) + yrecv[4].astype(F32)).astype(BF16)
    send("g_dn_b", part(y, 1), part(y, 1), dev(dy=-1))
    send("g_up_b", part(y, 1), part(y, 1), dev(dy=1))
    send("g_dn_a", part(y, 0), part(y, 0), dev(dy=-1))
    send("c_own", pfull.at[y, c], pfull.at[y, c], dev(dc=1))

    loss_own[...] = jnp.zeros((1, 128), F32)

    def mix(w, k, t, r0, behind=()):
        for b in range(6):
            o = t * 96 + b * 16
            u = k * 3 + b // 2
            proj = jnp.concatenate([pfull[k, q, t, b * 16 : b * 16 + 16, :] for q in range(2)], axis=1).astype(F32)
            v = emb[r0 + b * 16 : r0 + b * 16 + 16, :] + mod_g[pl.ds(u, 1), :] * proj
            v = v - jnp.mean(v, axis=-1, keepdims=True)
            i = lax.rsqrt(jnp.mean(v * v, axis=-1, keepdims=True) + EPS)
            v = v * i
            fin[w, o : o + 16, :] = v
            finb[w, o : o + 16, :] = v.astype(BF16)
            inv[w, o : o + 16, :] = jnp.broadcast_to(i, (16, 128))
        for slot, lo in behind:
            dact(slot * CH, lo)

    def rest(w, k, offs):
        velocity = lax.dot_general(finb[w], wv[...], (((1,), (1,)), ((), ())), preferred_element_type=F32)
        drawn, target = spread(nz[k]), spread(od[k])
        err = velocity - target
        dv = [None] * 6
        for j in range(3):
            u = k * 3 + j
            cu = coef_u[pl.ds(u, 1), :][:, :64]
            au = adv_u[pl.ds(u, 1), :][:, :1]
            part = jnp.zeros((32, 64), F32)
            for h in range(2):
                o = h * 96 + j * 32
                e, n = err[o : o + 32], drawn[o : o + 32]
                part = part + cu * n * e + 0.5 * cu * cu * e * e
            logratio = -jnp.sum(jnp.sum(part, axis=0, keepdims=True), axis=1, keepdims=True) * (1.0 / 4096)
            ratio = jnp.exp(logratio)
            plain = ratio * au
            bounded = jnp.clip(ratio, 0.8, 1.2) * au
            loss_own[...] += jnp.broadcast_to(-jnp.minimum(plain, bounded), (1, 128))
            slope = jnp.where(plain <= bounded, -au * ratio * (1.0 / (SURV * 2)), 0.0)
            for h in range(2):
                o = h * 96 + j * 32
                e, n = err[o : o + 32], drawn[o : o + 32]
                dv[h * 3 + j] = slope * (-(cu * n + cu * cu * e) * (1.0 / 4096))
        dvel = jnp.concatenate(dv, axis=0).astype(BF16)
        dfin = jnp.dot(dvel, wv[...], preferred_element_type=F32)
        dfin_s[...] = dfin

        for t in range(2):
            for b in range(6):
                o = t * 96 + b * 16
                u = k * 3 + b // 2
                g = dfin_s[o : o + 16, :]
                f = fin[w, o : o + 16, :]
                m1 = jnp.mean(g, axis=-1, keepdims=True)
                m2 = jnp.mean(g * f, axis=-1, keepdims=True)
                i = inv[w, o : o + 16, :][:, :1]
                r = offs[t] + b * 16
                ups[r : r + 16, :] = (mod_g[pl.ds(u, 1), :] * (i * (g - m1 - f * m2))).astype(BF16)

    def dact(r0, lo):
        rows, cols = slice(r0, r0 + CH), slice(lo, lo + 512)
        v = jnp.dot(ups[rows, :], wdn[:, cols], preferred_element_type=F32)
        dpre[rows, cols] = (v * dg[rows, cols]).astype(BF16)

    def fwd_core(name, k, h):
        send(name, part(k, h), part(k, h), dev(dc=1))

    def got(name, k, h):
        recv(name, part(k, h))

    def core(name, k, h):
        recv(name, pfull.at[k, 1 - c, h])

    recv("shift_b", rcv_b)
    for i in range(TRAJ):
        for arr, which, dst in ((noi, 0, nz), (old, 1, od)):
            for step, v in enumerate(assemble(arr[slots[i]], rcv_b[which, i], i)):
                u = 2 * i + step
                dst[u // 3, (u % 3) * 32 : (u % 3) * 32 + 32, :] = v

    meta_step(4)

    def bounds(g, carry):
        end = carry[0] + cnt_s[g]
        out = [end]
        for i in range(TRAJ):
            hit = (lead + i >= carry[0]) & (lead + i < end)
            out += [jnp.where(hit, carry[0], carry[1 + 2 * i]), jnp.where(hit, end, carry[2 + 2 * i])]
        return tuple(out)

    ends = lax.fori_loop(0, 48, bounds, (jnp.int32(0),) * (1 + 2 * TRAJ))
    recv("c_own", pfull.at[y, 1 - c])
    own = (3 * CH, 3 * CH + 96)
    for t in range(2):
        mix(0, y, t, own[t])
    meta_step(5)
    meta_sent()
    for r in range(NZ * NX):
        meta_flat[r : r + 1, :] = meta_all[r, 0:1, :]
    ranks = meta_flat[...]
    hot = (lax.broadcasted_iota(I32, (NZ * NX, SURV), 0) == src_v[...]).astype(F32).astype(BF16)
    first = (((0,), (0,)), ((), ()))
    hi = lax.dot_general((ranks >> 4).astype(F32).astype(BF16), hot, first, preferred_element_type=F32)[:16]
    lo = lax.dot_general((ranks & 15).astype(F32).astype(BF16), hot, first, preferred_element_type=F32)[:16]
    by_slot = hi * 16.0 + lo
    rank = jnp.sum(
        jnp.where(lax.broadcasted_iota(I32, (16, SURV), 0) == slot_v[...], by_slot, 0.0), axis=0, keepdims=True
    )
    rank_i = rank.astype(I32)
    sq_i = rank_i * rank_i
    sq_hi, sq_lo = (sq_i >> 10).astype(F32), (sq_i & 1023).astype(F32)
    jdx = lax.broadcasted_iota(I32, (1, SURV), 1)

    for i in range(TRAJ):
        lo_i, hi_i = ends[1 + 2 * i], ends[2 + 2 * i]
        inside = (jdx >= lo_i) & (jdx < hi_i)

        def total(v):
            return jnp.sum(jnp.where(inside, v, 0.0), axis=1, keepdims=True)

        s1 = total(rank)
        s1_i = s1.astype(I32)
        s2_i = total(sq_hi).astype(I32) * 1024 + total(sq_lo).astype(I32)
        n_i = jnp.full((1, 1), hi_i - lo_i, I32)
        n = n_i.astype(F32)
        r = jnp.sum(jnp.where(jdx == lead + i, rank, 0.0), axis=1, keepdims=True)
        dev_i = jnp.sqrt((n_i * s2_i - s1_i * s1_i).astype(F32)) / n
        a = (r - s1 / n) / jnp.maximum(dev_i, 1.0)
        adv_u[2 * i : 2 * i + 2, :] = jnp.broadcast_to(a, (2, 128))

    slope_of(0)
    got("g_up_a", yd, 0)
    send("r_up", part(yd, 0), part(yd, 0), dev(dy=1))
    fwd_core("c_da", yd, 0)
    got("g_dn_b", yu, 1)
    send("r_dn", part(yu, 1), part(yu, 1), dev(dy=-1))
    fwd_core("c_ub", yu, 1)
    rest(0, y, own)
    slope_of(3)
    for p in range(2):
        transpose_pair(p, modb, put_mod)

    core("c_da", yd, 0)
    core("c_ub", yu, 1)
    mix(0, yu, 1, CH + 96, [(3, 0)])
    mix(1, yd, 0, CH, [(3, 512)])
    got("g_dn_a", yu, 0)
    fwd_core("c_ua", yu, 0)
    got("g_up_b", yd, 1)
    fwd_core("c_db", yd, 1)
    slope_of(1)
    slope_of(2)
    core("c_ua", yu, 0)
    mix(0, yu, 0, 2 * CH)
    rest(0, yu, (2 * CH, CH + 96))
    core("c_db", yd, 1)
    mix(1, yd, 1, 2 * CH + 96)
    got("r_up", yo, 0)
    fwd_core("c_oa", yo, 0)
    got("r_dn", yo, 1)
    fwd_core("c_ob", yo, 1)
    rest(1, yd, (CH, 2 * CH + 96))
    transpose_pair(1, ups, put_up)
    core("c_oa", yo, 0)
    core("c_ob", yo, 1)
    mix(0, yo, 0, 0, [(1, 0)])
    mix(0, yo, 1, 96, [(2, 0)])
    rest(0, yo, (0, 96))
    transpose_pair(0, ups, put_up)

    def grad_x(off, b):
        k = at(x, NX, off)
        v = jnp.dot(mod_t[k], dpre[:, 512 * b : 512 * b + 512], preferred_element_type=F32).astype(BF16)
        gd[k, 2 * b], gd[k, 2 * b + 1] = v[:, :256], v[:, 256:]

    def grad_z(off, b):
        k = at(z, NZ, off)
        v = jnp.dot(up_t[k], act[:, 512 * b : 512 * b + 512], preferred_element_type=F32).astype(BF16)
        gu[k, 2 * b], gu[k, 2 * b + 1] = v[:, :256], v[:, 256:]

    def at(axis_pos, n, off):
        return lax.rem(axis_pos + (off + n), n)

    def ring(n):
        spec = {}
        for d in (1, -1):
            for h in range(2):
                far = (h == 0) == (d == 1)
                last = n // 2 if far else n // 2 - 1
                for i in range(1, last + 1):
                    spec[d, h, i] = (d * (last + 1 - i), h, d)
        return spec, {m: i for i, m in enumerate(spec)}

    zspec, zi = ring(NZ)
    xspec, xi = ring(NX)

    class Stream:
        def __init__(self, tag, axis, buf, land):
            self.tag, self.axis, self.buf, self.land = tag, axis, buf, land
            self.spec, self.idx = (zspec, zi) if axis == "z" else (xspec, xi)
            self.pos, self.n = (z, NZ) if axis == "z" else (x, NX)

        def slot(self, b, m):
            return self.land.at[b * len(self.spec) + self.idx[m]]

        def go(self, b, *m):
            off, h, d = self.spec[m]
            to = dev(dz=d) if self.axis == "z" else dev(dx=d)
            send(f"{self.tag}{b}{m}", self.buf.at[at(self.pos, self.n, off), 2 * b + h], self.slot(b, m), to)

        def got(self, b, m):
            recv(f"{self.tag}{b}{m}", self.slot(b, m))
            return self.land[b * len(self.spec) + self.idx[m]].astype(F32)

        def relay(self, b, d, h, i):
            off = self.spec[d, h, i][0]
            k = at(self.pos, self.n, off)
            v = self.got(b, (d, h, i - 1))
            self.buf[k, 2 * b + h] = (self.buf[k, 2 * b + h].astype(F32) + v).astype(BF16)
            self.go(b, d, h, i)

        def far(self, b, i):
            self.relay(b, 1, 0, i)
            self.relay(b, -1, 1, i)

        def near(self, b, i):
            self.relay(b, 1, 1, i)
            self.relay(b, -1, 0, i)

        def total(self, b, h):
            v = self.buf[at(self.pos, self.n, 0), 2 * b + h].astype(F32)
            for d in (1, -1):
                last = max(i for e, g, i in self.spec if (e, g) == (d, h))
                v = v + self.got(b, (d, h, last))
            return v

        def first(self, b):
            self.go(b, 1, 0, 1)
            self.go(b, -1, 1, 1)

    Z1 = Stream("z", "z", gu, zr)
    X1 = Stream("x", "x", gd, xr)
    X2 = Stream("s", "z", s2d, s2dr)

    def finish_x(b):
        for h in range(2):
            v = X1.total(b, h).astype(BF16)
            for i in range(NZ):
                s2d[i, 2 * b + h] = v[48 * i : 48 * i + 48]
        X2.first(b)
        X2.go(b, 1, 1, 1)
        X2.go(b, -1, 0, 1)

    def hop(b, i):
        X2.far(b, i)
        if i < 4:
            X2.near(b, i)

    def done_x(b):
        for h in range(2):
            up_v[b, :, 256 * h : 256 * h + 256] = X2.total(b, h)
        store(f"up{b}", up_v.at[b], out.at[0, :, pl.ds(512 * b, 512)])

    def finish_z(b):
        for h in range(2):
            v = Z1.total(b, h).astype(BF16)
            for i in range(NX):
                s2u[b, i, :, 256 * h : 256 * h + 256] = v[48 * i : 48 * i + 48]
        for i in (2, 1, 3):
            send(f"t{b}{i}", s2u.at[b, at(x, NX, i)], s2ur.at[b, i], dev(dx=i))

    def done_z(b):
        v = s2u[b, x].astype(F32)
        for i in (1, 3, 2):
            recv(f"t{b}{i}", s2ur.at[b, i])
            v = v + s2ur[b, i].astype(F32)
        dn_v[b] = v
        store(f"dn{b}", dn_v.at[b], out.at[1, :, pl.ds(512 * b, 512)])

    stores = []

    def store(name, src, dst):
        d = pltpu.make_async_copy(src, dst, osem.at[len(stores)])
        d.start()
        stores.append(d)

    def loss_step(n):
        if n == 0:
            for d in (1, -1):
                send(f"loss_x{d}", loss_own, loss_x.at[d % 4], dev(dx=d))
        elif n == 1:
            recv("loss_x1", loss_x.at[1])
            recv("loss_x-1", loss_x.at[3])
            send("loss_xx", loss_x.at[1], loss_x.at[2], dev(dx=1))
        elif n == 2:
            recv("loss_xx", loss_x.at[2])
            loss_z[0] = loss_own[...] + loss_x[1] + loss_x[2] + loss_x[3]
        if n >= 2:
            for d in (1, -1):
                if n > 2 and (d == 1 or n < 6):
                    recv(f"loss_z{d}_{n - 1}", loss_z.at[(d * (n - 2)) % NZ])
                if n < 5 or (n == 5 and d == 1):
                    send(f"loss_z{d}_{n}", loss_z.at[(d * (n - 2)) % NZ], loss_z.at[(d * (n - 1)) % NZ], dev(dz=d))

    grad_z(4, 0)
    Z1.first(0)
    dact(0, 0)
    grad_x(2, 0)
    X1.first(0)
    grad_z(4, 1)
    Z1.first(1)
    grad_z(3, 0)
    Z1.go(0, 1, 1, 1)
    grad_z(-3, 0)
    Z1.go(0, -1, 0, 1)
    grad_x(-1, 0)
    X1.go(0, -1, 0, 1)
    grad_x(1, 0)
    X1.go(0, 1, 1, 1)
    loss_step(0)
    Z1.far(0, 2)
    grad_z(3, 1)
    Z1.go(1, 1, 1, 1)
    grad_z(-3, 1)
    Z1.go(1, -1, 0, 1)
    grad_z(2, 0)
    grad_z(-2, 0)
    Z1.far(1, 2)
    grad_z(2, 1)
    grad_z(-2, 1)
    Z1.near(0, 2)
    X1.far(0, 2)
    for slot in range(3):
        dact(slot * CH, 512)
    grad_x(2, 1)
    grad_z(1, 0)
    grad_z(-1, 0)
    grad_z(0, 0)
    grad_x(0, 0)
    Z1.near(1, 2)
    loss_step(1)
    Z1.far(0, 3)
    X1.first(1)
    grad_x(-1, 1)
    grad_x(1, 1)
    grad_z(1, 1)
    grad_z(-1, 1)
    Z1.far(1, 3)
    loss_step(2)
    Z1.near(0, 3)
    X1.go(1, 1, 1, 1)
    X1.go(1, -1, 0, 1)
    finish_x(0)
    grad_z(0, 1)
    grad_x(0, 1)
    X1.far(1, 2)
    Z1.near(1, 3)
    loss_step(3)
    Z1.far(0, 4)
    hop(0, 2)
    finish_x(1)
    Z1.far(1, 4)
    loss_step(4)
    hop(0, 3)
    hop(1, 2)
    finish_z(0)
    loss_step(5)
    hop(0, 4)
    hop(1, 3)
    finish_z(1)
    loss_step(6)
    v = loss_z[0]
    for i in range(1, NZ):
        v = v + loss_z[i]
    loss_v[...] = v * (1.0 / (SURV * 2))
    store("loss", loss_v, out_loss)
    hop(1, 4)
    done_x(0)
    done_z(0)
    done_x(1)
    done_z(1)
    for d in stores:
        d.wait()
    for d in sent:
        d.wait_send()
    assert len(ids) <= NSEM, len(ids)


NSEM = 136


def shards(
    latents, noise, behavior_velocity, timestep, reward_rank_integer, surviving_source_index,
    surviving_slot_index, group_kept_count, patch_input_weight, modulation_lookup,
    up_projection_weight, down_projection_weight, velocity_head_weight,
):
    def pairs(a):
        return a.reshape(SLOTS, 2, 32, 128).transpose(0, 2, 1, 3).reshape(SLOTS, 64, 128)

    smem = pl.BlockSpec(memory_space=pltpu.SMEM)
    vmem = pl.BlockSpec(memory_space=pltpu.VMEM)
    hbm = pl.BlockSpec(memory_space=pl.ANY)
    V = pltpu.VMEM
    piece = (CH // 2, 768)
    scratch = [
        V((1, SURV), I32), V((1, SURV), I32),
        V((SLOTS, 64, 128), BF16), V((SLOTS, 64, 128), BF16), V((SLOTS, 64, 128), BF16), V((64, D), BF16),
        V((KSTEPS, 3, D), F32), V((64, D), BF16), V((CH, D), F32), V((HID, D), BF16),
        V((8, 128), I32), V((D, HID), BF16), V((D, HID), BF16),
        V((TRAJ, 64, 128), BF16), V((2, TRAJ, 64, 128), BF16), V((TRAJ, 64, 128), BF16), V((2, TRAJ, 64, 128), BF16),
        V((8, 128), I32), V((NZ * NX, 8, 128), I32), V((NZ * NX, 128), I32), V((64, 128), F32),
        V((4, 96, 128), F32), V((4, 96, 128), F32), V((4, 96, 128), F32),
        V((16, D), F32), V((16, D), F32), V((16, D), F32), V((16, 128), F32), V((16, 128), F32),
        V((ROWS, D), F32), V((ROWS, D), BF16), V((ROWS, HID), BF16), V((ROWS, HID), F32), V((ROWS, HID), BF16),
        V((4, 2, *piece), BF16), V((4, 2, *piece), BF16), V((4, 2, *piece), F32),
        V((6, *piece), BF16), V((6, *piece), BF16), V((4, 2, 2, *piece), BF16),
        V((2, CH, D), F32), V((2, CH, D), BF16), V((2, CH, 128), F32), V((ROWS, D), BF16),
        V((NX, 384, ROWS), BF16), V((NZ, 192, ROWS), BF16),
        V((NZ, 4, 192, 256), BF16), V((NX, 4, 384, 256), BF16), V((28, 192, 256), BF16), V((12, 384, 256), BF16),
        V((2, NX, 48, 512), BF16), V((NZ, 4, 48, 256), BF16), V((2, NX, 48, 512), BF16), V((28, 48, 256), BF16),
        V((1, 128), F32), V((NX, 1, 128), F32), V((NZ, 1, 128), F32),
        V((2, 48, 512), F32), V((2, 48, 512), F32), V((1, 128), F32),
        pltpu.SemaphoreType.DMA((10,)), pltpu.SemaphoreType.DMA((5,)), pltpu.SemaphoreType.DMA((NSEM,)), pltpu.SemaphoreType.DMA((NSEM,)),
    ]
    grads, loss = pl.pallas_call(
        kernel,
        out_shape=(
            jax.ShapeDtypeStruct((2, 48, HID), F32),
            jax.ShapeDtypeStruct((1, 128), F32),
        ),
        in_specs=[smem] * 3 + [vmem] * 2 + [hbm] * 10,
        out_specs=(hbm,) * 2,
        scratch_shapes=scratch,
        compiler_params=pltpu.CompilerParams(collective_id=0, has_side_effects=True, vmem_limit_bytes=67043328),
    )(
        surviving_slot_index, surviving_source_index, group_kept_count,
        reward_rank_integer.reshape(1, SLOTS), timestep.T,
        surviving_source_index.reshape(1, SURV), surviving_slot_index.reshape(1, SURV), pairs(latents), pairs(noise), pairs(behavior_velocity),
        patch_input_weight, modulation_lookup, velocity_head_weight.T,
        up_projection_weight, down_projection_weight,
    )
    return grads[0], grads[1], loss[0, 0]


def solution(mesh):
    finer = Mesh(mesh.devices.reshape(NZ, NX, NY, NC), ("z", "x", "y", "c"))
    dp, fs = ("z", "x"), ("y", "c")
    in_specs = (
        P(dp, None, None), P(dp, None, None), P(dp, None, None), P(dp, None), P(dp), P(), P(), P(), P(), P(),
        P(None, fs), P(None, fs), P(),
    )
    out_specs = (P(dp, fs), P(dp, fs), P())
    return jax.shard_map(shards, mesh=finer, in_specs=in_specs, out_specs=out_specs, check_vma=False)
```
